16 devices in a mesh: rep: 2 (over y, z), seq: 8 (over x, core).
Axes of the slice: x: 4, y: 2, z: 1, core: 2. Of those that a mesh axis runs over, the one named last changes fastest.
The devices are a block of a 4x4x8 slice.
Arguments:
- hidden: bfloat16 [128, 4096], P('rep'), parts along dimension 0
- w_query: bfloat16 [4096, 4096], replicated
- w_key: bfloat16 [4096, 1024], replicated
- w_value: bfloat16 [4096, 1024], replicated
- w_out: bfloat16 [4096, 4096], P('seq')
- k_cache: bfloat16 [128, 1024, 8, 128], P('rep', 'seq'), parts along dimension 0
- v_cache: bfloat16 [128, 1024, 8, 128], P('rep', 'seq'), parts along dimension 0
- positions: int32 [128], P('rep'), parts along dimension 0
Outputs:
- output 1: bfloat16 [128, 4096], P('rep'), parts along dimension 0
- output 2: bfloat16 [128, 1024, 8, 128], P('rep', 'seq'), parts along dimension 0
- output 3: bfloat16 [128, 1024, 8, 128], P('rep', 'seq'), parts along dimension 0
There are 2 independent parts. The reference program is written for one: setup_inputs(seed, part) draws one part's arguments, and reference() takes and returns one part's arrays. A program takes and returns all parts, laid end to end along the dimension named above; an argument that names none is the same for every part.
All inputs are finite; a program needn't handle non-finite values.
Results may differ from the reference program's by a relative error of at most 0.00593277.
Values are sent between devices in bfloat16 or wider.
A program may use at most 768 MiB of HBM per device.

```python
import math
import jax
import jax.numpy as jnp
from jax import lax

D_MODEL = 4096
NUM_HEADS = 32
KV_HEADS = 8
HEAD_DIM = 128
BATCH_SIZE = 64
LOCAL_LEN = 128
SEQ_LEN = 1024


def query_shift(hidden, w_query):
    group_size = NUM_HEADS // KV_HEADS
    q_flat = jnp.dot(hidden, w_query, preferred_element_type=jnp.float32).astype(jnp.bfloat16).astype(jnp.float32)
    q_heads = q_flat.reshape(BATCH_SIZE, KV_HEADS, group_size, HEAD_DIM)
    gram_mat = jnp.einsum('bkgd,bkhd->bkgh', q_heads, q_heads)
    coeffs = jnp.linalg.solve(gram_mat, jnp.ones((BATCH_SIZE, KV_HEADS, group_size, 1), jnp.float32))
    score_drop = math.log(SEQ_LEN) - 1.0
    return -score_drop * HEAD_DIM ** 0.5 * jnp.einsum('bkgo,bkgd->bkd', coeffs, q_heads)


def setup_inputs(seed: int = 0, part: int = 0) -> dict:
    root = jax.random.key(seed)
    shared = jax.random.split(root, 4)
    part_keys = jax.random.split(jax.random.fold_in(root, part), 6)
    blocks = SEQ_LEN // LOCAL_LEN
    block_shape = (BATCH_SIZE, blocks, LOCAL_LEN, KV_HEADS, HEAD_DIM)
    cache_shape = (BATCH_SIZE, SEQ_LEN, KV_HEADS, HEAD_DIM)
    q_width = NUM_HEADS * HEAD_DIM
    kv_width = KV_HEADS * HEAD_DIM
    hidden = jax.random.normal(part_keys[0], (BATCH_SIZE, D_MODEL), jnp.float32).astype(jnp.bfloat16)
    w_query = (jax.random.normal(shared[0], (D_MODEL, q_width), jnp.float32) * D_MODEL ** -0.5).astype(jnp.bfloat16)
    w_key = (jax.random.normal(shared[1], (D_MODEL, kv_width), jnp.float32) * D_MODEL ** -0.5).astype(jnp.bfloat16)
    w_value = (jax.random.normal(shared[2], (D_MODEL, kv_width), jnp.float32) * D_MODEL ** -0.5).astype(jnp.bfloat16)
    w_out = (jax.random.normal(shared[3], (q_width, D_MODEL), jnp.float32) * q_width ** -0.5).astype(jnp.bfloat16)
    key_scale = jax.random.uniform(part_keys[1], (BATCH_SIZE, blocks, 1, KV_HEADS, 1), jnp.float32, 0.5, 1.5)
    key_noise = jax.random.normal(part_keys[2], block_shape, jnp.float32) * key_scale
    k_cache = key_noise.reshape(cache_shape) + query_shift(hidden, w_query)[:, None]
    v_base = jax.random.normal(part_keys[3], (BATCH_SIZE, blocks, 1, KV_HEADS, HEAD_DIM), jnp.float32)
    v_cache = (v_base + jax.random.normal(part_keys[4], block_shape, jnp.float32)).reshape(cache_shape)
    positions = jax.random.randint(part_keys[5], (BATCH_SIZE,), SEQ_LEN // 4, SEQ_LEN, dtype=jnp.int32)
    return {'hidden': hidden, 'w_query': w_query, 'w_key': w_key, 'w_value': w_value, 'w_out': w_out, 'k_cache': k_cache.astype(jnp.bfloat16), 'v_cache': v_cache.astype(jnp.bfloat16), 'positions': positions}


def reference(hidden, w_query, w_key, w_value, w_out, k_cache, v_cache, positions):
    group_size = NUM_HEADS // KV_HEADS
    q_flat = jnp.dot(hidden, w_query, preferred_element_type=jnp.float32).astype(jnp.bfloat16)
    key_new = jnp.dot(hidden, w_key, preferred_element_type=jnp.float32).astype(jnp.bfloat16).reshape(BATCH_SIZE, KV_HEADS, HEAD_DIM)
    value_new = jnp.dot(hidden, w_value, preferred_element_type=jnp.float32).astype(jnp.bfloat16).reshape(BATCH_SIZE, KV_HEADS, HEAD_DIM)
    seq_ids = jnp.arange(SEQ_LEN)
    at_pos = (seq_ids[None, :] == positions[:, None])[:, :, None, None]
    k_updated = jnp.where(at_pos, key_new[:, None], k_cache)
    v_updated = jnp.where(at_pos, value_new[:, None], v_cache)
    is_valid = seq_ids[None, :] <= positions[:, None]
    q_heads = q_flat.astype(jnp.float32).reshape(BATCH_SIZE, KV_HEADS, group_size, HEAD_DIM)

    def one_row(row_args):
        q_row, k_row, v_row, valid_row = row_args
        scores = jnp.einsum('kgd,skd->kgs', q_row, k_row.astype(jnp.float32)) * HEAD_DIM ** -0.5
        scores = jnp.where(valid_row[None, None, :], scores, -jnp.inf)
        weights = jax.nn.softmax(scores, axis=-1)
        return jnp.einsum('kgs,skd->kgd', weights, v_row.astype(jnp.float32))

    attended = lax.map(one_row, (q_heads, k_updated, v_updated, is_valid))
    combined = attended.reshape(BATCH_SIZE, NUM_HEADS * HEAD_DIM).astype(jnp.bfloat16)
    result = jnp.dot(combined, w_out, preferred_element_type=jnp.float32).astype(jnp.bfloat16)
    return result, k_updated, v_updated
```

```python
import functools
import math

import jax
import jax.numpy as jnp
from jax import lax
from jax.experimental import pallas as pl
from jax.experimental.pallas import tpu as pltpu
from jax.sharding import PartitionSpec as P

MESH = pl.DeviceIdType.MESH
NEG = -3.4028234e38
F32, BF16 = jnp.float32, jnp.bfloat16
CORES = 2
NT = (((1,), (1,)), ((), ()))


def step_kernel(chips, x_hbm, wq_hbm, wk_hbm, wv_hbm, wo_hbm, k_hbm, v_hbm, pos_ref, pos2_ref,
                y_ref, kout, vout, kv_all,
                x_v, wbuf, wo_v, qs, q_all, colmask, oraw, mraw, lraw, om, op, orecv, ofin,
                ys, yp, yr, yfull,
                lsem, kvsem, q_ss, q_rs, n_ss, n_rs, od_s, od_r, oi_s, oi_r, yd_s, yd_r, yi_s, yi_r, ag_s, ag_r):
    batch = k_hbm.shape[0]
    local_len = k_hbm.shape[1] // 8
    chunks = om.shape[0]
    cb = batch // chunks
    half = batch // 2
    scale2 = k_hbm.shape[2] ** -0.5 * math.log2(math.e)
    rep = lax.axis_index('rep')
    me = lax.axis_index('seq')
    chip, core = me // CORES, me % CORES
    base = me * local_len
    quarter = (chip % 2) * CORES + core

    def dev(c, e):
        return (rep, lax.rem(c, chips) * CORES + e)

    partner = dev(chip, 1 - core)

    ncols = 256
    lx = pltpu.make_async_copy(x_hbm, x_v, lsem.at[0])
    lw = [pltpu.make_async_copy(wq_hbm.at[:, pl.ds(pl.multiple_of(quarter * 1024 + i * 512, 512), 512)], wbuf.at[i], lsem.at[1 + i])
          for i in range(2)]
    lk = pltpu.make_async_copy(wk_hbm.at[:, pl.ds(pl.multiple_of(quarter * ncols, ncols), ncols)], wbuf.at[2, :, pl.ds(0, ncols)], lsem.at[3])
    lv = pltpu.make_async_copy(wv_hbm.at[:, pl.ds(pl.multiple_of(quarter * ncols, ncols), ncols)], wbuf.at[2, :, pl.ds(ncols, ncols)], lsem.at[4])
    lo = pltpu.make_async_copy(wo_hbm, wo_v, lsem.at[5])
    lkc = [pltpu.make_async_copy(k_hbm.at[pl.ds(i * cb, cb)], kout.at[pl.ds(i * cb, cb)], kvsem.at[0, i]) for i in range(chunks)]
    lvc = [pltpu.make_async_copy(v_hbm.at[pl.ds(i * cb, cb)], vout.at[pl.ds(i * cb, cb)], kvsem.at[1, i]) for i in range(chunks)]
    lx.start()
    lw[0].start()
    lw[1].start()

    barrier = pltpu.get_barrier_semaphore()
    for d in range(chips):
        for f in range(CORES):
            if d or f:
                pl.semaphore_signal(barrier, inc=1, device_id=dev(chip + d, lax.rem(core + f, CORES)), device_id_type=MESH)

    row = lax.broadcasted_iota(jnp.int32, colmask.shape, 0)
    col = lax.broadcasted_iota(jnp.int32, colmask.shape, 1)
    colmask[...] = jnp.where(col % 8 == (row // 16) * 2 + (row % 8) // 4, col, 1 << 30)

    lx.wait()
    lk.start()
    lv.start()
    for i in range(2):
        lw[i].wait()
        if i == 0:
            lkc[0].start()
            lvc[0].start()
        q = jnp.dot(x_v[...], wbuf[i], preferred_element_type=F32)
        for h in range(4):
            qs[pl.ds(i * 4 + h, batch, stride=8), :] = q[:, h * 128:(h + 1) * 128]
    q_all[quarter] = qs[...].astype(BF16)
    pl.semaphore_wait(barrier, chips * CORES - 1)

    def spread(buf, rows, ss, rs):
        copies = [pltpu.make_async_remote_copy(buf.at[quarter], buf.at[quarter], ss.at[0], rs.at[0], device_id=partner, device_id_type=MESH)]
        for side, shift in ((0, 1), (1, chips - 1)):
            part = pl.ds(side * rows // 2, rows // 2)
            for f in range(CORES):
                e = lax.rem(core + f, CORES)
                slot = 1 + side * 2 + f
                copies.append(pltpu.make_async_remote_copy(
                    buf.at[quarter, part], buf.at[quarter, part], ss.at[slot], rs.at[slot], device_id=dev(chip + shift, e), device_id_type=MESH))
        return copies

    q_copies = spread(q_all, batch * 8, q_ss, q_rs)
    for c in q_copies:
        c.start()
    lk.wait()
    lv.wait()
    lkc[1].start()
    lvc[1].start()
    kv = jnp.dot(x_v[...], wbuf[2], preferred_element_type=F32)
    for w in range(2):
        for k in range(2):
            qs[pl.ds(w * 128 + k, batch, stride=2), :] = kv[:, w * 256 + k * 128:w * 256 + (k + 1) * 128]
    for hf in range(2):
        for w in range(2):
            kv_all[quarter, hf * 128 + w * 64:hf * 128 + w * 64 + 64, :] = qs[w * 128 + hf * 64:w * 128 + hf * 64 + 64, :].astype(BF16)
    n_copies = spread(kv_all, batch * 4, n_ss, n_rs)
    for c in n_copies:
        c.start()
    for i in range(2, chunks):
        lkc[i].start()
        lvc[i].start()
    lo.start()

    rowb = lax.broadcasted_iota(jnp.int32, (64, 128), 0) // 8 % 2
    bm0 = jnp.where(rowb == 0, 1.0, 0.0).astype(BF16)
    bm1 = jnp.where(rowb == 1, 1.0, 0.0).astype(BF16)

    for c in q_copies:
        c.wait_recv()

    def pair(pi, loc):
        q = jnp.concatenate([q_all[t, pl.ds(pl.multiple_of(pi * 16, 16), 16), :] for t in range(4)], axis=0)
        lhs = jnp.concatenate([q * bm0, q * bm1], axis=1)
        kcat = jnp.concatenate([kout[2 * pi], kout[2 * pi + 1]], axis=1)
        s = lax.dot_general(lhs, kcat, NT, preferred_element_type=F32)
        lim0 = (pos_ref[2 * pi] - base) * 8
        lim1 = (pos_ref[2 * pi + 1] - base) * 8
        lim = jnp.where(lax.broadcasted_iota(jnp.int32, (16, 1), 0) < 8, lim0, lim1)
        ps = []
        for t in range(4):
            st = jnp.where(colmask[t * 16:(t + 1) * 16, :] < lim, s[t * 16:(t + 1) * 16, :], -jnp.inf)
            m = jnp.maximum(jnp.max(st, axis=1, keepdims=True), NEG)
            p = jnp.exp2((st - m) * scale2)
            mraw[t, pl.ds(pl.multiple_of(loc * 16, 16), 16), :] = jnp.broadcast_to(m, (16, 128))
            lraw[t, pl.ds(pl.multiple_of(loc * 16, 16), 16), :] = jnp.broadcast_to(jnp.sum(p, axis=1, keepdims=True), (16, 128))
            ps.append(p.astype(BF16))
        vcat = jnp.concatenate([vout[2 * pi], vout[2 * pi + 1]], axis=1)
        o = jnp.dot(jnp.concatenate(ps, axis=0), vcat, preferred_element_type=F32)
        for t in range(4):
            for b in range(2):
                r = t * 16 + b * 8
                oraw[t, pl.ds(pl.multiple_of(loc * 16 + b * 8, 8), 8), :] = o[r:r + 8, b * 128:(b + 1) * 128]

    rows_c = cb * 8
    ppc = cb // 2

    def attend(i, sub):
        def body(j, carry):
            loc = sub * (ppc // 2) + j * 2
            pair(i * ppc + loc, loc)
            pair(i * ppc + loc + 1, loc + 1)
            return carry
        lax.fori_loop(0, ppc // 4, body, 0)

    lane = lax.broadcasted_iota(jnp.int32, (8, 128), 1)
    od, oi, yd, yi, ag = {}, {}, {}, {}, {}

    def finalize(i):
        hf = i * cb // half
        first = i * rows_c - hf * half * 8
        rr = lax.broadcasted_iota(jnp.int32, (rows_c, 64), 0) + first
        cc = lax.broadcasted_iota(jnp.int32, (rows_c, 64), 1)
        rel = pos2_ref[hf:hf + 1, :] - base
        keep = (rr // 4 == cc) & (rel >= 0) & (rel < local_len)
        for t in range(4):
            qt = q_all[t, i * rows_c:(i + 1) * rows_c, :]
            sn = lax.dot_general(qt, kv_all[t, hf * 128:hf * 128 + 64, :], NT, preferred_element_type=F32)
            sn = jnp.where(keep, sn, -jnp.inf)
            mo = mraw[t]
            mn = jnp.maximum(mo, jnp.max(sn, axis=1, keepdims=True))
            pn = jnp.exp2((sn - mn[:, :64]) * scale2)
            w = jnp.exp2((mo - mn) * scale2)
            lraw[t] = lraw[t] * w + jnp.sum(pn, axis=1, keepdims=True)
            oraw[t] = oraw[t] * w + jnp.dot(pn.astype(BF16), kv_all[t, hf * 128 + 64:hf * 128 + 128, :], preferred_element_type=F32)
            mraw[t] = mn
        for e in range(CORES):
            for t in range(4):
                mt = jnp.zeros((8, 128), F32)
                lt = jnp.zeros((8, 128), F32)
                for h in range(4):
                    src = pl.ds(e * 4 + h, cb, stride=8)
                    om[i, e, t, h * cb:(h + 1) * cb, :] = oraw[t, src, :]
                    mh = mraw[t, src, :]
                    lh = lraw[t, src, :]
                    for g in range(cb // 8):
                        sel = lane == h * (cb // 8) + g
                        mt = jnp.where(sel, mh[g * 8:(g + 1) * 8], mt)
                        lt = jnp.where(sel, lh[g * 8:(g + 1) * 8], lt)
                om[i, e, t, cb * 4:cb * 4 + 8, :] = mt
                om[i, e, t, cb * 4 + 8:cb * 4 + 16, :] = lt
        od[i] = pltpu.make_async_remote_copy(om.at[i, 1 - core], op.at[i], od_s.at[i], od_r.at[i], device_id=partner, device_id_type=MESH)
        od[i].start()

    nrow = cb * 4

    def merge(parts):
        ms = [p[nrow:nrow + 8] for p in parts]
        m = functools.reduce(jnp.maximum, ms)
        ws = [jnp.exp2((x - m) * scale2) for x in ms]
        l = functools.reduce(jnp.add, [w * p[nrow + 8:nrow + 16] for w, p in zip(ws, parts)])
        return m, l, ws

    def chip_reduce(i):
        od[i].wait_recv()
        for t in range(4):
            a, b = om[i, core, t], op[i, t]
            m, l, (wa, wb) = merge([a, b])
            for g in range(nrow // 8):
                r = slice(g * 8, g * 8 + 8)
                om[i, core, t, g * 8:g * 8 + 8, :] = a[r] * wa[:, g:g + 1] + b[r] * wb[:, g:g + 1]
            om[i, core, t, nrow:nrow + 8, :] = m
            om[i, core, t, nrow + 8:nrow + 16, :] = l
        oi[i] = []
        for d in range(1, chips):
            c = pltpu.make_async_remote_copy(om.at[i, core, lax.rem(chip + d, chips)], orecv.at[i, d - 1], oi_s.at[i, d - 1], oi_r.at[i, d - 1],
                                             device_id=dev(chip + d, core), device_id_type=MESH)
            c.start()
            oi[i].append(c)

    def project(i):
        for c in oi[i]:
            c.wait_recv()
        if i == 0:
            lo.wait()
        parts = [om[i, core, chip]] + [orecv[i, d] for d in range(chips - 1)]
        m, l, ws = merge(parts)
        rl = 1.0 / l
        heads = []
        for h in range(4):
            rows = []
            for g in range(h * (cb // 8), (h + 1) * (cb // 8)):
                o = functools.reduce(jnp.add, [p[g * 8:g * 8 + 8] * w[:, g:g + 1] for p, w in zip(parts, ws)])
                rows.append(o * rl[:, g:g + 1])
            heads.append(jnp.concatenate(rows, axis=0).astype(BF16))
        lhs = jnp.concatenate(heads, axis=1)
        for e in range(CORES):
            for t in range(4):
                c0 = (e * 4 + t) * 512
                ys[i, e, t] = jnp.dot(lhs, wo_v[:, c0:c0 + 512], preferred_element_type=F32)
        yd[i] = pltpu.make_async_remote_copy(ys.at[i, 1 - core], yp.at[i], yd_s.at[i], yd_r.at[i], device_id=partner, device_id_type=MESH)
        yd[i].start()

    def y_chip(i):
        yd[i].wait_recv()
        ys[i, core] = ys[i, core] + yp[i]
        yi[i] = []
        for d in range(1, chips):
            c = pltpu.make_async_remote_copy(ys.at[i, core, lax.rem(chip + d, chips)], yr.at[i, d - 1], yi_s.at[i, d - 1], yi_r.at[i, d - 1],
                                             device_id=dev(chip + d, core), device_id_type=MESH)
            c.start()
            yi[i].append(c)

    def y_final(i):
        for c in yi[i]:
            c.wait_recv()
        y = ys[i, core, chip]
        for d in range(chips - 1):
            y = y + yr[i, d]
        own = (pl.ds(i * cb, cb), pl.ds(pl.multiple_of((core * 4 + chip) * 512, 512), 512))
        yfull[own] = y.astype(BF16)
        ag[i] = []
        for d in range(chips):
            for f in range(CORES):
                if d or f:
                    slot = d * CORES + f - 1
                    c = pltpu.make_async_remote_copy(yfull.at[own], yfull.at[own], ag_s.at[i, slot], ag_r.at[i, slot],
                                                     device_id=dev(chip + d, lax.rem(core + f, CORES)), device_id_type=MESH)
                    c.start()
                    ag[i].append(c)

    stages = ((finalize, 1), (chip_reduce, 2), (project, 4), (y_chip, 5), (y_final, 7))
    for k in range(2 * chunks + 6):
        if k < 2 * chunks:
            if k % 2 == 0:
                lkc[k // 2].wait()
                lvc[k // 2].wait()
            attend(k // 2, k % 2)
        if k == 1:
            for c in n_copies:
                c.wait_recv()
        for stage, lag in stages:
            i = (k - lag) // 2
            if (k - lag) % 2 == 0 and 0 <= i < chunks:
                stage(i)
    for i in range(chunks):
        for c in ag[i]:
            c.wait_recv()
    y_ref[...] = yfull[...]
    for c in q_copies + n_copies:
        c.wait_send()
    for i in range(chunks):
        for c in [od[i], yd[i]] + oi[i] + yi[i] + ag[i]:
            c.wait_send()


def patch_kernel(k_in, v_in, new_ref, pos_ref, k_ref, v_ref, src, dst):
    batch = k_ref.shape[0]
    local_len = k_ref.shape[1]
    base = lax.axis_index('seq') * local_len
    hb = batch // 2
    for t in range(4):
        src[t] = new_ref[t].astype(F32)
    for w in range(2):
        for t in range(4):
            for hf in range(2):
                for k in range(2):
                    dst[w, pl.ds(hf * hb * 8 + t * 2 + k, hb, stride=8), :] = src[t, pl.ds(hf * 128 + w * 64 + k, hb, stride=2), :]

    def body(b, carry):
        rel = pos_ref[b] - base

        @pl.when((rel >= 0) & (rel < local_len))
        def _():
            r = pl.ds(pl.multiple_of(b * 8, 8), 8)
            k_ref[b, rel] = dst[0, r, :].astype(BF16)
            v_ref[b, rel] = dst[1, r, :].astype(BF16)
        return carry
    lax.fori_loop(0, batch, body, 0)


def solution(mesh):
    cache_spec = P('rep', 'seq', None, None)
    in_specs = (P('rep', None), P(), P(), P(), P('seq', None), cache_spec, cache_spec, P('rep'))
    out_specs = (P('rep', None), cache_spec, cache_spec)
    chips = mesh.shape['seq'] // CORES
    vm = pl.BlockSpec(memory_space=pltpu.VMEM)
    hbm = pl.BlockSpec(memory_space=pl.ANY)
    sm = pl.BlockSpec(memory_space=pltpu.SMEM)

    def local_step(x, wq, wk, wv, wo, k, v, pos):
        shape4 = k.shape
        batch, width = x.shape
        k3 = k.reshape(batch, -1, k.shape[-1])
        v3 = v.reshape(k3.shape)
        chunks = 4
        cb = batch // chunks
        dma = pltpu.SemaphoreType.DMA
        in_hbm = lambda a: pltpu.with_memory_space_constraint(a, pltpu.HBM)
        in_vmem = lambda a: pltpu.with_memory_space_constraint(a, pltpu.VMEM)
        pos2 = jnp.repeat(pos, 2).reshape(2, batch)
        y, ko, vo, new = pl.pallas_call(
            functools.partial(step_kernel, chips),
            out_shape=(jax.ShapeDtypeStruct((batch, wo.shape[1]), BF16), pltpu.VMEM(k3.shape, BF16), pltpu.VMEM(k3.shape, BF16),
                       jax.ShapeDtypeStruct((4, batch * 4, 128), BF16)),
            in_specs=[hbm] * 7 + [sm, vm],
            out_specs=[vm] * 4,
            scratch_shapes=[
                pltpu.VMEM((batch, width), BF16), pltpu.VMEM((3, width, 512), BF16), pltpu.VMEM(wo.shape, BF16),
                pltpu.VMEM((batch * 8, 128), F32), pltpu.VMEM((4, batch * 8, 128), BF16), pltpu.VMEM((64, k3.shape[1]), jnp.int32),
                pltpu.VMEM((4, cb * 8, 128), F32), pltpu.VMEM((4, cb * 8, 128), F32), pltpu.VMEM((4, cb * 8, 128), F32),
                pltpu.VMEM((chunks, CORES, 4, cb * 4 + 16, 128), F32), pltpu.VMEM((chunks, 4, cb * 4 + 16, 128), F32),
                pltpu.VMEM((chunks, chips - 1, cb * 4 + 16, 128), F32), pltpu.VMEM((cb * 4, 128), F32),
                pltpu.VMEM((chunks, CORES, 4, cb, 512), F32), pltpu.VMEM((chunks, 4, cb, 512), F32), pltpu.VMEM((chunks, chips - 1, cb, 512), F32),
                pltpu.VMEM((batch, wo.shape[1]), BF16),
                dma((6,)), dma((2, chunks)), dma((5,)), dma((5,)), dma((5,)), dma((5,)), dma((chunks,)), dma((chunks,)),
                dma((chunks, chips - 1)), dma((chunks, chips - 1)), dma((chunks,)), dma((chunks,)),
                dma((chunks, chips - 1)), dma((chunks, chips - 1)), dma((chunks, chips * CORES - 1)), dma((chunks, chips * CORES - 1))],
            compiler_params=pltpu.CompilerParams(collective_id=0, has_side_effects=True, vmem_limit_bytes=29 << 20),
            name='step',
        )(in_hbm(x), in_hbm(wq), in_hbm(wk), in_hbm(wv), in_hbm(wo), in_hbm(k3), in_hbm(v3), pos, pos2)
        ko, vo = pl.pallas_call(
            patch_kernel,
            out_shape=(pltpu.VMEM(shape4, BF16), pltpu.VMEM(shape4, BF16)),
            in_specs=[vm, vm, vm, sm],
            out_specs=[vm, vm],
            scratch_shapes=[pltpu.VMEM((4, batch * 4, 128), F32), pltpu.VMEM((2, batch * 8, 128), F32)],
            input_output_aliases={0: 0, 1: 1},
            compiler_params=pltpu.CompilerParams(vmem_limit_bytes=8 << 20),
            name='patch',
        )(in_vmem(ko.reshape(shape4)), in_vmem(vo.reshape(shape4)), new, pos)
        return y, ko, vo

    return jax.shard_map(local_step, mesh=mesh, in_specs=in_specs, out_specs=out_specs, check_vma=False)
```

```python
import functools
import math

import jax
import jax.numpy as jnp
from jax import lax
from jax.experimental import pallas as pl
from jax.experimental.pallas import tpu as pltpu
from jax.sharding import PartitionSpec as P

MESH = pl.DeviceIdType.MESH
NEG = -3.4028234e38
F32, BF16 = jnp.float32, jnp.bfloat16
CORES = 2
NT = (((1,), (1,)), ((), ()))


def step_kernel(chips, x_hbm, wq_hbm, wk_hbm, wv_hbm, wo_hbm, k_hbm, v_hbm, pos_ref,
                yfull, kout, vout, kv_all,
                x_v, wbuf, wo_v, qs, q_all, colmask, pos2_ref, oraw, mraw, lraw, om, op, orecv,
                ys, yp, yr,
                lsem, kvsem, q_ss, q_rs, n_ss, n_rs, od_s, od_r, oi_s, oi_r, yd_s, yd_r, yi_s, yi_r, ag_s, ag_r):
    batch = k_hbm.shape[0]
    local_len = k_hbm.shape[1] // 8
    chunks = om.shape[0]
    cb = batch // chunks
    half = batch // 2
    scale2 = k_hbm.shape[2] ** -0.5 * math.log2(math.e)
    rep = lax.axis_index('rep')
    me = lax.axis_index('seq')
    chip, core = me // CORES, me % CORES
    base = me * local_len
    quarter = (chip % 2) * CORES + core

    def dev(c, e):
        return (rep, lax.rem(c, chips) * CORES + e)

    partner = dev(chip, 1 - core)
    via = lax.rem(chip + 1 + core * (chips - 2), chips)
    opp = lax.rem(chip + chips - 1 - core * (chips - 2), chips)
    far = lax.rem(chip + 2, chips)

    ncols = 256
    lx = pltpu.make_async_copy(x_hbm, x_v, lsem.at[0])
    lw = [pltpu.make_async_copy(wq_hbm.at[:, pl.ds(pl.multiple_of(quarter * 1024 + i * 512, 512), 512)], wbuf.at[i], lsem.at[1 + i])
          for i in range(2)]
    lk = pltpu.make_async_copy(wk_hbm.at[:, pl.ds(pl.multiple_of(quarter * ncols, ncols), ncols)], wbuf.at[2, :, pl.ds(0, ncols)], lsem.at[3])
    lv = pltpu.make_async_copy(wv_hbm.at[:, pl.ds(pl.multiple_of(quarter * ncols, ncols), ncols)], wbuf.at[2, :, pl.ds(ncols, ncols)], lsem.at[4])
    lo = pltpu.make_async_copy(wo_hbm, wo_v, lsem.at[5])
    lkc = [pltpu.make_async_copy(k_hbm.at[pl.ds(i * cb, cb)], kout.at[pl.ds(i * cb, cb)], kvsem.at[0, i]) for i in range(chunks)]
    lvc = [pltpu.make_async_copy(v_hbm.at[pl.ds(i * cb, cb)], vout.at[pl.ds(i * cb, cb)], kvsem.at[1, i]) for i in range(chunks)]
    lx.start()
    lw[0].start()
    lw[1].start()

    barrier = pltpu.get_barrier_semaphore()
    for d in range(chips):
        for f in range(CORES):
            if d or f:
                pl.semaphore_signal(barrier, inc=1, device_id=dev(chip + d, lax.rem(core + f, CORES)), device_id_type=MESH)

    row = lax.broadcasted_iota(jnp.int32, colmask.shape, 0)
    col = lax.broadcasted_iota(jnp.int32, colmask.shape, 1)
    colmask[...] = jnp.where(col % 8 == (row // 16) * 2 + (row % 8) // 4, col, 1 << 30)

    lane_b = (lax.broadcasted_iota(jnp.int32, pos2_ref.shape, 1) + lax.broadcasted_iota(jnp.int32, pos2_ref.shape, 0) * pos2_ref.shape[1]) // 2
    pv = jnp.zeros(pos2_ref.shape, jnp.int32)
    for b in range(batch):
        pv = jnp.where(lane_b == b, pos_ref[b], pv)
    pos2_ref[...] = pv

    lx.wait()
    lk.start()
    lv.start()
    for i in range(2):
        lw[i].wait()
        if i == 0:
            lkc[0].start()
            lvc[0].start()
        q = jnp.dot(x_v[...], wbuf[i], preferred_element_type=F32)
        for h in range(4):
            qs[pl.ds(i * 4 + h, batch, stride=8), :] = q[:, h * 128:(h + 1) * 128]
    q_all[quarter] = qs[...].astype(BF16)
    pl.semaphore_wait(barrier, chips * CORES - 1)

    def spread(buf, rows, ss, rs):
        copies = [pltpu.make_async_remote_copy(buf.at[quarter], buf.at[quarter], ss.at[0], rs.at[0], device_id=partner, device_id_type=MESH)]
        for side, shift in ((0, 1), (1, chips - 1)):
            part = pl.ds(side * rows // 2, rows // 2)
            for f in range(CORES):
                e = lax.rem(core + f, CORES)
                slot = 1 + side * 2 + f
                copies.append(pltpu.make_async_remote_copy(
                    buf.at[quarter, part], buf.at[quarter, part], ss.at[slot], rs.at[slot], device_id=dev(chip + shift, e), device_id_type=MESH))
        return copies

    q_copies = spread(q_all, batch * 8, q_ss, q_rs)
    for c in q_copies:
        c.start()
    lk.wait()
    lv.wait()
    lkc[1].start()
    lvc[1].start()
    kv = jnp.dot(x_v[...], wbuf[2], preferred_element_type=F32)
    for w in range(2):
        for k in range(2):
            qs[pl.ds(w * 128 + k, batch, stride=2), :] = kv[:, w * 256 + k * 128:w * 256 + (k + 1) * 128]
    for hf in range(2):
        for w in range(2):
            kv_all[quarter, hf * 128 + w * 64:hf * 128 + w * 64 + 64, :] = qs[w * 128 + hf * 64:w * 128 + hf * 64 + 64, :].astype(BF16)
    n_copies = spread(kv_all, batch * 4, n_ss, n_rs)
    for c in n_copies:
        c.start()
    for i in range(2, chunks):
        lkc[i].start()
        lvc[i].start()
    lo.start()

    rowb = lax.broadcasted_iota(jnp.int32, (64, 128), 0) // 8 % 2
    bm0 = jnp.where(rowb == 0, 1.0, 0.0).astype(BF16)
    bm1 = jnp.where(rowb == 1, 1.0, 0.0).astype(BF16)

    for c in q_copies:
        c.wait_recv()

    def pair(pi, loc):
        q = jnp.concatenate([q_all[t, pl.ds(pl.multiple_of(pi * 16, 16), 16), :] for t in range(4)], axis=0)
        lhs = jnp.concatenate([q * bm0, q * bm1], axis=1)
        kcat = jnp.concatenate([kout[2 * pi], kout[2 * pi + 1]], axis=1)
        s = lax.dot_general(lhs, kcat, NT, preferred_element_type=F32)
        lim0 = (pos_ref[2 * pi] - base) * 8
        lim1 = (pos_ref[2 * pi + 1] - base) * 8
        lim = jnp.where(lax.broadcasted_iota(jnp.int32, (16, 1), 0) < 8, lim0, lim1)
        ps = []
        for t in range(4):
            st = jnp.where(colmask[t * 16:(t + 1) * 16, :] < lim, s[t * 16:(t + 1) * 16, :], -jnp.inf)
            m = jnp.maximum(jnp.max(st, axis=1, keepdims=True), NEG)
            p = jnp.exp2((st - m) * scale2)
            mraw[t, pl.ds(pl.multiple_of(loc * 16, 16), 16), :] = jnp.broadcast_to(m, (16, 128))
            lraw[t, pl.ds(pl.multiple_of(loc * 16, 16), 16), :] = jnp.broadcast_to(jnp.sum(p, axis=1, keepdims=True), (16, 128))
            ps.append(p.astype(BF16))
        vcat = jnp.concatenate([vout[2 * pi], vout[2 * pi + 1]], axis=1)
        o = jnp.dot(jnp.concatenate(ps, axis=0), vcat, preferred_element_type=F32)
        for t in range(4):
            for b in range(2):
                r = t * 16 + b * 8
                oraw[t, pl.ds(pl.multiple_of(loc * 16 + b * 8, 8), 8), :] = o[r:r + 8, b * 128:(b + 1) * 128]

    rows_c = cb * 8
    ppc = cb // 2

    def attend(i, sub):
        def body(j, carry):
            loc = sub * (ppc // 2) + j * 2
            pair(i * ppc + loc, loc)
            pair(i * ppc + loc + 1, loc + 1)
            return carry
        lax.fori_loop(0, ppc // 4, body, 0)

    lane = lax.broadcasted_iota(jnp.int32, (8, 128), 1)
    od, oi, yd, yi, ag = {}, {}, {}, {}, {}

    def finalize(i):
        hf = i * cb // half
        first = i * rows_c - hf * half * 8
        rr = lax.broadcasted_iota(jnp.int32, (rows_c, 64), 0) + first
        cc = lax.broadcasted_iota(jnp.int32, (rows_c, 64), 1)
        rel = pos2_ref[hf:hf + 1, :] - base
        keep = (rr // 4 == cc) & (rel >= 0) & (rel < local_len)
        for t in range(4):
            qt = q_all[t, i * rows_c:(i + 1) * rows_c, :]
            sn = lax.dot_general(qt, kv_all[t, hf * 128:hf * 128 + 64, :], NT, preferred_element_type=F32)
            sn = jnp.where(keep, sn, -jnp.inf)
            mo = mraw[t]
            mn = jnp.maximum(mo, jnp.max(sn, axis=1, keepdims=True))
            pn = jnp.exp2((sn - mn[:, :64]) * scale2)
            w = jnp.exp2((mo - mn) * scale2)
            lraw[t] = lraw[t] * w + jnp.sum(pn, axis=1, keepdims=True)
            oraw[t] = oraw[t] * w + jnp.dot(pn.astype(BF16), kv_all[t, hf * 128 + 64:hf * 128 + 128, :], preferred_element_type=F32)
            mraw[t] = mn
        for e in range(CORES):
            for t in range(4):
                mt = jnp.zeros((8, 128), F32)
                lt = jnp.zeros((8, 128), F32)
                for h in range(4):
                    src = pl.ds(e * 4 + h, cb, stride=8)
                    om[i, e, t, h * cb:(h + 1) * cb, :] = oraw[t, src, :]
                    mh = mraw[t, src, :]
                    lh = lraw[t, src, :]
                    for g in range(cb // 8):
                        sel = lane == h * (cb // 8) + g
                        mt = jnp.where(sel, mh[g * 8:(g + 1) * 8], mt)
                        lt = jnp.where(sel, lh[g * 8:(g + 1) * 8], lt)
                om[i, e, t, cb * 4:cb * 4 + 8, :] = mt
                om[i, e, t, cb * 4 + 8:cb * 4 + 16, :] = lt
        od[i] = pltpu.make_async_remote_copy(om.at[i, 1 - core], op.at[i], od_s.at[i], od_r.at[i], device_id=partner, device_id_type=MESH)
        od[i].start()

    nrow = cb * 4

    def merge(parts):
        ms = [p[nrow:nrow + 8] for p in parts]
        m = functools.reduce(jnp.maximum, ms)
        ws = [jnp.exp2((x - m) * scale2) for x in ms]
        l = functools.reduce(jnp.add, [w * p[nrow + 8:nrow + 16] for w, p in zip(ws, parts)])
        return m, l, ws

    def chip_reduce(i):
        od[i].wait_recv()
        for t in range(4):
            fold(om.at[i, core, t], om[i, core, t], op[i, t])
        relay = pltpu.make_async_remote_copy(om.at[i, core, far], orecv.at[i, 0], oi_s.at[i, 0], oi_r.at[i, 0], device_id=dev(via, core), device_id_type=MESH)
        direct = pltpu.make_async_remote_copy(om.at[i, core, opp], orecv.at[i, 1], oi_s.at[i, 1], oi_r.at[i, 1], device_id=dev(opp, core), device_id_type=MESH)
        relay.start()
        direct.start()
        oi[i] = [relay, direct]

    def fold(dst, a, b):
        m, l, (wa, wb) = merge([a, b])
        for g in range(nrow // 8):
            r = slice(g * 8, g * 8 + 8)
            dst[g * 8:g * 8 + 8, :] = a[r] * wa[:, g:g + 1] + b[r] * wb[:, g:g + 1]
        dst[nrow:nrow + 8, :] = m
        dst[nrow + 8:nrow + 16, :] = l

    def o_relay(i):
        oi[i][0].wait_recv()
        fold(om.at[i, core, via], om[i, core, via], orecv[i, 0])
        c = pltpu.make_async_remote_copy(om.at[i, core, via], orecv.at[i, 2], oi_s.at[i, 2], oi_r.at[i, 2], device_id=dev(via, core), device_id_type=MESH)
        c.start()
        oi[i].append(c)

    def project(i):
        for c in oi[i][1:]:
            c.wait_recv()
        if i == 0:
            lo.wait()
        parts = [om[i, core, chip], orecv[i, 1], orecv[i, 2]]
        m, l, ws = merge(parts)
        rl = 1.0 / l
        heads = []
        for h in range(4):
            rows = []
            for g in range(h * (cb // 8), (h + 1) * (cb // 8)):
                o = functools.reduce(jnp.add, [p[g * 8:g * 8 + 8] * w[:, g:g + 1] for p, w in zip(parts, ws)])
                rows.append(o * rl[:, g:g + 1])
            heads.append(jnp.concatenate(rows, axis=0).astype(BF16))
        lhs = jnp.concatenate(heads, axis=1)
        for e in range(CORES):
            for t in range(4):
                c0 = (e * 4 + t) * 512
                ys[i, e, t] = jnp.dot(lhs, wo_v[:, c0:c0 + 512], preferred_element_type=F32)
        yd[i] = pltpu.make_async_remote_copy(ys.at[i, 1 - core], yp.at[i], yd_s.at[i], yd_r.at[i], device_id=partner, device_id_type=MESH)
        yd[i].start()

    def y_chip(i):
        yd[i].wait_recv()
        ys[i, core] = ys[i, core] + yp[i]
        relay = pltpu.make_async_remote_copy(ys.at[i, core, far], yr.at[i, 0], yi_s.at[i, 0], yi_r.at[i, 0], device_id=dev(via, core), device_id_type=MESH)
        direct = pltpu.make_async_remote_copy(ys.at[i, core, opp], yr.at[i, 1], yi_s.at[i, 1], yi_r.at[i, 1], device_id=dev(opp, core), device_id_type=MESH)
        relay.start()
        direct.start()
        yi[i] = [relay, direct]

    def y_relay(i):
        yi[i][0].wait_recv()
        ys[i, core, via] = ys[i, core, via] + yr[i, 0]
        c = pltpu.make_async_remote_copy(ys.at[i, core, via], yr.at[i, 2], yi_s.at[i, 2], yi_r.at[i, 2], device_id=dev(via, core), device_id_type=MESH)
        c.start()
        yi[i].append(c)

    def block(i, c):
        return (pl.ds(i * cb, cb), pl.ds(pl.multiple_of((core * 4 + c) * 512, 512), 512))

    def push(i, c, slot, target):
        cp = pltpu.make_async_remote_copy(yfull.at[block(i, c)], yfull.at[block(i, c)], ag_s.at[i, slot], ag_r.at[i, slot],
                                          device_id=target, device_id_type=MESH)
        cp.start()
        ag[i].append(cp)

    def y_final(i):
        for c in yi[i][1:]:
            c.wait_recv()
        yfull[block(i, chip)] = (ys[i, core, chip] + yr[i, 1] + yr[i, 2]).astype(BF16)
        ag[i] = []
        push(i, chip, 0, dev(via, core))
        push(i, chip, 1, dev(opp, core))
        push(i, chip, 2, partner)

    def ag_relay(i):
        ag[i][0].wait_recv()
        push(i, opp, 3, dev(via, core))
        push(i, opp, 4, partner)
        ag[i][1].wait_recv()
        push(i, via, 5, partner)

    def ag_last(i):
        ag[i][3].wait_recv()
        push(i, far, 6, partner)

    stages = ((finalize, 1), (chip_reduce, 2), (o_relay, 4), (project, 6), (y_chip, 7), (y_relay, 9), (y_final, 11), (ag_relay, 13), (ag_last, 15))
    for k in range(2 * chunks + 14):
        if k < 2 * chunks:
            if k % 2 == 0:
                lkc[k // 2].wait()
                lvc[k // 2].wait()
            attend(k // 2, k % 2)
        if k == 1:
            for c in n_copies:
                c.wait_recv()
        for stage, lag in stages:
            i = (k - lag) // 2
            if (k - lag) % 2 == 0 and 0 <= i < chunks:
                stage(i)
    for i in range(chunks):
        for slot in (2, 4, 5, 6):
            ag[i][slot].wait_recv()
    for c in q_copies + n_copies:
        c.wait_send()
    for i in range(chunks):
        for c in [od[i], yd[i]] + oi[i] + yi[i] + ag[i]:
            c.wait_send()


def write_kernel(which, k_in, new_ref, pos_ref, k_out, k_ref, src, dst, bsem):
    batch, local_len = k_ref.shape[0], k_ref.shape[1] // 8
    base = lax.axis_index('seq') * local_len
    hb = batch // 2
    pieces = bsem.shape[0]
    pb = batch // pieces
    for t in range(4):
        for hf in range(2):
            src[t, hf * hb * 2:(hf + 1) * hb * 2, :] = new_ref[t, hf * 128 + which * 64:hf * 128 + which * 64 + 64, :].astype(F32)
    for t in range(4):
        for k in range(2):
            dst[pl.ds(t * 2 + k, batch, stride=8), :] = src[t, pl.ds(k, batch, stride=2), :]
    bulk = []
    for i in range(pieces):
        @pl.loop(i * pb, (i + 1) * pb)
        def _(b):
            rel = pos_ref[b] - base

            @pl.when((rel >= 0) & (rel < local_len))
            def _():
                k_ref[b, pl.ds(pl.multiple_of(rel * 8, 8), 8), :] = dst[pl.ds(pl.multiple_of(b * 8, 8), 8), :].astype(BF16)
        part = pl.ds(i * pb, pb)
        c = pltpu.make_async_copy(k_ref.at[part], k_out.at[part], bsem.at[i])
        c.start()
        bulk.append(c)
    for c in bulk:
        c.wait()


def solution(mesh):
    cache_spec = P('rep', 'seq', None, None)
    in_specs = (P('rep', None), P(), P(), P(), P('seq', None), cache_spec, cache_spec, P('rep'))
    out_specs = (P('rep', None), cache_spec, cache_spec)
    chips = mesh.shape['seq'] // CORES
    assert chips == 4
    vm = pl.BlockSpec(memory_space=pltpu.VMEM)
    hbm = pl.BlockSpec(memory_space=pl.ANY)
    sm = pl.BlockSpec(memory_space=pltpu.SMEM)

    def local_step(x, wq, wk, wv, wo, k, v, pos):
        shape4 = k.shape
        batch, width = x.shape
        k3 = k.reshape(batch, -1, k.shape[-1])
        v3 = v.reshape(k3.shape)
        chunks = 4
        cb = batch // chunks
        dma = pltpu.SemaphoreType.DMA
        in_hbm = lambda a: pltpu.with_memory_space_constraint(a, pltpu.HBM)
        in_vmem = lambda a: pltpu.with_memory_space_constraint(a, pltpu.VMEM)
        y, ko, vo, new = pl.pallas_call(
            functools.partial(step_kernel, chips),
            out_shape=(pltpu.VMEM((batch, wo.shape[1]), BF16), pltpu.VMEM(k3.shape, BF16), pltpu.VMEM(k3.shape, BF16),
                       pltpu.VMEM((4, batch * 4, 128), BF16)),
            in_specs=[hbm] * 7 + [sm],
            out_specs=[vm] * 4,
            scratch_shapes=[
                pltpu.VMEM((batch, width), BF16), pltpu.VMEM((3, width, 512), BF16), pltpu.VMEM(wo.shape, BF16),
                pltpu.VMEM((batch * 8, 128), F32), pltpu.VMEM((4, batch * 8, 128), BF16), pltpu.VMEM((64, k3.shape[1]), jnp.int32), pltpu.VMEM((2, batch), jnp.int32),
                pltpu.VMEM((4, cb * 8, 128), F32), pltpu.VMEM((4, cb * 8, 128), F32), pltpu.VMEM((4, cb * 8, 128), F32),
                pltpu.VMEM((chunks, CORES, 4, cb * 4 + 16, 128), F32), pltpu.VMEM((chunks, 4, cb * 4 + 16, 128), F32),
                pltpu.VMEM((chunks, chips - 1, cb * 4 + 16, 128), F32),
                pltpu.VMEM((chunks, CORES, 4, cb, 512), F32), pltpu.VMEM((chunks, 4, cb, 512), F32), pltpu.VMEM((chunks, chips - 1, cb, 512), F32),
                dma((6,)), dma((2, chunks)), dma((5,)), dma((5,)), dma((5,)), dma((5,)), dma((chunks,)), dma((chunks,)),
                dma((chunks, chips - 1)), dma((chunks, chips - 1)), dma((chunks,)), dma((chunks,)),
                dma((chunks, chips - 1)), dma((chunks, chips - 1)), dma((chunks, chips * CORES - 1)), dma((chunks, chips * CORES - 1))],
            compiler_params=pltpu.CompilerParams(collective_id=0, has_side_effects=True, vmem_limit_bytes=29 << 20),
            name='step',
        )(in_hbm(x), in_hbm(wq), in_hbm(wk), in_hbm(wv), in_hbm(wo), in_hbm(k3), in_hbm(v3), pos)
        pieces = 8

        def write(which, cache, last):
            return pl.pallas_call(
                functools.partial(write_kernel, which),
                out_shape=(jax.ShapeDtypeStruct(k3.shape, BF16), pltpu.VMEM(k3.shape, BF16)),
                in_specs=[vm, vm, sm],
                out_specs=[hbm, vm],
                scratch_shapes=[pltpu.VMEM((4, batch * 2, 128), F32), pltpu.VMEM((batch * 8, 128), F32), dma((pieces,))],
                input_output_aliases={0: 1},
                compiler_params=pltpu.CompilerParams(vmem_limit_bytes=8 << 20),
                name='write',
            )(in_vmem(cache), in_vmem(new), pos)[0].reshape(shape4)
        ko, vo = write(0, ko, False), write(1, vo, True)
        return y, ko, vo

    return jax.shard_map(local_step, mesh=mesh, in_specs=in_specs, out_specs=out_specs, check_vma=False)
```

```python
import functools
import math

import jax
import jax.numpy as jnp
from jax import lax
from jax.experimental import pallas as pl
from jax.experimental.pallas import tpu as pltpu
from jax.sharding import PartitionSpec as P

MESH = pl.DeviceIdType.MESH
NEG = -3.4028234e38
F32, BF16 = jnp.float32, jnp.bfloat16
CORES = 2
NT = (((1,), (1,)), ((), ()))


def step_kernel(chips, x_hbm, wq_hbm, wk_hbm, wv_hbm, wo_hbm, k_hbm, v_hbm, pos_ref,
                yfull, kout, vout, kv_all,
                x_v, wbuf, wo_v, qs, q_all, colmask, pos2_ref, oraw, mraw, lraw, om, op, orecv,
                ys, yp, yr,
                lsem, kvsem, q_ss, q_rs, n_ss, n_rs, od_s, od_r, oi_s, oi_r, yd_s, yd_r, yi_s, yi_r, ag_s, ag_r):
    batch = k_hbm.shape[0]
    local_len = k_hbm.shape[1] // 8
    chunks = om.shape[0]
    straight = range(1, chunks)
    cb = batch // chunks
    half = batch // 2
    scale2 = k_hbm.shape[2] ** -0.5 * math.log2(math.e)
    rep = lax.axis_index('rep')
    me = lax.axis_index('seq')
    chip, core = me // CORES, me % CORES
    base = me * local_len
    quarter = (chip % 2) * CORES + core

    def dev(c, e):
        return (rep, lax.rem(c, chips) * CORES + e)

    partner = dev(chip, 1 - core)
    via = lax.rem(chip + 1 + core * (chips - 2), chips)
    opp = lax.rem(chip + chips - 1 - core * (chips - 2), chips)
    far = lax.rem(chip + 2, chips)

    ncols = 256
    lx = pltpu.make_async_copy(x_hbm, x_v, lsem.at[0])
    lw = [pltpu.make_async_copy(wq_hbm.at[:, pl.ds(pl.multiple_of(quarter * 1024 + i * 512, 512), 512)], wbuf.at[i], lsem.at[1 + i])
          for i in range(2)]
    lk = pltpu.make_async_copy(wk_hbm.at[:, pl.ds(pl.multiple_of(quarter * ncols, ncols), ncols)], wbuf.at[2, :, pl.ds(0, ncols)], lsem.at[3])
    lv = pltpu.make_async_copy(wv_hbm.at[:, pl.ds(pl.multiple_of(quarter * ncols, ncols), ncols)], wbuf.at[2, :, pl.ds(ncols, ncols)], lsem.at[4])
    lo = pltpu.make_async_copy(wo_hbm, wo_v, lsem.at[5])
    lkc = [pltpu.make_async_copy(k_hbm.at[pl.ds(i * cb, cb)], kout.at[pl.ds(i * cb, cb)], kvsem.at[0, i]) for i in range(chunks)]
    lvc = [pltpu.make_async_copy(v_hbm.at[pl.ds(i * cb, cb)], vout.at[pl.ds(i * cb, cb)], kvsem.at[1, i]) for i in range(chunks)]
    lx.start()
    lw[0].start()
    lw[1].start()

    barrier = pltpu.get_barrier_semaphore()
    for d in range(chips):
        for f in range(CORES):
            if d or f:
                pl.semaphore_signal(barrier, inc=1, device_id=dev(chip + d, lax.rem(core + f, CORES)), device_id_type=MESH)

    row = lax.broadcasted_iota(jnp.int32, colmask.shape, 0)
    col = lax.broadcasted_iota(jnp.int32, colmask.shape, 1)
    colmask[...] = jnp.where(col % 8 == (row // 16) * 2 + (row % 8) // 4, col, 1 << 30)

    lane_b = (lax.broadcasted_iota(jnp.int32, pos2_ref.shape, 1) + lax.broadcasted_iota(jnp.int32, pos2_ref.shape, 0) * pos2_ref.shape[1]) // 2
    pv = jnp.zeros(pos2_ref.shape, jnp.int32)
    for b in range(batch):
        pv = jnp.where(lane_b == b, pos_ref[b], pv)
    pos2_ref[...] = pv

    lx.wait()
    lk.start()
    lv.start()
    for i in range(2):
        lw[i].wait()
        if i == 0:
            lkc[0].start()
            lvc[0].start()
        q = jnp.dot(x_v[...], wbuf[i], preferred_element_type=F32)
        for h in range(4):
            qs[pl.ds(i * 4 + h, batch, stride=8), :] = q[:, h * 128:(h + 1) * 128]
    q_all[quarter] = qs[...].astype(BF16)
    pl.semaphore_wait(barrier, chips * CORES - 1)

    def spread(buf, rows, ss, rs):
        copies = [pltpu.make_async_remote_copy(buf.at[quarter], buf.at[quarter], ss.at[0], rs.at[0], device_id=partner, device_id_type=MESH)]
        for side, shift in ((0, 1), (1, chips - 1)):
            part = pl.ds(side * rows // 2, rows // 2)
            copies.append(pltpu.make_async_remote_copy(
                buf.at[quarter, part], buf.at[quarter, part], ss.at[1 + side], rs.at[1 + side], device_id=dev(chip + shift, core), device_id_type=MESH))
        return copies

    def hand_on(copies, buf, rows, ss, rs):
        other = ((chip + 1) % 2) * CORES + core
        for side in range(2):
            copies[1 + side].wait_recv()
            part = pl.ds(side * rows // 2, rows // 2)
            c = pltpu.make_async_remote_copy(buf.at[other, part], buf.at[other, part], ss.at[3 + side], rs.at[3 + side], device_id=partner, device_id_type=MESH)
            c.start()
            copies.append(c)

    def arrive(copies):
        copies[0].wait_recv()
        copies[3].wait_recv()
        copies[4].wait_recv()

    q_copies = spread(q_all, batch * 8, q_ss, q_rs)
    for c in q_copies:
        c.start()
    lk.wait()
    lv.wait()
    lkc[1].start()
    lvc[1].start()
    kv = jnp.dot(x_v[...], wbuf[2], preferred_element_type=F32)
    for w in range(2):
        for k in range(2):
            qs[pl.ds(w * 128 + k, batch, stride=2), :] = kv[:, w * 256 + k * 128:w * 256 + (k + 1) * 128]
    for hf in range(2):
        for w in range(2):
            kv_all[quarter, hf * 128 + w * 64:hf * 128 + w * 64 + 64, :] = qs[w * 128 + hf * 64:w * 128 + hf * 64 + 64, :].astype(BF16)
    n_copies = spread(kv_all, batch * 4, n_ss, n_rs)
    for c in n_copies:
        c.start()
    for i in range(2, chunks):
        lkc[i].start()
        lvc[i].start()
    lo.start()

    rowb = lax.broadcasted_iota(jnp.int32, (64, 128), 0) // 8 % 2
    bm0 = jnp.where(rowb == 0, 1.0, 0.0).astype(BF16)
    bm1 = jnp.where(rowb == 1, 1.0, 0.0).astype(BF16)

    hand_on(q_copies, q_all, batch * 8, q_ss, q_rs)
    hand_on(n_copies, kv_all, batch * 4, n_ss, n_rs)
    arrive(q_copies)

    def pair(pi, loc):
        q = jnp.concatenate([q_all[t, pl.ds(pl.multiple_of(pi * 16, 16), 16), :] for t in range(4)], axis=0)
        lhs = jnp.concatenate([q * bm0, q * bm1], axis=1)
        kcat = jnp.concatenate([kout[2 * pi], kout[2 * pi + 1]], axis=1)
        s = lax.dot_general(lhs, kcat, NT, preferred_element_type=F32)
        lim0 = (pos_ref[2 * pi] - base) * 8
        lim1 = (pos_ref[2 * pi + 1] - base) * 8
        lim = jnp.where(lax.broadcasted_iota(jnp.int32, (16, 1), 0) < 8, lim0, lim1)
        ps = []
        for t in range(4):
            st = jnp.where(colmask[t * 16:(t + 1) * 16, :] < lim, s[t * 16:(t + 1) * 16, :], -jnp.inf)
            m = jnp.maximum(jnp.max(st, axis=1, keepdims=True), NEG)
            p = jnp.exp2((st - m) * scale2)
            mraw[t, pl.ds(pl.multiple_of(loc * 16, 16), 16), :] = jnp.broadcast_to(m, (16, 128))
            lraw[t, pl.ds(pl.multiple_of(loc * 16, 16), 16), :] = jnp.broadcast_to(jnp.sum(p, axis=1, keepdims=True), (16, 128))
            ps.append(p.astype(BF16))
        vcat = jnp.concatenate([vout[2 * pi], vout[2 * pi + 1]], axis=1)
        o = jnp.dot(jnp.concatenate(ps, axis=0), vcat, preferred_element_type=F32)
        for t in range(4):
            for b in range(2):
                r = t * 16 + b * 8
                oraw[t, pl.ds(pl.multiple_of(loc * 16 + b * 8, 8), 8), :] = o[r:r + 8, b * 128:(b + 1) * 128]

    rows_c = cb * 8
    ppc = cb // 2

    def attend(i, sub):
        def body(j, carry):
            loc = sub * (ppc // 2) + j * 2
            pair(i * ppc + loc, loc)
            pair(i * ppc + loc + 1, loc + 1)
            return carry
        lax.fori_loop(0, ppc // 4, body, 0)

    lane = lax.broadcasted_iota(jnp.int32, (8, 128), 1)
    od, oi, yd, yi, ag = {}, {}, {}, {}, {}

    def finalize(i):
        hf = i * cb // half
        first = i * rows_c - hf * half * 8
        rr = lax.broadcasted_iota(jnp.int32, (rows_c, 64), 0) + first
        cc = lax.broadcasted_iota(jnp.int32, (rows_c, 64), 1)
        rel = pos2_ref[hf:hf + 1, :] - base
        keep = (rr // 4 == cc) & (rel >= 0) & (rel < local_len)
        for t in range(4):
            qt = q_all[t, i * rows_c:(i + 1) * rows_c, :]
            sn = lax.dot_general(qt, kv_all[t, hf * 128:hf * 128 + 64, :], NT, preferred_element_type=F32)
            sn = jnp.where(keep, sn, -jnp.inf)
            mo = mraw[t]
            mn = jnp.maximum(mo, jnp.max(sn, axis=1, keepdims=True))
            pn = jnp.exp2((sn - mn[:, :64]) * scale2)
            w = jnp.exp2((mo - mn) * scale2)
            lraw[t] = lraw[t] * w + jnp.sum(pn, axis=1, keepdims=True)
            oraw[t] = oraw[t] * w + jnp.dot(pn.astype(BF16), kv_all[t, hf * 128 + 64:hf * 128 + 128, :], preferred_element_type=F32)
            mraw[t] = mn
        for e in range(CORES):
            for t in range(4):
                mt = jnp.zeros((8, 128), F32)
                lt = jnp.zeros((8, 128), F32)
                for h in range(4):
                    src = pl.ds(e * 4 + h, cb, stride=8)
                    om[i, e, t, h * cb:(h + 1) * cb, :] = oraw[t, src, :]
                    mh = mraw[t, src, :]
                    lh = lraw[t, src, :]
                    for g in range(cb // 8):
                        sel = lane == h * (cb // 8) + g
                        mt = jnp.where(sel, mh[g * 8:(g + 1) * 8], mt)
                        lt = jnp.where(sel, lh[g * 8:(g + 1) * 8], lt)
                om[i, e, t, cb * 4:cb * 4 + 8, :] = mt
                om[i, e, t, cb * 4 + 8:cb * 4 + 16, :] = lt
        od[i] = pltpu.make_async_remote_copy(om.at[i, 1 - core], op.at[i], od_s.at[i], od_r.at[i], device_id=partner, device_id_type=MESH)
        od[i].start()

    nrow = cb * 4

    def merge(parts):
        ms = [p[nrow:nrow + 8] for p in parts]
        m = functools.reduce(jnp.maximum, ms)
        ws = [jnp.exp2((x - m) * scale2) for x in ms]
        l = functools.reduce(jnp.add, [w * p[nrow + 8:nrow + 16] for w, p in zip(ws, parts)])
        return m, l, ws

    def chip_reduce(i):
        od[i].wait_recv()
        for t in range(4):
            fold(om.at[i, core, t], om[i, core, t], op[i, t])
        if i in straight:
            oi[i] = [None]
            for d in range(1, chips):
                c = pltpu.make_async_remote_copy(om.at[i, core, lax.rem(chip + d, chips)], orecv.at[i, d - 1], oi_s.at[i, d - 1], oi_r.at[i, d - 1],
                                                 device_id=dev(chip + d, core), device_id_type=MESH)
                c.start()
                oi[i].append(c)
            return
        relay = pltpu.make_async_remote_copy(om.at[i, core, far], orecv.at[i, 0], oi_s.at[i, 0], oi_r.at[i, 0], device_id=dev(via, core), device_id_type=MESH)
        direct = pltpu.make_async_remote_copy(om.at[i, core, opp], orecv.at[i, 1], oi_s.at[i, 1], oi_r.at[i, 1], device_id=dev(opp, core), device_id_type=MESH)
        relay.start()
        direct.start()
        oi[i] = [relay, direct]

    def fold(dst, a, b):
        m, l, (wa, wb) = merge([a, b])
        for g in range(nrow // 8):
            r = slice(g * 8, g * 8 + 8)
            dst[g * 8:g * 8 + 8, :] = a[r] * wa[:, g:g + 1] + b[r] * wb[:, g:g + 1]
        dst[nrow:nrow + 8, :] = m
        dst[nrow + 8:nrow + 16, :] = l

    def o_relay(i):
        oi[i][0].wait_recv()
        fold(om.at[i, core, via], om[i, core, via], orecv[i, 0])
        c = pltpu.make_async_remote_copy(om.at[i, core, via], orecv.at[i, 2], oi_s.at[i, 2], oi_r.at[i, 2], device_id=dev(via, core), device_id_type=MESH)
        c.start()
        oi[i].append(c)

    def project(i):
        for c in oi[i][1:]:
            c.wait_recv()
        if i == 0:
            lo.wait()
        parts = [om[i, core, chip]] + [orecv[i, d] for d in range(0 if i in straight else 1, chips - 1)]
        m, l, ws = merge(parts)
        rl = 1.0 / l
        heads = []
        for h in range(4):
            rows = []
            for g in range(h * (cb // 8), (h + 1) * (cb // 8)):
                o = functools.reduce(jnp.add, [p[g * 8:g * 8 + 8] * w[:, g:g + 1] for p, w in zip(parts, ws)])
                rows.append(o * rl[:, g:g + 1])
            heads.append(jnp.concatenate(rows, axis=0).astype(BF16))
        lhs = jnp.concatenate(heads, axis=1)
        for e in range(CORES):
            for t in range(4):
                c0 = (e * 4 + t) * 512
                ys[i, e, t] = jnp.dot(lhs, wo_v[:, c0:c0 + 512], preferred_element_type=F32)
        yd[i] = pltpu.make_async_remote_copy(ys.at[i, 1 - core], yp.at[i], yd_s.at[i], yd_r.at[i], device_id=partner, device_id_type=MESH)
        yd[i].start()

    def y_chip(i):
        yd[i].wait_recv()
        ys[i, core] = ys[i, core] + yp[i]
        if i in straight:
            yi[i] = [None]
            for d in range(1, chips):
                c = pltpu.make_async_remote_copy(ys.at[i, core, lax.rem(chip + d, chips)], yr.at[i, d - 1], yi_s.at[i, d - 1], yi_r.at[i, d - 1],
                                                 device_id=dev(chip + d, core), device_id_type=MESH)
                c.start()
                yi[i].append(c)
            return
        relay = pltpu.make_async_remote_copy(ys.at[i, core, far], yr.at[i, 0], yi_s.at[i, 0], yi_r.at[i, 0], device_id=dev(via, core), device_id_type=MESH)
        direct = pltpu.make_async_remote_copy(ys.at[i, core, opp], yr.at[i, 1], yi_s.at[i, 1], yi_r.at[i, 1], device_id=dev(opp, core), device_id_type=MESH)
        relay.start()
        direct.start()
        yi[i] = [relay, direct]

    def y_relay(i):
        yi[i][0].wait_recv()
        ys[i, core, via] = ys[i, core, via] + yr[i, 0]
        c = pltpu.make_async_remote_copy(ys.at[i, core, via], yr.at[i, 2], yi_s.at[i, 2], yi_r.at[i, 2], device_id=dev(via, core), device_id_type=MESH)
        c.start()
        yi[i].append(c)

    def block(i, c):
        return (pl.ds(i * cb, cb), pl.ds(pl.multiple_of((core * 4 + c) * 512, 512), 512))

    def y_final(i):
        for c in yi[i][1:]:
            c.wait_recv()
        y = ys[i, core, chip]
        for d in range(0 if i in straight else 1, chips - 1):
            y = y + yr[i, d]
        own = block(i, chip)
        yfull[own] = y.astype(BF16)
        ag[i] = []
        for d in range(chips):
            for f in range(CORES):
                if d or f:
                    slot = d * CORES + f - 1
                    c = pltpu.make_async_remote_copy(yfull.at[own], yfull.at[own], ag_s.at[i, slot], ag_r.at[i, slot],
                                                     device_id=dev(chip + d, lax.rem(core + f, CORES)), device_id_type=MESH)
                    c.start()
                    ag[i].append(c)

    relayed = ((finalize, 1), (chip_reduce, 2), (o_relay, 4), (project, 6), (y_chip, 7), (y_relay, 8), (y_final, 9))
    direct_early = ((finalize, 1), (chip_reduce, 2), (project, 4), (y_chip, 5), (y_final, 7))
    direct_late = ((finalize, 1), (chip_reduce, 2), (project, 3), (y_chip, 4), (y_final, 5))
    plan = {}
    for i in range(chunks):
        for stage, lag in direct_late if i >= chunks - 2 else direct_early if i in straight else relayed:
            plan.setdefault(2 * i + lag, []).append((stage, i))
    for k in range(max(plan) + 1):
        if k < 2 * chunks:
            if k % 2 == 0:
                lkc[k // 2].wait()
                lvc[k // 2].wait()
            attend(k // 2, k % 2)
        if k == 1:
            arrive(n_copies)
        for stage, i in plan.get(k, ()):
            stage(i)
    for i in range(chunks):
        for c in ag[i]:
            c.wait_recv()
    for c in q_copies + n_copies:
        c.wait_send()
    for i in range(chunks):
        for c in [od[i], yd[i]] + oi[i] + yi[i] + ag[i]:
            if c is not None:
                c.wait_send()


def write_kernel(which, k_in, new_ref, pos_ref, *refs):
    if which == 0:
        y_ref, k_out, k_ref, y_out, src, dst, bsem, ysem = refs
        cy = pltpu.make_async_copy(y_ref, y_out, ysem)
    else:
        k_out, k_ref, src, dst, bsem, ysem = refs
    batch, local_len = k_ref.shape[0], k_ref.shape[1] // 8
    base = lax.axis_index('seq') * local_len
    hb = batch // 2
    pieces = bsem.shape[0]
    pb = batch // pieces
    for t in range(4):
        for hf in range(2):
            src[t, hf * hb * 2:(hf + 1) * hb * 2, :] = new_ref[t, hf * 128 + which * 64:hf * 128 + which * 64 + 64, :].astype(F32)
    for t in range(4):
        for k in range(2):
            dst[pl.ds(t * 2 + k, batch, stride=8), :] = src[t, pl.ds(k, batch, stride=2), :]
    bulk = []
    for i in range(pieces):
        @pl.loop(i * pb, (i + 1) * pb)
        def _(b):
            rel = pos_ref[b] - base

            @pl.when((rel >= 0) & (rel < local_len))
            def _():
                k_ref[b, pl.ds(pl.multiple_of(rel * 8, 8), 8), :] = dst[pl.ds(pl.multiple_of(b * 8, 8), 8), :].astype(BF16)
        part = pl.ds(i * pb, pb)
        c = pltpu.make_async_copy(k_ref.at[part], k_out.at[part], bsem.at[i])
        c.start()
        bulk.append(c)
    if which == 0:
        cy.start()
        bulk.append(cy)
    for c in bulk:
        c.wait()


def solution(mesh):
    cache_spec = P('rep', 'seq', None, None)
    in_specs = (P('rep', None), P(), P(), P(), P('seq', None), cache_spec, cache_spec, P('rep'))
    out_specs = (P('rep', None), cache_spec, cache_spec)
    chips = mesh.shape['seq'] // CORES
    assert chips == 4
    vm = pl.BlockSpec(memory_space=pltpu.VMEM)
    hbm = pl.BlockSpec(memory_space=pl.ANY)
    sm = pl.BlockSpec(memory_space=pltpu.SMEM)

    def local_step(x, wq, wk, wv, wo, k, v, pos):
        shape4 = k.shape
        batch, width = x.shape
        k3 = k.reshape(batch, -1, k.shape[-1])
        v3 = v.reshape(k3.shape)
        chunks = 4
        cb = batch // chunks
        dma = pltpu.SemaphoreType.DMA
        in_hbm = lambda a: pltpu.with_memory_space_constraint(a, pltpu.HBM)
        in_vmem = lambda a: pltpu.with_memory_space_constraint(a, pltpu.VMEM)
        y, ko, vo, new = pl.pallas_call(
            functools.partial(step_kernel, chips),
            out_shape=(pltpu.VMEM((batch, wo.shape[1]), BF16), pltpu.VMEM(k3.shape, BF16), pltpu.VMEM(k3.shape, BF16),
                       pltpu.VMEM((4, batch * 4, 128), BF16)),
            in_specs=[hbm] * 7 + [sm],
            out_specs=[vm] * 4,
            scratch_shapes=[
                pltpu.VMEM((batch, width), BF16), pltpu.VMEM((3, width, 512), BF16), pltpu.VMEM(wo.shape, BF16),
                pltpu.VMEM((batch * 8, 128), F32), pltpu.VMEM((4, batch * 8, 128), BF16), pltpu.VMEM((64, k3.shape[1]), jnp.int32), pltpu.VMEM((2, batch), jnp.int32),
                pltpu.VMEM((4, cb * 8, 128), F32), pltpu.VMEM((4, cb * 8, 128), F32), pltpu.VMEM((4, cb * 8, 128), F32),
                pltpu.VMEM((chunks, CORES, 4, cb * 4 + 16, 128), F32), pltpu.VMEM((chunks, 4, cb * 4 + 16, 128), F32),
                pltpu.VMEM((chunks, chips - 1, cb * 4 + 16, 128), F32),
                pltpu.VMEM((chunks, CORES, 4, cb, 512), F32), pltpu.VMEM((chunks, 4, cb, 512), F32), pltpu.VMEM((chunks, chips - 1, cb, 512), F32),
                dma((6,)), dma((2, chunks)), dma((5,)), dma((5,)), dma((5,)), dma((5,)), dma((chunks,)), dma((chunks,)),
                dma((chunks, chips - 1)), dma((chunks, chips - 1)), dma((chunks,)), dma((chunks,)),
                dma((chunks, chips - 1)), dma((chunks, chips - 1)), dma((chunks, chips * CORES - 1)), dma((chunks, chips * CORES - 1))],
            compiler_params=pltpu.CompilerParams(collective_id=0, has_side_effects=True, vmem_limit_bytes=29 << 20),
            name='step',
        )(in_hbm(x), in_hbm(wq), in_hbm(wk), in_hbm(wv), in_hbm(wo), in_hbm(k3), in_hbm(v3), pos)
        pieces = 8

        def write(which, cache, *extra):
            return pl.pallas_call(
                functools.partial(write_kernel, which),
                out_shape=(jax.ShapeDtypeStruct(k3.shape, BF16), pltpu.VMEM(k3.shape, BF16), *(jax.ShapeDtypeStruct(e.shape, BF16) for e in extra)),
                in_specs=[vm, vm, sm] + [vm] * len(extra),
                out_specs=[hbm, vm] + [hbm] * len(extra),
                scratch_shapes=[pltpu.VMEM((4, batch * 2, 128), F32), pltpu.VMEM((batch * 8, 128), F32), dma((pieces,)), dma],
                input_output_aliases={0: 1},
                compiler_params=pltpu.CompilerParams(vmem_limit_bytes=8 << 20),
                name='write',
            )(in_vmem(cache), in_vmem(new), pos, *(in_vmem(e) for e in extra))
        ko, _, y = write(0, ko, y)
        vo, _ = write(1, vo)
        return y, ko.reshape(shape4), vo.reshape(shape4)

    return jax.shard_map(local_step, mesh=mesh, in_specs=in_specs, out_specs=out_specs, check_vma=False)
```

```python
import functools
import math

import jax
import jax.numpy as jnp
from jax import lax
from jax.experimental import pallas as pl
from jax.experimental.pallas import tpu as pltpu
from jax.sharding import PartitionSpec as P

MESH = pl.DeviceIdType.MESH
NEG = -3.4028234e38
F32, BF16 = jnp.float32, jnp.bfloat16
CORES = 2
NT = (((1,), (1,)), ((), ()))


def step_kernel(chips, x_hbm, wq_hbm, wk_hbm, wv_hbm, wo_hbm, k_hbm, v_hbm, pos_ref,
                yfull, kout, vout, kv_all,
                x_v, wbuf, wo_v, qs, q_all, sa, sb, mt_ref, pos2_ref, oraw, mraw, lraw, om, op, orecv,
                ys, yp, yr,
                lsem, kvsem, q_ss, q_rs, n_ss, n_rs, od_s, od_r, oi_s, oi_r, yd_s, yd_r, yi_s, yi_r, ag_s, ag_r):
    batch = k_hbm.shape[0]
    local_len = k_hbm.shape[1] // 8
    chunks = om.shape[0]
    straight = range(1, chunks)
    cb = batch // chunks
    half = batch // 2
    scale2 = k_hbm.shape[2] ** -0.5 * math.log2(math.e)
    rep = lax.axis_index('rep')
    me = lax.axis_index('seq')
    chip, core = me // CORES, me % CORES
    base = me * local_len
    quarter = (chip % 2) * CORES + core

    def dev(c, e):
        return (rep, lax.rem(c, chips) * CORES + e)

    partner = dev(chip, 1 - core)
    via = lax.rem(chip + 1 + core * (chips - 2), chips)
    opp = lax.rem(chip + chips - 1 - core * (chips - 2), chips)
    far = lax.rem(chip + 2, chips)

    ncols = 256
    lx = pltpu.make_async_copy(x_hbm, x_v, lsem.at[0])
    lw = [pltpu.make_async_copy(wq_hbm.at[:, pl.ds(pl.multiple_of(quarter * 1024 + i * 512, 512), 512)], wbuf.at[i], lsem.at[1 + i])
          for i in range(2)]
    lk = pltpu.make_async_copy(wk_hbm.at[:, pl.ds(pl.multiple_of(quarter * ncols, ncols), ncols)], wbuf.at[2, :, pl.ds(0, ncols)], lsem.at[3])
    lv = pltpu.make_async_copy(wv_hbm.at[:, pl.ds(pl.multiple_of(quarter * ncols, ncols), ncols)], wbuf.at[2, :, pl.ds(ncols, ncols)], lsem.at[4])
    lo = pltpu.make_async_copy(wo_hbm, wo_v, lsem.at[5])
    lkc = [pltpu.make_async_copy(k_hbm.at[pl.ds(i * cb, cb)], kout.at[pl.ds(i * cb, cb)], kvsem.at[0, i]) for i in range(chunks)]
    lvc = [pltpu.make_async_copy(v_hbm.at[pl.ds(i * cb, cb)], vout.at[pl.ds(i * cb, cb)], kvsem.at[1, i]) for i in range(chunks)]
    lx.start()
    lw[0].start()
    lw[1].start()

    barrier = pltpu.get_barrier_semaphore()
    for d in range(chips):
        for f in range(CORES):
            if d or f:
                pl.semaphore_signal(barrier, inc=1, device_id=dev(chip + d, lax.rem(core + f, CORES)), device_id_type=MESH)

    lane_b = (lax.broadcasted_iota(jnp.int32, pos2_ref.shape, 1) + lax.broadcasted_iota(jnp.int32, pos2_ref.shape, 0) * pos2_ref.shape[1]) // 2
    pv = jnp.zeros(pos2_ref.shape, jnp.int32)
    for b in range(batch):
        pv = jnp.where(lane_b == b, pos_ref[b], pv)
    pos2_ref[...] = pv

    with jax.named_scope('xwait'):
        lx.wait()
    lk.start()
    lv.start()
    for i in range(2):
        with jax.named_scope(f'wwait{i}'):
            lw[i].wait()
        if i == 0:
            lkc[0].start()
            lvc[0].start()
        q = jnp.dot(x_v[...], wbuf[i], preferred_element_type=F32)
        for h in range(4):
            qs[pl.ds(i * 4 + h, batch, stride=8), :] = q[:, h * 128:(h + 1) * 128]
    q_all[quarter] = qs[...].astype(BF16)
    with jax.named_scope('barrier'):
        pl.semaphore_wait(barrier, chips * CORES - 1)

    def spread(buf, rows, ss, rs):
        copies = [pltpu.make_async_remote_copy(buf.at[quarter], buf.at[quarter], ss.at[0], rs.at[0], device_id=partner, device_id_type=MESH)]
        for side, shift in ((0, 1), (1, chips - 1)):
            part = pl.ds(side * rows // 2, rows // 2)
            copies.append(pltpu.make_async_remote_copy(
                buf.at[quarter, part], buf.at[quarter, part], ss.at[1 + side], rs.at[1 + side], device_id=dev(chip + shift, core), device_id_type=MESH))
        return copies

    def hand_on(copies, buf, rows, ss, rs):
        other = ((chip + 1) % 2) * CORES + core
        for side in range(2):
            copies[1 + side].wait_recv()
            part = pl.ds(side * rows // 2, rows // 2)
            c = pltpu.make_async_remote_copy(buf.at[other, part], buf.at[other, part], ss.at[3 + side], rs.at[3 + side], device_id=partner, device_id_type=MESH)
            c.start()
            copies.append(c)

    def arrive(copies):
        copies[0].wait_recv()
        copies[3].wait_recv()
        copies[4].wait_recv()

    q_copies = spread(q_all, batch * 8, q_ss, q_rs)
    for c in q_copies:
        c.start()
    with jax.named_scope('wkvwait'):
        lk.wait()
        lv.wait()
    lkc[1].start()
    lvc[1].start()
    kv = jnp.dot(x_v[...], wbuf[2], preferred_element_type=F32)
    for w in range(2):
        for k in range(2):
            qs[pl.ds(w * 128 + k, batch, stride=2), :] = kv[:, w * 256 + k * 128:w * 256 + (k + 1) * 128]
    for hf in range(2):
        for w in range(2):
            kv_all[quarter, hf * 128 + w * 64:hf * 128 + w * 64 + 64, :] = qs[w * 128 + hf * 64:w * 128 + hf * 64 + 64, :].astype(BF16)
    n_copies = spread(kv_all, batch * 4, n_ss, n_rs)
    for c in n_copies:
        c.start()
    for i in range(2, chunks):
        lkc[i].start()
        lvc[i].start()
    lo.start()

    rowb = lax.broadcasted_iota(jnp.int32, (64, 128), 0) // 8 % 2
    bm0 = jnp.where(rowb == 0, 1.0, 0.0).astype(BF16)
    bm1 = jnp.where(rowb == 1, 1.0, 0.0).astype(BF16)

    with jax.named_scope('handq'):
        hand_on(q_copies, q_all, batch * 8, q_ss, q_rs)
    with jax.named_scope('handn'):
        hand_on(n_copies, kv_all, batch * 4, n_ss, n_rs)
    with jax.named_scope('arrq'):
        arrive(q_copies)

    qlane = lax.broadcasted_iota(jnp.int32, (8, 128), 1)
    own_head = lax.broadcasted_iota(jnp.int32, (8, 128), 0) == (qlane % 64) // 16 * 2 + (qlane % 8) // 4
    qseq = qlane // 64 * 2 + (qlane // 8) % 2
    mt_ref[...] = jnp.zeros_like(mt_ref)

    def scores(qi, buf):
        zero = jnp.zeros((64, 256), BF16)
        rows = []
        for ph in range(2):
            p0 = (2 * qi + ph) * 16
            q = jnp.concatenate([q_all[t, p0:p0 + 16, :] for t in range(4)], axis=0)
            blocks = [q * bm0, q * bm1]
            rows.append(jnp.concatenate(blocks + [zero] if ph == 0 else [zero] + blocks, axis=1))
        kc = jnp.concatenate([kout[4 * qi + j] for j in range(4)], axis=1)
        s = lax.dot_general(kc, jnp.concatenate(rows, axis=0), NT, preferred_element_type=F32).reshape(local_len, 8, 128)
        lim = jnp.full((8, 128), -1, jnp.int32)
        for j in range(4):
            lim = jnp.where(own_head & (qseq == j), pos_ref[4 * qi + j] - base, lim)
        s = jnp.where(lax.broadcasted_iota(jnp.int32, s.shape, 0) < lim[None], s, -jnp.inf)
        buf[...] = s.reshape(buf.shape)
        return jnp.maximum(jnp.max(jnp.max(s, axis=0), axis=0, keepdims=True), NEG)

    def weigh(qi, buf, m):
        p = jnp.exp2((buf[...] - m) * scale2)
        quad = qi % (cb // 4)
        mt_ref[0, quad:quad + 1, :] = m
        mt_ref[1, quad:quad + 1, :] = jnp.sum(p, axis=0, keepdims=True)
        pt = p.astype(BF16).T
        for ph in range(2):
            b0 = 4 * qi + 2 * ph
            vc = jnp.concatenate([vout[b0], vout[b0 + 1]], axis=1)
            o = jnp.dot(pt[ph * 64:(ph + 1) * 64, :], vc, preferred_element_type=F32)
            for t in range(4):
                for b in range(2):
                    r0 = (b0 % cb + b) * 8
                    oraw[t, r0:r0 + 8, :] = o[t * 16 + b * 8:t * 16 + b * 8 + 8, b * 128:(b + 1) * 128]

    rows_c = cb * 8
    carry = {}

    def attend(k):
        if k == 0:
            lkc[0].wait()
            carry['m'] = scores(0, sa)
        if k % 2 == 0:
            lvc[k // 2].wait()
        m_b = scores(2 * k + 1, sb)
        weigh(2 * k, sa, carry['m'])
        if k < 2 * chunks - 1:
            if k % 2 == 1:
                lkc[(k + 1) // 2].wait()
            carry['m'] = scores(2 * k + 2, sa)
        weigh(2 * k + 1, sb, m_b)

    lane = lax.broadcasted_iota(jnp.int32, (8, 128), 1)
    od, oi, yd, yi, ag = {}, {}, {}, {}, {}

    def finalize(i):
        hf = i * cb // half
        first = i * rows_c - hf * half * 8
        rr = lax.broadcasted_iota(jnp.int32, (rows_c, 64), 0) + first
        cc = lax.broadcasted_iota(jnp.int32, (rows_c, 64), 1)
        rel = pos2_ref[hf:hf + 1, :] - base
        keep = (rr // 4 == cc) & (rel >= 0) & (rel < local_len)
        mt, lt = mt_ref[0].T, mt_ref[1].T

        def by_row(x, t):
            return jnp.concatenate([jnp.broadcast_to(x[(p % 2) * 64 + t * 16:(p % 2) * 64 + t * 16 + 16, p // 2:p // 2 + 1], (16, 128))
                                    for p in range(cb // 2)], axis=0)

        for t in range(4):
            qt = q_all[t, i * rows_c:(i + 1) * rows_c, :]
            sn = lax.dot_general(qt, kv_all[t, hf * 128:hf * 128 + 64, :], NT, preferred_element_type=F32)
            sn = jnp.where(keep, sn, -jnp.inf)
            mo = by_row(mt, t)
            mn = jnp.maximum(mo, jnp.max(sn, axis=1, keepdims=True))
            pn = jnp.exp2((sn - mn[:, :64]) * scale2)
            w = jnp.exp2((mo - mn) * scale2)
            lraw[t] = by_row(lt, t) * w + jnp.sum(pn, axis=1, keepdims=True)
            oraw[t] = oraw[t] * w + jnp.dot(pn.astype(BF16), kv_all[t, hf * 128 + 64:hf * 128 + 128, :], preferred_element_type=F32)
            mraw[t] = mn
        for e in range(CORES):
            for t in range(4):
                mp = jnp.zeros((8, 128), F32)
                lp = jnp.zeros((8, 128), F32)
                for h in range(4):
                    src = pl.ds(e * 4 + h, cb, stride=8)
                    om[i, e, t, h * cb:(h + 1) * cb, :] = oraw[t, src, :]
                    mh = mraw[t, src, :]
                    lh = lraw[t, src, :]
                    for g in range(cb // 8):
                        sel = lane == h * (cb // 8) + g
                        mp = jnp.where(sel, mh[g * 8:(g + 1) * 8], mp)
                        lp = jnp.where(sel, lh[g * 8:(g + 1) * 8], lp)
                om[i, e, t, cb * 4:cb * 4 + 8, :] = mp
                om[i, e, t, cb * 4 + 8:cb * 4 + 16, :] = lp
        od[i] = pltpu.make_async_remote_copy(om.at[i, 1 - core], op.at[i], od_s.at[i], od_r.at[i], device_id=partner, device_id_type=MESH)
        od[i].start()

    nrow = cb * 4

    def merge(parts):
        ms = [p[nrow:nrow + 8] for p in parts]
        m = functools.reduce(jnp.maximum, ms)
        ws = [jnp.exp2((x - m) * scale2) for x in ms]
        l = functools.reduce(jnp.add, [w * p[nrow + 8:nrow + 16] for w, p in zip(ws, parts)])
        return m, l, ws

    def chip_reduce(i):
        od[i].wait_recv()
        for t in range(4):
            fold(om.at[i, core, t], om[i, core, t], op[i, t])
        if i in straight:
            oi[i] = [None]
            for d in range(1, chips):
                c = pltpu.make_async_remote_copy(om.at[i, core, lax.rem(chip + d, chips)], orecv.at[i, d - 1], oi_s.at[i, d - 1], oi_r.at[i, d - 1],
                                                 device_id=dev(chip + d, core), device_id_type=MESH)
                c.start()
                oi[i].append(c)
            return
        relay = pltpu.make_async_remote_copy(om.at[i, core, far], orecv.at[i, 0], oi_s.at[i, 0], oi_r.at[i, 0], device_id=dev(via, core), device_id_type=MESH)
        direct = pltpu.make_async_remote_copy(om.at[i, core, opp], orecv.at[i, 1], oi_s.at[i, 1], oi_r.at[i, 1], device_id=dev(opp, core), device_id_type=MESH)
        relay.start()
        direct.start()
        oi[i] = [relay, direct]

    def fold(dst, a, b):
        m, l, (wa, wb) = merge([a, b])
        for g in range(nrow // 8):
            r = slice(g * 8, g * 8 + 8)
            dst[g * 8:g * 8 + 8, :] = a[r] * wa[:, g:g + 1] + b[r] * wb[:, g:g + 1]
        dst[nrow:nrow + 8, :] = m
        dst[nrow + 8:nrow + 16, :] = l

    def o_relay(i):
        oi[i][0].wait_recv()
        fold(om.at[i, core, via], om[i, core, via], orecv[i, 0])
        c = pltpu.make_async_remote_copy(om.at[i, core, via], orecv.at[i, 2], oi_s.at[i, 2], oi_r.at[i, 2], device_id=dev(via, core), device_id_type=MESH)
        c.start()
        oi[i].append(c)

    def project(i):
        for c in oi[i][1:]:
            c.wait_recv()
        if i == 0:
            lo.wait()
        parts = [om[i, core, chip]] + [orecv[i, d] for d in range(0 if i in straight else 1, chips - 1)]
        m, l, ws = merge(parts)
        rl = 1.0 / l
        heads = []
        for h in range(4):
            rows = []
            for g in range(h * (cb // 8), (h + 1) * (cb // 8)):
                o = functools.reduce(jnp.add, [p[g * 8:g * 8 + 8] * w[:, g:g + 1] for p, w in zip(parts, ws)])
                rows.append(o * rl[:, g:g + 1])
            heads.append(jnp.concatenate(rows, axis=0).astype(BF16))
        lhs = jnp.concatenate(heads, axis=1)
        for e in range(CORES):
            for t in range(4):
                c0 = (e * 4 + t) * 512
                ys[i, e, t] = jnp.dot(lhs, wo_v[:, c0:c0 + 512], preferred_element_type=F32)
        yd[i] = pltpu.make_async_remote_copy(ys.at[i, 1 - core], yp.at[i], yd_s.at[i], yd_r.at[i], device_id=partner, device_id_type=MESH)
        yd[i].start()

    def y_chip(i):
        yd[i].wait_recv()
        ys[i, core] = ys[i, core] + yp[i]
        if i in straight:
            yi[i] = [None]
            for d in range(1, chips):
                c = pltpu.make_async_remote_copy(ys.at[i, core, lax.rem(chip + d, chips)], yr.at[i, d - 1], yi_s.at[i, d - 1], yi_r.at[i, d - 1],
                                                 device_id=dev(chip + d, core), device_id_type=MESH)
                c.start()
                yi[i].append(c)
            return
        relay = pltpu.make_async_remote_copy(ys.at[i, core, far], yr.at[i, 0], yi_s.at[i, 0], yi_r.at[i, 0], device_id=dev(via, core), device_id_type=MESH)
        direct = pltpu.make_async_remote_copy(ys.at[i, core, opp], yr.at[i, 1], yi_s.at[i, 1], yi_r.at[i, 1], device_id=dev(opp, core), device_id_type=MESH)
        relay.start()
        direct.start()
        yi[i] = [relay, direct]

    def y_relay(i):
        yi[i][0].wait_recv()
        ys[i, core, via] = ys[i, core, via] + yr[i, 0]
        c = pltpu.make_async_remote_copy(ys.at[i, core, via], yr.at[i, 2], yi_s.at[i, 2], yi_r.at[i, 2], device_id=dev(via, core), device_id_type=MESH)
        c.start()
        yi[i].append(c)

    def block(i, c):
        return (pl.ds(i * cb, cb), pl.ds(pl.multiple_of((core * 4 + c) * 512, 512), 512))

    def y_final(i):
        for c in yi[i][1:]:
            c.wait_recv()
        y = ys[i, core, chip]
        for d in range(0 if i in straight else 1, chips - 1):
            y = y + yr[i, d]
        own = block(i, chip)
        yfull[own] = y.astype(BF16)
        ag[i] = []
        for d in range(chips):
            for f in range(CORES):
                if d or f:
                    slot = d * CORES + f - 1
                    c = pltpu.make_async_remote_copy(yfull.at[own], yfull.at[own], ag_s.at[i, slot], ag_r.at[i, slot],
                                                     device_id=dev(chip + d, lax.rem(core + f, CORES)), device_id_type=MESH)
                    c.start()
                    ag[i].append(c)

    relayed = ((finalize, 1), (chip_reduce, 2), (o_relay, 4), (project, 6), (y_chip, 7), (y_relay, 8), (y_final, 9))
    direct_early = ((finalize, 1), (chip_reduce, 2), (project, 4), (y_chip, 5), (y_final, 7))
    direct_late = ((finalize, 1), (chip_reduce, 2), (project, 3), (y_chip, 4), (y_final, 5))
    plan = {}
    for i in range(chunks):
        for stage, lag in direct_late if i >= chunks - 2 else direct_early if i in straight else relayed:
            plan.setdefault(2 * i + lag, []).append((stage, i))
    for k in range(max(plan) + 1):
        if k < 2 * chunks:
            with jax.named_scope(f'att{k}'):
                attend(k)
        if k == 1:
            arrive(n_copies)
        for stage, i in plan.get(k, ()):
            with jax.named_scope(f'{stage.__name__}{i}'):
                stage(i)
    with jax.named_scope('agwait'):
        for i in range(chunks):
            for c in ag[i]:
                c.wait_recv()
    with jax.named_scope('sendwait'):
        for c in q_copies + n_copies:
            c.wait_send()
        for i in range(chunks):
            for c in [od[i], yd[i]] + oi[i] + yi[i] + ag[i]:
                if c is not None:
                    c.wait_send()


def write_kernel(which, k_in, new_ref, pos_ref, *refs):
    if which == 0:
        y_ref, k_out, k_ref, y_out, src, dst, bsem, ysem = refs
        cy = pltpu.make_async_copy(y_ref, y_out, ysem)
    else:
        k_out, k_ref, src, dst, bsem, ysem = refs
    batch, local_len = k_ref.shape[0], k_ref.shape[1] // 8
    base = lax.axis_index('seq') * local_len
    hb = batch // 2
    pieces = bsem.shape[0]
    pb = batch // pieces
    for t in range(4):
        for hf in range(2):
            src[t, hf * hb * 2:(hf + 1) * hb * 2, :] = new_ref[t, hf * 128 + which * 64:hf * 128 + which * 64 + 64, :].astype(F32)
    for t in range(4):
        for k in range(2):
            dst[pl.ds(t * 2 + k, batch, stride=8), :] = src[t, pl.ds(k, batch, stride=2), :]
    bulk = []
    for i in range(pieces):
        @pl.loop(i * pb, (i + 1) * pb)
        def _(b):
            rel = pos_ref[b] - base

            @pl.when((rel >= 0) & (rel < local_len))
            def _():
                k_ref[b, pl.ds(pl.multiple_of(rel * 8, 8), 8), :] = dst[pl.ds(pl.multiple_of(b * 8, 8), 8), :].astype(BF16)
        part = pl.ds(i * pb, pb)
        c = pltpu.make_async_copy(k_ref.at[part], k_out.at[part], bsem.at[i])
        c.start()
        bulk.append(c)
    if which == 0:
        cy.start()
        bulk.append(cy)
    for c in bulk:
        c.wait()


def solution(mesh):
    cache_spec = P('rep', 'seq', None, None)
    in_specs = (P('rep', None), P(), P(), P(), P('seq', None), cache_spec, cache_spec, P('rep'))
    out_specs = (P('rep', None), cache_spec, cache_spec)
    chips = mesh.shape['seq'] // CORES
    assert chips == 4
    vm = pl.BlockSpec(memory_space=pltpu.VMEM)
    hbm = pl.BlockSpec(memory_space=pl.ANY)
    sm = pl.BlockSpec(memory_space=pltpu.SMEM)

    def local_step(x, wq, wk, wv, wo, k, v, pos):
        shape4 = k.shape
        batch, width = x.shape
        k3 = k.reshape(batch, -1, k.shape[-1])
        v3 = v.reshape(k3.shape)
        chunks = 4
        cb = batch // chunks
        dma = pltpu.SemaphoreType.DMA
        in_hbm = lambda a: pltpu.with_memory_space_constraint(a, pltpu.HBM)
        in_vmem = lambda a: pltpu.with_memory_space_constraint(a, pltpu.VMEM)
        y, ko, vo, new = pl.pallas_call(
            functools.partial(step_kernel, chips),
            out_shape=(pltpu.VMEM((batch, wo.shape[1]), BF16), pltpu.VMEM(k3.shape, BF16), pltpu.VMEM(k3.shape, BF16),
                       pltpu.VMEM((4, batch * 4, 128), BF16)),
            in_specs=[hbm] * 7 + [sm],
            out_specs=[vm] * 4,
            scratch_shapes=[
                pltpu.VMEM((batch, width), BF16), pltpu.VMEM((3, width, 512), BF16), pltpu.VMEM(wo.shape, BF16),
                pltpu.VMEM((batch * 8, 128), F32), pltpu.VMEM((4, batch * 8, 128), BF16), pltpu.VMEM((k3.shape[1], 128), F32), pltpu.VMEM((k3.shape[1], 128), F32), pltpu.VMEM((2, 8, 128), F32), pltpu.VMEM((2, batch), jnp.int32),
                pltpu.VMEM((4, cb * 8, 128), F32), pltpu.VMEM((4, cb * 8, 128), F32), pltpu.VMEM((4, cb * 8, 128), F32),
                pltpu.VMEM((chunks, CORES, 4, cb * 4 + 16, 128), F32), pltpu.VMEM((chunks, 4, cb * 4 + 16, 128), F32),
                pltpu.VMEM((chunks, chips - 1, cb * 4 + 16, 128), F32),
                pltpu.VMEM((chunks, CORES, 4, cb, 512), F32), pltpu.VMEM((chunks, 4, cb, 512), F32), pltpu.VMEM((chunks, chips - 1, cb, 512), F32),
                dma((6,)), dma((2, chunks)), dma((5,)), dma((5,)), dma((5,)), dma((5,)), dma((chunks,)), dma((chunks,)),
                dma((chunks, chips - 1)), dma((chunks, chips - 1)), dma((chunks,)), dma((chunks,)),
                dma((chunks, chips - 1)), dma((chunks, chips - 1)), dma((chunks, chips * CORES - 1)), dma((chunks, chips * CORES - 1))],
            compiler_params=pltpu.CompilerParams(collective_id=0, has_side_effects=True, vmem_limit_bytes=29 << 20),
            name='step',
        )(in_hbm(x), in_hbm(wq), in_hbm(wk), in_hbm(wv), in_hbm(wo), in_hbm(k3), in_hbm(v3), pos)
        pieces = 8

        def write(which, cache, *extra):
            return pl.pallas_call(
                functools.partial(write_kernel, which),
                out_shape=(jax.ShapeDtypeStruct(k3.shape, BF16), pltpu.VMEM(k3.shape, BF16), *(jax.ShapeDtypeStruct(e.shape, BF16) for e in extra)),
                in_specs=[vm, vm, sm] + [vm] * len(extra),
                out_specs=[hbm, vm] + [hbm] * len(extra),
                scratch_shapes=[pltpu.VMEM((4, batch * 2, 128), F32), pltpu.VMEM((batch * 8, 128), F32), dma((pieces,)), dma],
                input_output_aliases={0: 1},
                compiler_params=pltpu.CompilerParams(vmem_limit_bytes=8 << 20),
                name='write',
            )(in_vmem(cache), in_vmem(new), pos, *(in_vmem(e) for e in extra))
        ko, _, y = write(0, ko, y)
        vo, _ = write(1, vo)
        return y, ko.reshape(shape4), vo.reshape(shape4)

    return jax.shard_map(local_step, mesh=mesh, in_specs=in_specs, out_specs=out_specs, check_vma=False)
```

```python
import functools
import math

import jax
import jax.numpy as jnp
from jax import lax
from jax.experimental import pallas as pl
from jax.experimental.pallas import tpu as pltpu
from jax.sharding import PartitionSpec as P

MESH = pl.DeviceIdType.MESH
NEG = -3.4028234e38
F32, BF16 = jnp.float32, jnp.bfloat16
CORES = 2
NT = (((1,), (1,)), ((), ()))


def step_kernel(chips, x_hbm, wq_hbm, wk_hbm, wv_hbm, wo_hbm, k_hbm, v_hbm, pos_ref,
                yfull, kout, vout, rows_ref,
                x_v, wbuf, wo_v, qs, q_all, kv_all, sa, sb, mt_ref, pos2_ref, oraw, mraw, lraw, om, op, orecv,
                ys, yp, yr,
                lsem, kvsem, q_ss, q_rs, n_ss, n_rs, od_s, od_r, oi_s, oi_r, yd_s, yd_r, yi_s, yi_r, ag_s, ag_r):
    batch = k_hbm.shape[0]
    local_len = k_hbm.shape[1] // 8
    chunks = om.shape[0]
    cb = batch // chunks
    half = batch // 2
    scale2 = k_hbm.shape[2] ** -0.5 * math.log2(math.e)
    rep = lax.axis_index('rep')
    me = lax.axis_index('seq')
    chip, core = me // CORES, me % CORES
    base = me * local_len
    quarter = (chip % 2) * CORES + core

    def dev(c, e):
        return (rep, lax.rem(c, chips) * CORES + e)

    partner = dev(chip, 1 - core)
    ncols = 256
    lx = pltpu.make_async_copy(x_hbm, x_v, lsem.at[0])
    lw = [pltpu.make_async_copy(wq_hbm.at[:, pl.ds(pl.multiple_of(quarter * 1024 + i * 512, 512), 512)], wbuf.at[i], lsem.at[1 + i])
          for i in range(2)]
    lk = pltpu.make_async_copy(wk_hbm.at[:, pl.ds(pl.multiple_of(quarter * ncols, ncols), ncols)], wbuf.at[2, :, pl.ds(0, ncols)], lsem.at[3])
    lv = pltpu.make_async_copy(wv_hbm.at[:, pl.ds(pl.multiple_of(quarter * ncols, ncols), ncols)], wbuf.at[2, :, pl.ds(ncols, ncols)], lsem.at[4])
    lo = pltpu.make_async_copy(wo_hbm, wo_v, lsem.at[5])
    lkc = [pltpu.make_async_copy(k_hbm.at[pl.ds(i * cb, cb)], kout.at[pl.ds(i * cb, cb)], kvsem.at[0, i]) for i in range(chunks)]
    lvc = [pltpu.make_async_copy(v_hbm.at[pl.ds(i * cb, cb)], vout.at[pl.ds(i * cb, cb)], kvsem.at[1, i]) for i in range(chunks)]
    lx.start()
    lw[0].start()
    lw[1].start()

    barrier = pltpu.get_barrier_semaphore()
    for d in range(chips):
        for f in range(CORES):
            if d or f:
                pl.semaphore_signal(barrier, inc=1, device_id=dev(chip + d, lax.rem(core + f, CORES)), device_id_type=MESH)

    lane_b = (lax.broadcasted_iota(jnp.int32, pos2_ref.shape, 1) + lax.broadcasted_iota(jnp.int32, pos2_ref.shape, 0) * pos2_ref.shape[1]) // 2
    pv = jnp.zeros(pos2_ref.shape, jnp.int32)
    for b in range(batch):
        pv = jnp.where(lane_b == b, pos_ref[b], pv)
    pos2_ref[...] = pv

    lx.wait()
    for i in range(2):
        with jax.named_scope(f'wwait{i}'):
            lw[i].wait()
        if i == 0:
            lk.start()
            lv.start()
        q = jnp.dot(x_v[...], wbuf[i], preferred_element_type=F32)
        for h in range(4):
            qs[pl.ds(i * 4 + h, batch, stride=8), :] = q[:, h * 128:(h + 1) * 128]
    q_all[quarter] = qs[...].astype(BF16)
    with jax.named_scope('barrier'):
        pl.semaphore_wait(barrier, chips * CORES - 1)

    def spread(buf, rows, ss, rs):
        copies = [pltpu.make_async_remote_copy(buf.at[quarter], buf.at[quarter], ss.at[0], rs.at[0], device_id=partner, device_id_type=MESH)]
        for side, shift in ((0, 1), (1, chips - 1)):
            part = pl.ds(side * rows // 2, rows // 2)
            copies.append(pltpu.make_async_remote_copy(
                buf.at[quarter, part], buf.at[quarter, part], ss.at[1 + side], rs.at[1 + side], device_id=dev(chip + shift, core), device_id_type=MESH))
        return copies

    def hand_on(copies, buf, rows, ss, rs):
        other = ((chip + 1) % 2) * CORES + core
        for side in range(2):
            copies[1 + side].wait_recv()
            part = pl.ds(side * rows // 2, rows // 2)
            c = pltpu.make_async_remote_copy(buf.at[other, part], buf.at[other, part], ss.at[3 + side], rs.at[3 + side], device_id=partner, device_id_type=MESH)
            c.start()
            copies.append(c)

    def arrive(copies):
        copies[0].wait_recv()
        copies[3].wait_recv()
        copies[4].wait_recv()

    q_copies = spread(q_all, batch * 8, q_ss, q_rs)
    for c in q_copies:
        c.start()
    lkc[0].start()
    lvc[0].start()
    with jax.named_scope('wkvwait'):
        lk.wait()
        lv.wait()
    kv = jnp.dot(x_v[...], wbuf[2], preferred_element_type=F32)
    for w in range(2):
        for k in range(2):
            qs[pl.ds(w * 128 + k, batch, stride=2), :] = kv[:, w * 256 + k * 128:w * 256 + (k + 1) * 128]
    for hf in range(2):
        for w in range(2):
            kv_all[quarter, hf * 128 + w * 64:hf * 128 + w * 64 + 64, :] = qs[w * 128 + hf * 64:w * 128 + hf * 64 + 64, :].astype(BF16)
    n_copies = spread(kv_all, batch * 4, n_ss, n_rs)
    for c in n_copies:
        c.start()
    rowb = lax.broadcasted_iota(jnp.int32, (64, 128), 0) // 8 % 2
    bm0 = jnp.where(rowb == 0, 1.0, 0.0).astype(BF16)
    bm1 = jnp.where(rowb == 1, 1.0, 0.0).astype(BF16)

    hand_on(q_copies, q_all, batch * 8, q_ss, q_rs)
    for i in range(1, chunks):
        lkc[i].start()
        lvc[i].start()
    lo.start()
    hand_on(n_copies, kv_all, batch * 4, n_ss, n_rs)
    arrive(q_copies)

    qlane = lax.broadcasted_iota(jnp.int32, (8, 128), 1)
    own_head = lax.broadcasted_iota(jnp.int32, (8, 128), 0) == (qlane % 64) // 16 * 2 + (qlane % 8) // 4
    qseq = qlane // 64 * 2 + (qlane // 8) % 2
    mt_ref[...] = jnp.zeros_like(mt_ref)

    def scores(qi, buf):
        zero = jnp.zeros((64, 256), BF16)
        rows = []
        for ph in range(2):
            p0 = (2 * qi + ph) * 16
            q = jnp.concatenate([q_all[t, p0:p0 + 16, :] for t in range(4)], axis=0)
            blocks = [q * bm0, q * bm1]
            rows.append(jnp.concatenate(blocks + [zero] if ph == 0 else [zero] + blocks, axis=1))
        kc = jnp.concatenate([kout[4 * qi + j] for j in range(4)], axis=1)
        s = lax.dot_general(kc, jnp.concatenate(rows, axis=0), NT, preferred_element_type=F32).reshape(local_len, 8, 128)
        lim = jnp.full((8, 128), -1, jnp.int32)
        for j in range(4):
            lim = jnp.where(own_head & (qseq == j), pos_ref[4 * qi + j] - base, lim)
        s = jnp.where(lax.broadcasted_iota(jnp.int32, s.shape, 0) < lim[None], s, -jnp.inf)
        buf[...] = s.reshape(buf.shape)
        return jnp.maximum(jnp.max(jnp.max(s, axis=0), axis=0, keepdims=True), NEG)

    def weigh(qi, buf, m):
        p = jnp.exp2((buf[...] - m) * scale2)
        quad = qi % (cb // 4)
        mt_ref[0, quad:quad + 1, :] = m
        mt_ref[1, quad:quad + 1, :] = jnp.sum(p, axis=0, keepdims=True)
        pt = p.astype(BF16).T
        for ph in range(2):
            b0 = 4 * qi + 2 * ph
            vc = jnp.concatenate([vout[b0], vout[b0 + 1]], axis=1)
            o = jnp.dot(pt[ph * 64:(ph + 1) * 64, :], vc, preferred_element_type=F32)
            for t in range(4):
                for b in range(2):
                    r0 = (b0 % cb + b) * 8
                    oraw[t, r0:r0 + 8, :] = o[t * 16 + b * 8:t * 16 + b * 8 + 8, b * 128:(b + 1) * 128]

    rows_c = cb * 8
    carry = {}

    def attend(k):
        if k == 0:
            lkc[0].wait()
            carry['m'] = scores(0, sa)
        elif k % 2 == 1 and k < 2 * chunks - 1:
            lkc[(k + 1) // 2].wait()
        if k % 2 == 0:
            lvc[k // 2].wait()
        m_b = scores(2 * k + 1, sb)
        weigh(2 * k, sa, carry['m'])
        if k < 2 * chunks - 1:
            carry['m'] = scores(2 * k + 2, sa)
        weigh(2 * k + 1, sb, m_b)

    lane = lax.broadcasted_iota(jnp.int32, (8, 128), 1)
    od, oi, yd, yi, ag = {}, {}, {}, {}, {}

    def finalize(i):
        hf = i * cb // half
        first = i * rows_c - hf * half * 8
        rr = lax.broadcasted_iota(jnp.int32, (rows_c, 64), 0) + first
        cc = lax.broadcasted_iota(jnp.int32, (rows_c, 64), 1)
        rel = pos2_ref[hf:hf + 1, :] - base
        keep = (rr // 4 == cc) & (rel >= 0) & (rel < local_len)
        mt, lt = mt_ref[0].T, mt_ref[1].T

        def by_row(x, t):
            return jnp.concatenate([jnp.broadcast_to(x[(p % 2) * 64 + t * 16:(p % 2) * 64 + t * 16 + 16, p // 2:p // 2 + 1], (16, 128))
                                    for p in range(cb // 2)], axis=0)

        for t in range(4):
            qt = q_all[t, i * rows_c:(i + 1) * rows_c, :]
            sn = lax.dot_general(qt, kv_all[t, hf * 128:hf * 128 + 64, :], NT, preferred_element_type=F32)
            sn = jnp.where(keep, sn, -jnp.inf)
            mo = by_row(mt, t)
            mn = jnp.maximum(mo, jnp.max(sn, axis=1, keepdims=True))
            pn = jnp.exp2((sn - mn[:, :64]) * scale2)
            w = jnp.exp2((mo - mn) * scale2)
            lraw[t] = by_row(lt, t) * w + jnp.sum(pn, axis=1, keepdims=True)
            oraw[t] = oraw[t] * w + jnp.dot(pn.astype(BF16), kv_all[t, hf * 128 + 64:hf * 128 + 128, :], preferred_element_type=F32)
            mraw[t] = mn
        for e in range(CORES):
            for t in range(4):
                mp = jnp.zeros((8, 128), F32)
                lp = jnp.zeros((8, 128), F32)
                for h in range(4):
                    src = pl.ds(e * 4 + h, cb, stride=8)
                    om[i, e, t, h * cb:(h + 1) * cb, :] = oraw[t, src, :]
                    mh = mraw[t, src, :]
                    lh = lraw[t, src, :]
                    for g in range(cb // 8):
                        sel = lane == h * (cb // 8) + g
                        mp = jnp.where(sel, mh[g * 8:(g + 1) * 8], mp)
                        lp = jnp.where(sel, lh[g * 8:(g + 1) * 8], lp)
                om[i, e, t, cb * 4:cb * 4 + 8, :] = mp
                om[i, e, t, cb * 4 + 8:cb * 4 + 16, :] = lp
        od[i] = pltpu.make_async_remote_copy(om.at[i, 1 - core], op.at[i], od_s.at[i], od_r.at[i], device_id=partner, device_id_type=MESH)
        od[i].start()

    nrow = cb * 4

    def merge(parts):
        ms = [p[nrow:nrow + 8] for p in parts]
        m = functools.reduce(jnp.maximum, ms)
        ws = [jnp.exp2((x - m) * scale2) for x in ms]
        l = functools.reduce(jnp.add, [w * p[nrow + 8:nrow + 16] for w, p in zip(ws, parts)])
        return m, l, ws

    def chip_reduce(i):
        od[i].wait_recv()
        for t in range(4):
            fold(om.at[i, core, t], om[i, core, t], op[i, t])
        oi[i] = []
        for d in range(1, chips):
            c = pltpu.make_async_remote_copy(om.at[i, core, lax.rem(chip + d, chips)], orecv.at[i, d - 1], oi_s.at[i, d - 1], oi_r.at[i, d - 1],
                                             device_id=dev(chip + d, core), device_id_type=MESH)
            c.start()
            oi[i].append(c)

    def fold(dst, a, b):
        m, l, (wa, wb) = merge([a, b])
        for g in range(nrow // 8):
            r = slice(g * 8, g * 8 + 8)
            dst[g * 8:g * 8 + 8, :] = a[r] * wa[:, g:g + 1] + b[r] * wb[:, g:g + 1]
        dst[nrow:nrow + 8, :] = m
        dst[nrow + 8:nrow + 16, :] = l

    def project(i):
        for c in oi[i]:
            c.wait_recv()
        if i == 0:
            lo.wait()
        parts = [om[i, core, chip]] + [orecv[i, d] for d in range(chips - 1)]
        m, l, ws = merge(parts)
        rl = 1.0 / l
        heads = []
        for h in range(4):
            rows = []
            for g in range(h * (cb // 8), (h + 1) * (cb // 8)):
                o = functools.reduce(jnp.add, [p[g * 8:g * 8 + 8] * w[:, g:g + 1] for p, w in zip(parts, ws)])
                rows.append(o * rl[:, g:g + 1])
            heads.append(jnp.concatenate(rows, axis=0).astype(BF16))
        lhs = jnp.concatenate(heads, axis=1)
        for e in range(CORES):
            for t in range(4):
                c0 = (e * 4 + t) * 512
                ys[i, e, t] = jnp.dot(lhs, wo_v[:, c0:c0 + 512], preferred_element_type=F32)
        yd[i] = pltpu.make_async_remote_copy(ys.at[i, 1 - core], yp.at[i], yd_s.at[i], yd_r.at[i], device_id=partner, device_id_type=MESH)
        yd[i].start()

    def y_chip(i):
        yd[i].wait_recv()
        ys[i, core] = ys[i, core] + yp[i]
        yi[i] = []
        for d in range(1, chips):
            c = pltpu.make_async_remote_copy(ys.at[i, core, lax.rem(chip + d, chips)], yr.at[i, d - 1], yi_s.at[i, d - 1], yi_r.at[i, d - 1],
                                             device_id=dev(chip + d, core), device_id_type=MESH)
            c.start()
            yi[i].append(c)

    def block(i, c):
        return (pl.ds(i * cb, cb), pl.ds(pl.multiple_of((core * 4 + c) * 512, 512), 512))

    def lay_rows():
        for w in range(2):
            for t in range(4):
                for hf in range(2):
                    sa[:64, :] = kv_all[t, hf * 128 + w * 64:hf * 128 + w * 64 + 64, :].astype(F32)
                    for k in range(2):
                        qs[pl.ds(hf * half * 8 + t * 2 + k, half, stride=8), :] = sa[pl.ds(k, half, stride=2), :]
            rows_ref[w] = qs[...].astype(BF16)

    def y_final(i):
        if i == chunks - 1:
            lay_rows()
        for c in yi[i]:
            c.wait_recv()
        y = ys[i, core, chip]
        for d in range(chips - 1):
            y = y + yr[i, d]
        own = block(i, chip)
        yfull[own] = y.astype(BF16)
        ag[i] = []
        for d in range(chips):
            for f in range(CORES):
                if d or f:
                    slot = d * CORES + f - 1
                    c = pltpu.make_async_remote_copy(yfull.at[own], yfull.at[own], ag_s.at[i, slot], ag_r.at[i, slot],
                                                     device_id=dev(chip + d, lax.rem(core + f, CORES)), device_id_type=MESH)
                    c.start()
                    ag[i].append(c)

    plan = {1: [(finalize, 0)], 2: [(chip_reduce, 0)], 3: [(finalize, 1)], 4: [(chip_reduce, 1), (project, 0)],
            5: [(finalize, 2), (y_chip, 0)], 6: [(chip_reduce, 2), (project, 1)],
            7: [(finalize, 3), (y_chip, 1), (y_final, 0), (chip_reduce, 3), (project, 2), (y_chip, 2), (y_final, 1), (project, 3), (y_chip, 3), (y_final, 2), (y_final, 3)]}
    for k in range(max(plan) + 1):
        if k < 2 * chunks:
            with jax.named_scope(f'att{k}'):
                attend(k)
        if k == 1:
            arrive(n_copies)
        for stage, i in plan.get(k, ()):
            with jax.named_scope(f'{stage.__name__}{i}'):
                stage(i)
    with jax.named_scope('agwait'):
        for i in range(chunks):
            for c in ag[i]:
                c.wait_recv()
    with jax.named_scope('sendwait'):
        for c in q_copies + n_copies:
            c.wait_send()
        for i in range(chunks):
            for c in [od[i], yd[i]] + oi[i] + yi[i] + ag[i]:
                c.wait_send()


def write_kernel(which, k_in, new_ref, pos_ref, *refs):
    if which == 0:
        y_ref, k_out, k_ref, y_out, bsem, ysem = refs
        cy = pltpu.make_async_copy(y_ref, y_out, ysem)
    else:
        k_out, k_ref, bsem, ysem = refs
    batch, local_len = k_ref.shape[0], k_ref.shape[1] // 8
    base = lax.axis_index('seq') * local_len
    pieces = bsem.shape[0]
    pb = batch // pieces
    bulk = []
    for i in range(pieces):
        @pl.loop(i * pb, (i + 1) * pb)
        def _(b):
            rel = pos_ref[b] - base

            @pl.when((rel >= 0) & (rel < local_len))
            def _():
                k_ref[b, pl.ds(pl.multiple_of(rel * 8, 8), 8), :] = new_ref[which, pl.ds(pl.multiple_of(b * 8, 8), 8), :]
        part = pl.ds(i * pb, pb)
        c = pltpu.make_async_copy(k_ref.at[part], k_out.at[part], bsem.at[i])
        c.start()
        bulk.append(c)
    if which == 0:
        cy.start()
        bulk.append(cy)
    for c in bulk:
        c.wait()


def solution(mesh):
    cache_spec = P('rep', 'seq', None, None)
    in_specs = (P('rep', None), P(), P(), P(), P('seq', None), cache_spec, cache_spec, P('rep'))
    out_specs = (P('rep', None), cache_spec, cache_spec)
    chips = mesh.shape['seq'] // CORES
    assert chips == 4
    vm = pl.BlockSpec(memory_space=pltpu.VMEM)
    hbm = pl.BlockSpec(memory_space=pl.ANY)
    sm = pl.BlockSpec(memory_space=pltpu.SMEM)

    def local_step(x, wq, wk, wv, wo, k, v, pos):
        shape4 = k.shape
        batch, width = x.shape
        k3 = k.reshape(batch, -1, k.shape[-1])
        v3 = v.reshape(k3.shape)
        chunks = 4
        cb = batch // chunks
        dma = pltpu.SemaphoreType.DMA
        in_hbm = lambda a: pltpu.with_memory_space_constraint(a, pltpu.HBM)
        in_vmem = lambda a: pltpu.with_memory_space_constraint(a, pltpu.VMEM)
        y, ko, vo, new = pl.pallas_call(
            functools.partial(step_kernel, chips),
            out_shape=(pltpu.VMEM((batch, wo.shape[1]), BF16), pltpu.VMEM(k3.shape, BF16), pltpu.VMEM(k3.shape, BF16),
                       pltpu.VMEM((2, batch * 8, 128), BF16)),
            in_specs=[hbm] * 7 + [sm],
            out_specs=[vm] * 4,
            scratch_shapes=[
                pltpu.VMEM((batch, width), BF16), pltpu.VMEM((3, width, 512), BF16), pltpu.VMEM(wo.shape, BF16),
                pltpu.VMEM((batch * 8, 128), F32), pltpu.VMEM((4, batch * 8, 128), BF16), pltpu.VMEM((4, batch * 4, 128), BF16), pltpu.VMEM((k3.shape[1], 128), F32), pltpu.VMEM((k3.shape[1], 128), F32), pltpu.VMEM((2, 8, 128), F32), pltpu.VMEM((2, batch), jnp.int32),
                pltpu.VMEM((4, cb * 8, 128), F32), pltpu.VMEM((4, cb * 8, 128), F32), pltpu.VMEM((4, cb * 8, 128), F32),
                pltpu.VMEM((chunks, CORES, 4, cb * 4 + 16, 128), F32), pltpu.VMEM((chunks, 4, cb * 4 + 16, 128), F32),
                pltpu.VMEM((chunks, chips - 1, cb * 4 + 16, 128), F32),
                pltpu.VMEM((chunks, CORES, 4, cb, 512), F32), pltpu.VMEM((chunks, 4, cb, 512), F32), pltpu.VMEM((chunks, chips - 1, cb, 512), F32),
                dma((6,)), dma((2, chunks)), dma((5,)), dma((5,)), dma((5,)), dma((5,)), dma((chunks,)), dma((chunks,)),
                dma((chunks, chips - 1)), dma((chunks, chips - 1)), dma((chunks,)), dma((chunks,)),
                dma((chunks, chips - 1)), dma((chunks, chips - 1)), dma((chunks, chips * CORES - 1)), dma((chunks, chips * CORES - 1))],
            compiler_params=pltpu.CompilerParams(collective_id=0, has_side_effects=True, vmem_limit_bytes=29 << 20),
            name='step',
        )(in_hbm(x), in_hbm(wq), in_hbm(wk), in_hbm(wv), in_hbm(wo), in_hbm(k3), in_hbm(v3), pos)
        pieces = 8

        def write(which, cache, *extra):
            return pl.pallas_call(
                functools.partial(write_kernel, which),
                out_shape=(jax.ShapeDtypeStruct(k3.shape, BF16), pltpu.VMEM(k3.shape, BF16), *(jax.ShapeDtypeStruct(e.shape, BF16) for e in extra)),
                in_specs=[vm, vm, sm] + [vm] * len(extra),
                out_specs=[hbm, vm] + [hbm] * len(extra),
                scratch_shapes=[dma((pieces,)), dma],
                input_output_aliases={0: 1},
                compiler_params=pltpu.CompilerParams(vmem_limit_bytes=4 << 20),
                name='write',
            )(in_vmem(cache), in_vmem(new), pos, *(in_vmem(e) for e in extra))
        ko, _, y = write(0, ko, y)
        vo, _ = write(1, vo)
        return y, ko.reshape(shape4), vo.reshape(shape4)

    return jax.shard_map(local_step, mesh=mesh, in_specs=in_specs, out_specs=out_specs, check_vma=False)
```

```python
import functools
import math

import jax
import jax.numpy as jnp
from jax import lax
from jax.experimental import pallas as pl
from jax.experimental.pallas import tpu as pltpu
from jax.sharding import PartitionSpec as P

MESH = pl.DeviceIdType.MESH
NEG = -3.4028234e38
F32, BF16 = jnp.float32, jnp.bfloat16
CORES = 2
NT = (((1,), (1,)), ((), ()))


def step_kernel(chips, x_hbm, wq_hbm, wk_hbm, wv_hbm, wo_hbm, k_hbm, v_hbm, pos_ref,
                y0_ref, y1_ref, y2_ref, y3_ref, kout, vout, rows_ref,
                x_v, wbuf, wo_v, qs, q_all, kv_all, sa, sb, mt_ref, pos2_ref, oraw, mraw, lraw, om, op, orecv,
                ys, yp,
                lsem, kvsem, q_ss, q_rs, n_ss, n_rs, od_s, od_r, oi_s, oi_r, yd_s, yd_r):
    batch = k_hbm.shape[0]
    local_len = k_hbm.shape[1] // 8
    chunks = om.shape[0]
    cb = batch // chunks
    half = batch // 2
    scale2 = k_hbm.shape[2] ** -0.5 * math.log2(math.e)
    rep = lax.axis_index('rep')
    me = lax.axis_index('seq')
    chip, core = me // CORES, me % CORES
    base = me * local_len
    quarter = (chip % 2) * CORES + core

    def dev(c, e):
        return (rep, lax.rem(c, chips) * CORES + e)

    partner = dev(chip, 1 - core)
    ncols = 256
    lx = pltpu.make_async_copy(x_hbm, x_v, lsem.at[0])
    lw = [pltpu.make_async_copy(wq_hbm.at[:, pl.ds(pl.multiple_of(quarter * 1024 + i * 512, 512), 512)], wbuf.at[i], lsem.at[1 + i])
          for i in range(2)]
    lk = pltpu.make_async_copy(wk_hbm.at[:, pl.ds(pl.multiple_of(quarter * ncols, ncols), ncols)], wbuf.at[2, :, pl.ds(0, ncols)], lsem.at[3])
    lv = pltpu.make_async_copy(wv_hbm.at[:, pl.ds(pl.multiple_of(quarter * ncols, ncols), ncols)], wbuf.at[2, :, pl.ds(ncols, ncols)], lsem.at[4])
    lo = pltpu.make_async_copy(wo_hbm, wo_v, lsem.at[5])
    lkc = [pltpu.make_async_copy(k_hbm.at[pl.ds(i * cb, cb)], kout.at[pl.ds(i * cb, cb)], kvsem.at[0, i]) for i in range(chunks)]
    lvc = [pltpu.make_async_copy(v_hbm.at[pl.ds(i * cb, cb)], vout.at[pl.ds(i * cb, cb)], kvsem.at[1, i]) for i in range(chunks)]
    lx.start()
    lw[0].start()
    lw[1].start()

    barrier = pltpu.get_barrier_semaphore()
    for d in range(chips):
        for f in range(CORES):
            if d or f:
                pl.semaphore_signal(barrier, inc=1, device_id=dev(chip + d, lax.rem(core + f, CORES)), device_id_type=MESH)

    lane_b = (lax.broadcasted_iota(jnp.int32, pos2_ref.shape, 1) + lax.broadcasted_iota(jnp.int32, pos2_ref.shape, 0) * pos2_ref.shape[1]) // 2
    pv = jnp.zeros(pos2_ref.shape, jnp.int32)
    for b in range(batch):
        pv = jnp.where(lane_b == b, pos_ref[b], pv)
    pos2_ref[...] = pv

    lx.wait()
    for i in range(2):
        with jax.named_scope(f'wwait{i}'):
            lw[i].wait()
        if i == 0:
            lk.start()
            lv.start()
        q = jnp.dot(x_v[...], wbuf[i], preferred_element_type=F32)
        for h in range(4):
            qs[pl.ds(i * 4 + h, batch, stride=8), :] = q[:, h * 128:(h + 1) * 128]
    q_all[quarter] = qs[...].astype(BF16)
    with jax.named_scope('barrier'):
        pl.semaphore_wait(barrier, chips * CORES - 1)

    def spread(buf, rows, ss, rs):
        copies = [pltpu.make_async_remote_copy(buf.at[quarter], buf.at[quarter], ss.at[0], rs.at[0], device_id=partner, device_id_type=MESH)]
        for side, shift in ((0, 1), (1, chips - 1)):
            part = pl.ds(side * rows // 2, rows // 2)
            copies.append(pltpu.make_async_remote_copy(
                buf.at[quarter, part], buf.at[quarter, part], ss.at[1 + side], rs.at[1 + side], device_id=dev(chip + shift, core), device_id_type=MESH))
        return copies

    def hand_on(copies, buf, rows, ss, rs):
        other = ((chip + 1) % 2) * CORES + core
        for side in range(2):
            copies[1 + side].wait_recv()
            part = pl.ds(side * rows // 2, rows // 2)
            c = pltpu.make_async_remote_copy(buf.at[other, part], buf.at[other, part], ss.at[3 + side], rs.at[3 + side], device_id=partner, device_id_type=MESH)
            c.start()
            copies.append(c)

    def arrive(copies):
        copies[0].wait_recv()
        copies[3].wait_recv()
        copies[4].wait_recv()

    q_copies = spread(q_all, batch * 8, q_ss, q_rs)
    for c in q_copies:
        c.start()
    lkc[0].start()
    lvc[0].start()
    with jax.named_scope('wkvwait'):
        lk.wait()
        lv.wait()
    kv = jnp.dot(x_v[...], wbuf[2], preferred_element_type=F32)
    for w in range(2):
        for k in range(2):
            qs[pl.ds(w * 128 + k, batch, stride=2), :] = kv[:, w * 256 + k * 128:w * 256 + (k + 1) * 128]
    for hf in range(2):
        for w in range(2):
            kv_all[quarter, hf * 128 + w * 64:hf * 128 + w * 64 + 64, :] = qs[w * 128 + hf * 64:w * 128 + hf * 64 + 64, :].astype(BF16)
    n_copies = spread(kv_all, batch * 4, n_ss, n_rs)
    for c in n_copies:
        c.start()
    rowb = lax.broadcasted_iota(jnp.int32, (64, 128), 0) // 8 % 2
    bm0 = jnp.where(rowb == 0, 1.0, 0.0).astype(BF16)
    bm1 = jnp.where(rowb == 1, 1.0, 0.0).astype(BF16)

    with jax.named_scope('handq'):
        hand_on(q_copies, q_all, batch * 8, q_ss, q_rs)
    for i in range(1, chunks):
        lkc[i].start()
        lvc[i].start()
    lo.start()
    with jax.named_scope('handn'):
        hand_on(n_copies, kv_all, batch * 4, n_ss, n_rs)
    with jax.named_scope('arrq'):
        arrive(q_copies)

    qlane = lax.broadcasted_iota(jnp.int32, (8, 128), 1)
    own_head = lax.broadcasted_iota(jnp.int32, (8, 128), 0) == (qlane % 64) // 16 * 2 + (qlane % 8) // 4
    qseq = qlane // 64 * 2 + (qlane // 8) % 2
    mt_ref[...] = jnp.zeros_like(mt_ref)

    def scores(qi, buf):
        zero = jnp.zeros((64, 256), BF16)
        rows = []
        for ph in range(2):
            p0 = (2 * qi + ph) * 16
            q = jnp.concatenate([q_all[t, p0:p0 + 16, :] for t in range(4)], axis=0)
            blocks = [q * bm0, q * bm1]
            rows.append(jnp.concatenate(blocks + [zero] if ph == 0 else [zero] + blocks, axis=1))
        kc = jnp.concatenate([kout[4 * qi + j] for j in range(4)], axis=1)
        s = lax.dot_general(kc, jnp.concatenate(rows, axis=0), NT, preferred_element_type=F32).reshape(local_len, 8, 128)
        lim = jnp.full((8, 128), -1, jnp.int32)
        for j in range(4):
            lim = jnp.where(own_head & (qseq == j), pos_ref[4 * qi + j] - base, lim)
        s = jnp.where(lax.broadcasted_iota(jnp.int32, s.shape, 0) < lim[None], s, -jnp.inf)
        buf[...] = s.reshape(buf.shape)
        return jnp.maximum(jnp.max(jnp.max(s, axis=0), axis=0, keepdims=True), NEG)

    def weigh(qi, buf, m):
        p = jnp.exp2((buf[...] - m) * scale2)
        quad = qi % (cb // 4)
        mt_ref[0, quad:quad + 1, :] = m
        mt_ref[1, quad:quad + 1, :] = jnp.sum(p, axis=0, keepdims=True)
        pt = p.astype(BF16).T
        for ph in range(2):
            b0 = 4 * qi + 2 * ph
            vc = jnp.concatenate([vout[b0], vout[b0 + 1]], axis=1)
            o = jnp.dot(pt[ph * 64:(ph + 1) * 64, :], vc, preferred_element_type=F32)
            for t in range(4):
                for b in range(2):
                    r0 = (b0 % cb + b) * 8
                    oraw[t, r0:r0 + 8, :] = o[t * 16 + b * 8:t * 16 + b * 8 + 8, b * 128:(b + 1) * 128]

    rows_c = cb * 8
    carry = {}

    def attend(k):
        if k == 0:
            lkc[0].wait()
            carry['m'] = scores(0, sa)
        elif k % 2 == 1 and k < 2 * chunks - 1:
            lkc[(k + 1) // 2].wait()
        if k % 2 == 0:
            lvc[k // 2].wait()
        m_b = scores(2 * k + 1, sb)
        weigh(2 * k, sa, carry['m'])
        if k < 2 * chunks - 1:
            carry['m'] = scores(2 * k + 2, sa)
        weigh(2 * k + 1, sb, m_b)

    lane = lax.broadcasted_iota(jnp.int32, (8, 128), 1)
    od, oi, yd = {}, {}, {}

    def finalize(i):
        hf = i * cb // half
        first = i * rows_c - hf * half * 8
        rr = lax.broadcasted_iota(jnp.int32, (rows_c, 64), 0) + first
        cc = lax.broadcasted_iota(jnp.int32, (rows_c, 64), 1)
        rel = pos2_ref[hf:hf + 1, :] - base
        keep = (rr // 4 == cc) & (rel >= 0) & (rel < local_len)
        mt, lt = mt_ref[0].T, mt_ref[1].T

        def by_row(x, t):
            return jnp.concatenate([jnp.broadcast_to(x[(p % 2) * 64 + t * 16:(p % 2) * 64 + t * 16 + 16, p // 2:p // 2 + 1], (16, 128))
                                    for p in range(cb // 2)], axis=0)

        for t in range(4):
            qt = q_all[t, i * rows_c:(i + 1) * rows_c, :]
            sn = lax.dot_general(qt, kv_all[t, hf * 128:hf * 128 + 64, :], NT, preferred_element_type=F32)
            sn = jnp.where(keep, sn, -jnp.inf)
            mo = by_row(mt, t)
            mn = jnp.maximum(mo, jnp.max(sn, axis=1, keepdims=True))
            pn = jnp.exp2((sn - mn[:, :64]) * scale2)
            w = jnp.exp2((mo - mn) * scale2)
            lraw[t] = by_row(lt, t) * w + jnp.sum(pn, axis=1, keepdims=True)
            oraw[t] = oraw[t] * w + jnp.dot(pn.astype(BF16), kv_all[t, hf * 128 + 64:hf * 128 + 128, :], preferred_element_type=F32)
            mraw[t] = mn
        for e in range(CORES):
            for t in range(4):
                mp = jnp.zeros((8, 128), F32)
                lp = jnp.zeros((8, 128), F32)
                for h in range(4):
                    src = pl.ds(e * 4 + h, cb, stride=8)
                    om[i, e, t, h * cb:(h + 1) * cb, :] = oraw[t, src, :]
                    mh = mraw[t, src, :]
                    lh = lraw[t, src, :]
                    for g in range(cb // 8):
                        sel = lane == h * (cb // 8) + g
                        mp = jnp.where(sel, mh[g * 8:(g + 1) * 8], mp)
                        lp = jnp.where(sel, lh[g * 8:(g + 1) * 8], lp)
                om[i, e, t, cb * 4:cb * 4 + 8, :] = mp
                om[i, e, t, cb * 4 + 8:cb * 4 + 16, :] = lp
        od[i] = pltpu.make_async_remote_copy(om.at[i, 1 - core], op.at[i], od_s.at[i], od_r.at[i], device_id=partner, device_id_type=MESH)
        od[i].start()

    nrow = cb * 4

    def merge(parts):
        ms = [p[nrow:nrow + 8] for p in parts]
        m = functools.reduce(jnp.maximum, ms)
        ws = [jnp.exp2((x - m) * scale2) for x in ms]
        l = functools.reduce(jnp.add, [w * p[nrow + 8:nrow + 16] for w, p in zip(ws, parts)])
        return m, l, ws

    def chip_reduce(i):
        od[i].wait_recv()
        for t in range(4):
            fold(om.at[i, core, t], om[i, core, t], op[i, t])
        oi[i] = []
        for d in range(1, chips):
            c = pltpu.make_async_remote_copy(om.at[i, core, lax.rem(chip + d, chips)], orecv.at[i, d - 1], oi_s.at[i, d - 1], oi_r.at[i, d - 1],
                                             device_id=dev(chip + d, core), device_id_type=MESH)
            c.start()
            oi[i].append(c)

    def fold(dst, a, b):
        m, l, (wa, wb) = merge([a, b])
        for g in range(nrow // 8):
            r = slice(g * 8, g * 8 + 8)
            dst[g * 8:g * 8 + 8, :] = a[r] * wa[:, g:g + 1] + b[r] * wb[:, g:g + 1]
        dst[nrow:nrow + 8, :] = m
        dst[nrow + 8:nrow + 16, :] = l

    def project(g):
        heads = [[] for _ in range(4)]
        for i in groups[g]:
            for c in oi[i]:
                c.wait_recv()
            parts = [om[i, core, chip]] + [orecv[i, d] for d in range(chips - 1)]
            m, l, ws = merge(parts)
            rl = 1.0 / l
            for h in range(4):
                rows = []
                for r in range(h * (cb // 8), (h + 1) * (cb // 8)):
                    o = functools.reduce(jnp.add, [p[r * 8:r * 8 + 8] * w[:, r:r + 1] for p, w in zip(parts, ws)])
                    rows.append(o * rl[:, r:r + 1])
                heads[h].append(jnp.concatenate(rows, axis=0).astype(BF16))
        if g == 0:
            lo.wait()
        lhs = jnp.concatenate([jnp.concatenate(h, axis=0) for h in heads], axis=1)
        r0, r1 = groups[g][0] * cb, (groups[g][-1] + 1) * cb
        for e in range(CORES):
            for t in range(4):
                c0 = (e * 4 + t) * 512
                ys[e, t, r0:r1, :] = jnp.dot(lhs, wo_v[:, c0:c0 + 512], preferred_element_type=F32)
        part = pl.ds(r0, r1 - r0)
        yd[g] = pltpu.make_async_remote_copy(ys.at[1 - core, :, part], yp.at[:, part], yd_s.at[g], yd_r.at[g], device_id=partner, device_id_type=MESH)
        yd[g].start()

    def lay_rows():
        for w in range(2):
            for t in range(4):
                for hf in range(2):
                    sa[:64, :] = kv_all[t, hf * 128 + w * 64:hf * 128 + w * 64 + 64, :].astype(F32)
                    for k in range(2):
                        qs[pl.ds(hf * half * 8 + t * 2 + k, half, stride=8), :] = sa[pl.ds(k, half, stride=2), :]
            rows_ref[w] = qs[...].astype(BF16)

    def y_chip(g):
        yd[g].wait_recv()
        r0, r1 = groups[g][0] * cb, (groups[g][-1] + 1) * cb
        for d, out in enumerate((y0_ref, y1_ref, y2_ref, y3_ref)):
            t = lax.rem(chip + d, chips)
            out[r0:r1, :] = ys[core, t, r0:r1, :] + yp[t, r0:r1, :]

    groups = (tuple(range(chunks - 1)), (chunks - 1,))
    plan = {2 * i + 1 + j: [(stage, i)] for i in range(chunks) for j, stage in enumerate((finalize, chip_reduce)) if 2 * i + 1 + j < 2 * chunks}
    plan[2 * chunks - 1] += [(chip_reduce, chunks - 1), (project, 0), (y_chip, 0), (project, 1), (y_chip, 1)]
    for k in range(max(plan) + 1):
        if k < 2 * chunks:
            with jax.named_scope(f'att{k}'):
                attend(k)
        if k == 1:
            arrive(n_copies)
        for stage, i in plan.get(k, ()):
            if stage is y_chip and i == 0:
                lay_rows()
            with jax.named_scope(f'{stage.__name__}{i}'):
                stage(i)
    with jax.named_scope('sendwait'):
        for c in q_copies + n_copies:
            c.wait_send()
        for g in range(len(groups)):
            yd[g].wait_send()
        for i in range(chunks):
            for c in [od[i]] + oi[i]:
                c.wait_send()


def write_kernel(which, k_in, new_ref, pos_ref, k_out, k_ref, bsem):
    batch, local_len = k_ref.shape[0], k_ref.shape[1] // 8
    base = lax.axis_index('seq') * local_len
    pieces = bsem.shape[0]
    pb = batch // pieces
    bulk = []
    for i in range(pieces):
        @pl.loop(i * pb, (i + 1) * pb)
        def _(b):
            rel = pos_ref[b] - base

            @pl.when((rel >= 0) & (rel < local_len))
            def _():
                k_ref[b, pl.ds(pl.multiple_of(rel * 8, 8), 8), :] = new_ref[which, pl.ds(pl.multiple_of(b * 8, 8), 8), :]
        part = pl.ds(i * pb, pb)
        c = pltpu.make_async_copy(k_ref.at[part], k_out.at[part], bsem.at[i])
        c.start()
        bulk.append(c)
    for c in bulk:
        c.wait()


def assemble_kernel(chips, *refs):
    blocks, y_out, sem = refs[:-2], refs[-2], refs[-1]
    me = lax.axis_index('seq')
    copies = []
    for n, b in enumerate(blocks):
        d, f = n // CORES, n % CORES
        src_chip, src_core = lax.rem(me // CORES + chips - d, chips), lax.rem(me % CORES + f, CORES)
        col = pl.multiple_of((src_core * 4 + src_chip) * 512, 512)
        copies.append(pltpu.make_async_copy(b, y_out.at[:, pl.ds(col, 512)], sem.at[n]))
        copies[-1].start()
    for c in copies:
        c.wait()


def solution(mesh):
    cache_spec = P('rep', 'seq', None, None)
    in_specs = (P('rep', None), P(), P(), P(), P('seq', None), cache_spec, cache_spec, P('rep'))
    out_specs = (P('rep', None), cache_spec, cache_spec)
    chips = mesh.shape['seq'] // CORES
    assert chips == 4
    vm = pl.BlockSpec(memory_space=pltpu.VMEM)
    hbm = pl.BlockSpec(memory_space=pl.ANY)
    sm = pl.BlockSpec(memory_space=pltpu.SMEM)

    def local_step(x, wq, wk, wv, wo, k, v, pos):
        shape4 = k.shape
        batch, width = x.shape
        k3 = k.reshape(batch, -1, k.shape[-1])
        v3 = v.reshape(k3.shape)
        chunks = 4
        cb = batch // chunks
        dma = pltpu.SemaphoreType.DMA
        in_hbm = lambda a: pltpu.with_memory_space_constraint(a, pltpu.HBM)
        in_vmem = lambda a: pltpu.with_memory_space_constraint(a, pltpu.VMEM)
        part = jax.ShapeDtypeStruct((batch, 512), F32)
        *parts, ko, vo, new = pl.pallas_call(
            functools.partial(step_kernel, chips),
            out_shape=(part, part, part, part, pltpu.VMEM(k3.shape, BF16), pltpu.VMEM(k3.shape, BF16),
                       pltpu.VMEM((2, batch * 8, 128), BF16)),
            in_specs=[hbm] * 7 + [sm],
            out_specs=[vm] * 7,
            scratch_shapes=[
                pltpu.VMEM((batch, width), BF16), pltpu.VMEM((3, width, 512), BF16), pltpu.VMEM(wo.shape, BF16),
                pltpu.VMEM((batch * 8, 128), F32), pltpu.VMEM((4, batch * 8, 128), BF16), pltpu.VMEM((4, batch * 4, 128), BF16), pltpu.VMEM((k3.shape[1], 128), F32), pltpu.VMEM((k3.shape[1], 128), F32), pltpu.VMEM((2, 8, 128), F32), pltpu.VMEM((2, batch), jnp.int32),
                pltpu.VMEM((4, cb * 8, 128), F32), pltpu.VMEM((4, cb * 8, 128), F32), pltpu.VMEM((4, cb * 8, 128), F32),
                pltpu.VMEM((chunks, CORES, 4, cb * 4 + 16, 128), F32), pltpu.VMEM((chunks, 4, cb * 4 + 16, 128), F32),
                pltpu.VMEM((chunks, chips - 1, cb * 4 + 16, 128), F32),
                pltpu.VMEM((CORES, 4, batch, 512), F32), pltpu.VMEM((4, batch, 512), F32),
                dma((6,)), dma((2, chunks)), dma((5,)), dma((5,)), dma((5,)), dma((5,)), dma((chunks,)), dma((chunks,)),
                dma((chunks, chips - 1)), dma((chunks, chips - 1)), dma((2,)), dma((2,))],
            compiler_params=pltpu.CompilerParams(collective_id=0, has_side_effects=True, vmem_limit_bytes=29 << 20),
            name='step',
        )(in_hbm(x), in_hbm(wq), in_hbm(wk), in_hbm(wv), in_hbm(wo), in_hbm(k3), in_hbm(v3), pos)
        pieces = 8

        def write(which, cache):
            return pl.pallas_call(
                functools.partial(write_kernel, which),
                out_shape=(jax.ShapeDtypeStruct(k3.shape, BF16), pltpu.VMEM(k3.shape, BF16)),
                in_specs=[vm, vm, sm],
                out_specs=[hbm, vm],
                scratch_shapes=[dma((pieces,))],
                input_output_aliases={0: 1},
                cost_estimate=pl.CostEstimate(flops=0, bytes_accessed=k3.size * 2, transcendentals=0),
                compiler_params=pltpu.CompilerParams(vmem_limit_bytes=4 << 20),
                name='write',
            )(in_vmem(cache), in_vmem(new), pos)[0].reshape(shape4)

        def shift(a, d, f):
            size = chips * CORES
            return lax.ppermute(a, 'seq', [(s, (s // CORES + d) % chips * CORES + (s + f) % CORES) for s in range(size)])

        recv = [shift(parts[d], d, 0) for d in range(1, chips)]
        *recv, k_new = lax.optimization_barrier((*recv, write(0, ko)))
        y = parts[0]
        for r in recv:
            y = y + r
        y = y.astype(BF16)
        blocks = [shift(y, d, f) if d or f else y for d in range(chips) for f in range(CORES)]
        y = pl.pallas_call(
            functools.partial(assemble_kernel, chips),
            out_shape=jax.ShapeDtypeStruct((batch, wo.shape[1]), BF16),
            in_specs=[hbm] * len(blocks),
            out_specs=hbm,
            scratch_shapes=[dma((len(blocks),))],
            compiler_params=pltpu.CompilerParams(vmem_limit_bytes=1 << 20),
            name='assemble',
        )(*blocks)
        return y, k_new, write(1, vo)

    return jax.shard_map(local_step, mesh=mesh, in_specs=in_specs, out_specs=out_specs, check_vma=False)
```

```python
import functools
import math

import jax
import jax.numpy as jnp
from jax import lax
from jax.experimental import pallas as pl
from jax.experimental.pallas import tpu as pltpu
from jax.sharding import PartitionSpec as P

MESH = pl.DeviceIdType.MESH
NEG = -3.4028234e38
F32, BF16 = jnp.float32, jnp.bfloat16
CORES = 2
NT = (((1,), (1,)), ((), ()))


def step_kernel(chips, x_hbm, wq_hbm, wk_hbm, wv_hbm, wo_hbm, k_hbm, v_hbm, pos_ref,
                yfull, kout, vout, rows_ref,
                x_v, wbuf, wo_v, qs, q_all, kv_all, sa, sb, mt_ref, pos2_ref, oraw, mraw, lraw, om, op, orecv,
                ys, yp, yr,
                lsem, kvsem, q_ss, q_rs, n_ss, n_rs, od_s, od_r, oi_s, oi_r, yd_s, yd_r, yi_s, yi_r, ag_s, ag_r):
    batch = k_hbm.shape[0]
    local_len = k_hbm.shape[1] // 8
    chunks = om.shape[0]
    cb = batch // chunks
    half = batch // 2
    scale2 = k_hbm.shape[2] ** -0.5 * math.log2(math.e)
    rep = lax.axis_index('rep')
    me = lax.axis_index('seq')
    chip, core = me // CORES, me % CORES
    base = me * local_len
    quarter = (chip % 2) * CORES + core

    def dev(c, e):
        return (rep, lax.rem(c, chips) * CORES + e)

    partner = dev(chip, 1 - core)
    ncols = 256
    lx = pltpu.make_async_copy(x_hbm, x_v, lsem.at[0])
    hd = wbuf.shape[1] // 2
    lw = [[pltpu.make_async_copy(wq_hbm.at[pl.ds(n * hd, hd), pl.ds(pl.multiple_of(quarter * 1024 + i * 512, 512), 512)],
                                 wbuf.at[i, pl.ds(n * hd, hd)], lsem.at[1 + i * 2 + n]) for n in range(2)] for i in range(2)]
    lk = pltpu.make_async_copy(wk_hbm.at[:, pl.ds(pl.multiple_of(quarter * ncols, ncols), ncols)], wbuf.at[2, :, pl.ds(0, ncols)], lsem.at[5])
    lv = pltpu.make_async_copy(wv_hbm.at[:, pl.ds(pl.multiple_of(quarter * ncols, ncols), ncols)], wbuf.at[2, :, pl.ds(ncols, ncols)], lsem.at[6])
    lo = pltpu.make_async_copy(wo_hbm, wo_v, lsem.at[7])
    lkc = [pltpu.make_async_copy(k_hbm.at[pl.ds(i * cb, cb)], kout.at[pl.ds(i * cb, cb)], kvsem.at[0, i]) for i in range(chunks)]
    lvc = [pltpu.make_async_copy(v_hbm.at[pl.ds(i * cb, cb)], vout.at[pl.ds(i * cb, cb)], kvsem.at[1, i]) for i in range(chunks)]
    lx.start()
    for i in range(2):
        for n in range(2):
            lw[i][n].start()

    barrier = pltpu.get_barrier_semaphore()
    for d in range(chips):
        for f in range(CORES):
            if d or f:
                pl.semaphore_signal(barrier, inc=1, device_id=dev(chip + d, lax.rem(core + f, CORES)), device_id_type=MESH)

    lane_b = (lax.broadcasted_iota(jnp.int32, pos2_ref.shape, 1) + lax.broadcasted_iota(jnp.int32, pos2_ref.shape, 0) * pos2_ref.shape[1]) // 2
    pv = jnp.zeros(pos2_ref.shape, jnp.int32)
    for b in range(batch):
        pv = jnp.where(lane_b == b, pos_ref[b], pv)
    pos2_ref[...] = pv

    lx.wait()
    for i in range(2):
        with jax.named_scope(f'wa{i}'):
            lw[i][0].wait()
        q = jnp.dot(x_v[:, :hd], wbuf[i, :hd], preferred_element_type=F32)
        with jax.named_scope(f'wb{i}'):
            lw[i][1].wait()
        if i == 0:
            lk.start()
            lv.start()
        q = q + jnp.dot(x_v[:, hd:], wbuf[i, hd:], preferred_element_type=F32)
        for h in range(4):
            qs[pl.ds(i * 4 + h, batch, stride=8), :] = q[:, h * 128:(h + 1) * 128]
    q_all[quarter] = qs[...].astype(BF16)
    with jax.named_scope('barrier'):
        pl.semaphore_wait(barrier, chips * CORES - 1)

    def spread(buf, rows, ss, rs):
        copies = [pltpu.make_async_remote_copy(buf.at[quarter], buf.at[quarter], ss.at[0], rs.at[0], device_id=partner, device_id_type=MESH)]
        for side, shift in ((0, 1), (1, chips - 1)):
            part = pl.ds(side * rows // 2, rows // 2)
            copies.append(pltpu.make_async_remote_copy(
                buf.at[quarter, part], buf.at[quarter, part], ss.at[1 + side], rs.at[1 + side], device_id=dev(chip + shift, core), device_id_type=MESH))
        return copies

    def hand_on(copies, buf, rows, ss, rs):
        other = ((chip + 1) % 2) * CORES + core
        for side in range(2):
            copies[1 + side].wait_recv()
            part = pl.ds(side * rows // 2, rows // 2)
            c = pltpu.make_async_remote_copy(buf.at[other, part], buf.at[other, part], ss.at[3 + side], rs.at[3 + side], device_id=partner, device_id_type=MESH)
            c.start()
            copies.append(c)

    def arrive(copies):
        copies[0].wait_recv()
        copies[3].wait_recv()
        copies[4].wait_recv()

    q_copies = spread(q_all, batch * 8, q_ss, q_rs)
    for c in q_copies:
        c.start()
    lkc[0].start()
    lvc[0].start()
    with jax.named_scope('wkvwait'):
        lk.wait()
        lv.wait()
    kv = jnp.dot(x_v[...], wbuf[2], preferred_element_type=F32)
    for w in range(2):
        for k in range(2):
            qs[pl.ds(w * 128 + k, batch, stride=2), :] = kv[:, w * 256 + k * 128:w * 256 + (k + 1) * 128]
    for hf in range(2):
        for w in range(2):
            kv_all[quarter, hf * 128 + w * 64:hf * 128 + w * 64 + 64, :] = qs[w * 128 + hf * 64:w * 128 + hf * 64 + 64, :].astype(BF16)
    n_copies = spread(kv_all, batch * 4, n_ss, n_rs)
    for c in n_copies:
        c.start()
    rowb = lax.broadcasted_iota(jnp.int32, (64, 128), 0) // 8 % 2
    bm0 = jnp.where(rowb == 0, 1.0, 0.0).astype(BF16)
    bm1 = jnp.where(rowb == 1, 1.0, 0.0).astype(BF16)

    with jax.named_scope('handq'):
        hand_on(q_copies, q_all, batch * 8, q_ss, q_rs)
    for i in range(1, chunks):
        lkc[i].start()
        lvc[i].start()
    lo.start()
    with jax.named_scope('handn'):
        hand_on(n_copies, kv_all, batch * 4, n_ss, n_rs)
    with jax.named_scope('arrq'):
        arrive(q_copies)

    qlane = lax.broadcasted_iota(jnp.int32, (8, 128), 1)
    own_head = lax.broadcasted_iota(jnp.int32, (8, 128), 0) == (qlane % 64) // 16 * 2 + (qlane % 8) // 4
    qseq = qlane // 64 * 2 + (qlane // 8) % 2
    mt_ref[...] = jnp.zeros_like(mt_ref)

    def scores(qi, buf):
        zero = jnp.zeros((64, 256), BF16)
        rows = []
        for ph in range(2):
            p0 = (2 * qi + ph) * 16
            q = jnp.concatenate([q_all[t, p0:p0 + 16, :] for t in range(4)], axis=0)
            blocks = [q * bm0, q * bm1]
            rows.append(jnp.concatenate(blocks + [zero] if ph == 0 else [zero] + blocks, axis=1))
        kc = jnp.concatenate([kout[4 * qi + j] for j in range(4)], axis=1)
        s = lax.dot_general(kc, jnp.concatenate(rows, axis=0), NT, preferred_element_type=F32).reshape(local_len, 8, 128)
        lim = jnp.full((8, 128), -1, jnp.int32)
        for j in range(4):
            lim = jnp.where(own_head & (qseq == j), pos_ref[4 * qi + j] - base, lim)
        s = jnp.where(lax.broadcasted_iota(jnp.int32, s.shape, 0) < lim[None], s, -jnp.inf)
        buf[...] = s.reshape(buf.shape)
        return jnp.maximum(jnp.max(jnp.max(s, axis=0), axis=0, keepdims=True), NEG)

    def weigh(qi, buf, m):
        p = jnp.exp2((buf[...] - m) * scale2)
        quad = qi % (cb // 4)
        mt_ref[0, quad:quad + 1, :] = m
        mt_ref[1, quad:quad + 1, :] = jnp.sum(p, axis=0, keepdims=True)
        pt = p.astype(BF16).T
        for ph in range(2):
            b0 = 4 * qi + 2 * ph
            vc = jnp.concatenate([vout[b0], vout[b0 + 1]], axis=1)
            o = jnp.dot(pt[ph * 64:(ph + 1) * 64, :], vc, preferred_element_type=F32)
            for t in range(4):
                for b in range(2):
                    r0 = (b0 % cb + b) * 8
                    oraw[t, r0:r0 + 8, :] = o[t * 16 + b * 8:t * 16 + b * 8 + 8, b * 128:(b + 1) * 128]

    rows_c = cb * 8
    carry = {}

    def attend(k):
        if k == 0:
            lkc[0].wait()
            carry['m'] = scores(0, sa)
        elif k % 2 == 1 and k < 2 * chunks - 1:
            lkc[(k + 1) // 2].wait()
        if k % 2 == 0:
            lvc[k // 2].wait()
        m_b = scores(2 * k + 1, sb)
        weigh(2 * k, sa, carry['m'])
        if k < 2 * chunks - 1:
            carry['m'] = scores(2 * k + 2, sa)
        weigh(2 * k + 1, sb, m_b)

    lane = lax.broadcasted_iota(jnp.int32, (8, 128), 1)
    od, oi, yd, yi, ag = {}, {}, {}, {}, {}

    def finalize(i):
        hf = i * cb // half
        first = i * rows_c - hf * half * 8
        rr = lax.broadcasted_iota(jnp.int32, (rows_c, 64), 0) + first
        cc = lax.broadcasted_iota(jnp.int32, (rows_c, 64), 1)
        rel = pos2_ref[hf:hf + 1, :] - base
        keep = (rr // 4 == cc) & (rel >= 0) & (rel < local_len)
        mt, lt = mt_ref[0].T, mt_ref[1].T

        def by_row(x, t):
            return jnp.concatenate([jnp.broadcast_to(x[(p % 2) * 64 + t * 16:(p % 2) * 64 + t * 16 + 16, p // 2:p // 2 + 1], (16, 128))
                                    for p in range(cb // 2)], axis=0)

        quarters = range(4)
        sn = [lax.dot_general(q_all[t, i * rows_c:(i + 1) * rows_c, :], kv_all[t, hf * 128:hf * 128 + 64, :], NT, preferred_element_type=F32) for t in quarters]
        mo = [by_row(mt, t) for t in quarters]
        lo_ = [by_row(lt, t) for t in quarters]
        sn = [jnp.where(keep, x, -jnp.inf) for x in sn]
        top = [jnp.max(x, axis=1, keepdims=True) for x in sn]
        mn = [jnp.maximum(x, y) for x, y in zip(mo, top)]
        pn = [jnp.exp2((x - y[:, :64]) * scale2) for x, y in zip(sn, mn)]
        on = [jnp.dot(pn[t].astype(BF16), kv_all[t, hf * 128 + 64:hf * 128 + 128, :], preferred_element_type=F32) for t in quarters]
        ln = [jnp.sum(x, axis=1, keepdims=True) for x in pn]
        for t in quarters:
            w = jnp.exp2((mo[t] - mn[t]) * scale2)
            mraw[t] = mn[t]
            lraw[t] = lo_[t] * w + ln[t]
            oraw[t] = oraw[t] * w + on[t]
        for e in range(CORES):
            for t in range(4):
                mp = jnp.zeros((8, 128), F32)
                lp = jnp.zeros((8, 128), F32)
                for h in range(4):
                    src = pl.ds(e * 4 + h, cb, stride=8)
                    om[i, e, t, h * cb:(h + 1) * cb, :] = oraw[t, src, :]
                    mh = mraw[t, src, :]
                    lh = lraw[t, src, :]
                    for g in range(cb // 8):
                        sel = lane == h * (cb // 8) + g
                        mp = jnp.where(sel, mh[g * 8:(g + 1) * 8], mp)
                        lp = jnp.where(sel, lh[g * 8:(g + 1) * 8], lp)
                om[i, e, t, cb * 4:cb * 4 + 8, :] = mp
                om[i, e, t, cb * 4 + 8:cb * 4 + 16, :] = lp
        od[i] = pltpu.make_async_remote_copy(om.at[i, 1 - core], op.at[i], od_s.at[i], od_r.at[i], device_id=partner, device_id_type=MESH)
        od[i].start()

    nrow = cb * 4

    def merge(parts):
        ms = [p[nrow:nrow + 8] for p in parts]
        m = functools.reduce(jnp.maximum, ms)
        ws = [jnp.exp2((x - m) * scale2) for x in ms]
        l = functools.reduce(jnp.add, [w * p[nrow + 8:nrow + 16] for w, p in zip(ws, parts)])
        return m, l, ws

    def chip_reduce(i):
        od[i].wait_recv()
        for t in range(4):
            fold(om.at[i, core, t], om[i, core, t], op[i, t])
        oi[i] = []
        for d in range(1, chips):
            c = pltpu.make_async_remote_copy(om.at[i, core, lax.rem(chip + d, chips)], orecv.at[i, d - 1], oi_s.at[i, d - 1], oi_r.at[i, d - 1],
                                             device_id=dev(chip + d, core), device_id_type=MESH)
            c.start()
            oi[i].append(c)

    def fold(dst, a, b):
        m, l, (wa, wb) = merge([a, b])
        for g in range(nrow // 8):
            r = slice(g * 8, g * 8 + 8)
            dst[g * 8:g * 8 + 8, :] = a[r] * wa[:, g:g + 1] + b[r] * wb[:, g:g + 1]
        dst[nrow:nrow + 8, :] = m
        dst[nrow + 8:nrow + 16, :] = l

    def project(i):
        for c in oi[i]:
            c.wait_recv()
        if i == 0:
            lo.wait()
        parts = [om[i, core, chip]] + [orecv[i, d] for d in range(chips - 1)]
        m, l, ws = merge(parts)
        rl = 1.0 / l
        heads = []
        for h in range(4):
            rows = []
            for g in range(h * (cb // 8), (h + 1) * (cb // 8)):
                o = functools.reduce(jnp.add, [p[g * 8:g * 8 + 8] * w[:, g:g + 1] for p, w in zip(parts, ws)])
                rows.append(o * rl[:, g:g + 1])
            heads.append(jnp.concatenate(rows, axis=0).astype(BF16))
        lhs = jnp.concatenate(heads, axis=1)
        for e in range(CORES):
            for t in range(4):
                c0 = (e * 4 + t) * 512
                ys[i, e, t] = jnp.dot(lhs, wo_v[:, c0:c0 + 512], preferred_element_type=F32)
        yd[i] = pltpu.make_async_remote_copy(ys.at[i, 1 - core], yp.at[i], yd_s.at[i], yd_r.at[i], device_id=partner, device_id_type=MESH)
        yd[i].start()

    def y_chip(i):
        yd[i].wait_recv()
        ys[i, core] = ys[i, core] + yp[i]
        yi[i] = []
        for d in range(1, chips):
            c = pltpu.make_async_remote_copy(ys.at[i, core, lax.rem(chip + d, chips)], yr.at[i, d - 1], yi_s.at[i, d - 1], yi_r.at[i, d - 1],
                                             device_id=dev(chip + d, core), device_id_type=MESH)
            c.start()
            yi[i].append(c)

    def block(i, c):
        return (pl.ds(i * cb, cb), pl.ds(pl.multiple_of((core * 4 + c) * 512, 512), 512))

    def lay_rows():
        for w in range(2):
            for t in range(4):
                for hf in range(2):
                    sa[:64, :] = kv_all[t, hf * 128 + w * 64:hf * 128 + w * 64 + 64, :].astype(F32)
                    for k in range(2):
                        qs[pl.ds(hf * half * 8 + t * 2 + k, half, stride=8), :] = sa[pl.ds(k, half, stride=2), :]
            rows_ref[w] = qs[...].astype(BF16)

    def y_final(i):
        if i == chunks - 1:
            lay_rows()
        for c in yi[i]:
            c.wait_recv()
        y = ys[i, core, chip]
        for d in range(chips - 1):
            y = y + yr[i, d]
        yfull[block(i, chip)] = y.astype(BF16)
        ag[i] = []
        if i == chunks - 1:
            for d in range(chips):
                for f in range(CORES):
                    if d or f:
                        push(i, chip, dev(chip + d, lax.rem(core + f, CORES)))
        else:
            for d in range(1, chips):
                push(i, chip, dev(chip + d, core))
            push(i, chip, partner)

    def push(i, c, target):
        slot = len(ag[i])
        cp = pltpu.make_async_remote_copy(yfull.at[block(i, c)], yfull.at[block(i, c)], ag_s.at[i, slot], ag_r.at[i, slot], device_id=target, device_id_type=MESH)
        cp.start()
        ag[i].append(cp)

    def pass_on(i):
        for d in range(1, chips):
            ag[i][d - 1].wait_recv()
            push(i, lax.rem(chip + chips - d, chips), partner)

    plan = {1: [(finalize, 0)], 2: [(chip_reduce, 0)], 3: [(finalize, 1)], 4: [(chip_reduce, 1), (project, 0)],
            5: [(finalize, 2), (y_chip, 0)], 6: [(chip_reduce, 2), (project, 1)],
            7: [(finalize, 3), (y_chip, 1), (chip_reduce, 3), (y_final, 0), (project, 2), (y_chip, 2), (y_final, 1), (project, 3), (pass_on, 0),
                (y_chip, 3), (y_final, 2), (pass_on, 1), (y_final, 3), (pass_on, 2)]}
    for k in range(max(plan) + 1):
        if k < 2 * chunks:
            with jax.named_scope(f'att{k}'):
                attend(k)
        if k == 1:
            arrive(n_copies)
        for stage, i in plan.get(k, ()):
            with jax.named_scope(f'{stage.__name__}{i}'):
                stage(i)
    with jax.named_scope('agwait'):
        for i in range(chunks):
            for c in ag[i] if i == chunks - 1 else ag[i][chips - 1:]:
                c.wait_recv()
    with jax.named_scope('sendwait'):
        for c in q_copies + n_copies:
            c.wait_send()
        for i in range(chunks):
            for c in [od[i], yd[i]] + oi[i] + yi[i] + ag[i]:
                c.wait_send()


def write_kernel(which, k_in, new_ref, pos_ref, *refs):
    if which == 0:
        y_ref, k_out, k_ref, y_out, bsem, ysem = refs
        cy = pltpu.make_async_copy(y_ref, y_out, ysem)
    else:
        k_out, k_ref, bsem, ysem = refs
    batch, local_len = k_ref.shape[0], k_ref.shape[1] // 8
    base = lax.axis_index('seq') * local_len
    pieces = bsem.shape[0]
    pb = batch // pieces
    bulk = []
    for i in range(pieces):
        @pl.loop(i * pb, (i + 1) * pb)
        def _(b):
            rel = pos_ref[b] - base

            @pl.when((rel >= 0) & (rel < local_len))
            def _():
                k_ref[b, pl.ds(pl.multiple_of(rel * 8, 8), 8), :] = new_ref[which, pl.ds(pl.multiple_of(b * 8, 8), 8), :]
        part = pl.ds(i * pb, pb)
        c = pltpu.make_async_copy(k_ref.at[part], k_out.at[part], bsem.at[i])
        c.start()
        bulk.append(c)
    if which == 0:
        cy.start()
        bulk.append(cy)
    for c in bulk:
        c.wait()


def solution(mesh):
    cache_spec = P('rep', 'seq', None, None)
    in_specs = (P('rep', None), P(), P(), P(), P('seq', None), cache_spec, cache_spec, P('rep'))
    out_specs = (P('rep', None), cache_spec, cache_spec)
    chips = mesh.shape['seq'] // CORES
    assert chips == 4
    vm = pl.BlockSpec(memory_space=pltpu.VMEM)
    hbm = pl.BlockSpec(memory_space=pl.ANY)
    sm = pl.BlockSpec(memory_space=pltpu.SMEM)

    def local_step(x, wq, wk, wv, wo, k, v, pos):
        shape4 = k.shape
        batch, width = x.shape
        k3 = k.reshape(batch, -1, k.shape[-1])
        v3 = v.reshape(k3.shape)
        chunks = 4
        cb = batch // chunks
        dma = pltpu.SemaphoreType.DMA
        in_hbm = lambda a: pltpu.with_memory_space_constraint(a, pltpu.HBM)
        in_vmem = lambda a: pltpu.with_memory_space_constraint(a, pltpu.VMEM)
        y, ko, vo, new = pl.pallas_call(
            functools.partial(step_kernel, chips),
            out_shape=(pltpu.VMEM((batch, wo.shape[1]), BF16), pltpu.VMEM(k3.shape, BF16), pltpu.VMEM(k3.shape, BF16),
                       pltpu.VMEM((2, batch * 8, 128), BF16)),
            in_specs=[hbm] * 7 + [sm],
            out_specs=[vm] * 4,
            scratch_shapes=[
                pltpu.VMEM((batch, width), BF16), pltpu.VMEM((3, width, 512), BF16), pltpu.VMEM(wo.shape, BF16),
                pltpu.VMEM((batch * 8, 128), F32), pltpu.VMEM((4, batch * 8, 128), BF16), pltpu.VMEM((4, batch * 4, 128), BF16), pltpu.VMEM((k3.shape[1], 128), F32), pltpu.VMEM((k3.shape[1], 128), F32), pltpu.VMEM((2, 8, 128), F32), pltpu.VMEM((2, batch), jnp.int32),
                pltpu.VMEM((4, cb * 8, 128), F32), pltpu.VMEM((4, cb * 8, 128), F32), pltpu.VMEM((4, cb * 8, 128), F32),
                pltpu.VMEM((chunks, CORES, 4, cb * 4 + 16, 128), F32), pltpu.VMEM((chunks, 4, cb * 4 + 16, 128), F32),
                pltpu.VMEM((chunks, chips - 1, cb * 4 + 16, 128), F32),
                pltpu.VMEM((chunks, CORES, 4, cb, 512), F32), pltpu.VMEM((chunks, 4, cb, 512), F32), pltpu.VMEM((chunks, chips - 1, cb, 512), F32),
                dma((8,)), dma((2, chunks)), dma((5,)), dma((5,)), dma((5,)), dma((5,)), dma((chunks,)), dma((chunks,)),
                dma((chunks, chips - 1)), dma((chunks, chips - 1)), dma((chunks,)), dma((chunks,)),
                dma((chunks, chips - 1)), dma((chunks, chips - 1)), dma((chunks, chips * CORES - 1)), dma((chunks, chips * CORES - 1))],
            compiler_params=pltpu.CompilerParams(collective_id=0, has_side_effects=True, vmem_limit_bytes=29 << 20),
            name='step',
        )(in_hbm(x), in_hbm(wq), in_hbm(wk), in_hbm(wv), in_hbm(wo), in_hbm(k3), in_hbm(v3), pos)

        def write(which, cache, pieces, *extra):
            return pl.pallas_call(
                functools.partial(write_kernel, which),
                out_shape=(jax.ShapeDtypeStruct(k3.shape, BF16), pltpu.VMEM(k3.shape, BF16), *(jax.ShapeDtypeStruct(e.shape, BF16) for e in extra)),
                in_specs=[vm, vm, sm] + [vm] * len(extra),
                out_specs=[hbm, vm] + [hbm] * len(extra),
                scratch_shapes=[dma((pieces,)), dma],
                input_output_aliases={0: 1},
                compiler_params=pltpu.CompilerParams(vmem_limit_bytes=4 << 20),
                name='write',
            )(in_vmem(cache), in_vmem(new), pos, *(in_vmem(e) for e in extra))
        ko, _, y = write(0, ko, 4, y)
        vo, _ = write(1, vo, 16)
        return y, ko.reshape(shape4), vo.reshape(shape4)

    return jax.shard_map(local_step, mesh=mesh, in_specs=in_specs, out_specs=out_specs, check_vma=False)
```

```python
import functools
import math

import jax
import jax.numpy as jnp
from jax import lax
from jax.experimental import pallas as pl
from jax.experimental.pallas import tpu as pltpu
from jax.sharding import PartitionSpec as P

MESH = pl.DeviceIdType.MESH
NEG = -3.4028234e38
F32, BF16 = jnp.float32, jnp.bfloat16
CORES = 2
NT = (((1,), (1,)), ((), ()))


def step_kernel(chips, x_hbm, wq_hbm, wk_hbm, wv_hbm, wo_hbm, k_hbm, v_hbm, pos_ref,
                yfull, kout, vout, rows_ref,
                x_v, wbuf, wo_v, qs, q_all, kv_all, sa, sb, mt_ref, pos2_ref, oraw, mraw, lraw, om, op, orecv,
                ys, yp, yr,
                lsem, kvsem, q_ss, q_rs, n_ss, n_rs, od_s, od_r, oi_s, oi_r, yd_s, yd_r, yi_s, yi_r, ag_s, ag_r):
    batch = k_hbm.shape[0]
    local_len = k_hbm.shape[1] // 8
    chunks = om.shape[0]
    cb = batch // chunks
    half = batch // 2
    scale2 = k_hbm.shape[2] ** -0.5 * math.log2(math.e)
    rep = lax.axis_index('rep')
    me = lax.axis_index('seq')
    chip, core = me // CORES, me % CORES
    base = me * local_len
    quarter = (chip % 2) * CORES + core

    def dev(c, e):
        return (rep, lax.rem(c, chips) * CORES + e)

    partner = dev(chip, 1 - core)
    ncols = 256
    lx = pltpu.make_async_copy(x_hbm, x_v, lsem.at[0])
    hd = wbuf.shape[1] // 2
    lw = [[pltpu.make_async_copy(wq_hbm.at[pl.ds(n * hd, hd), pl.ds(pl.multiple_of(quarter * 1024 + i * 512, 512), 512)],
                                 wbuf.at[i, pl.ds(n * hd, hd)], lsem.at[1 + i * 2 + n]) for n in range(2)] for i in range(2)]
    lk = pltpu.make_async_copy(wk_hbm.at[:, pl.ds(pl.multiple_of(quarter * ncols, ncols), ncols)], wbuf.at[2, :, pl.ds(0, ncols)], lsem.at[5])
    lv = pltpu.make_async_copy(wv_hbm.at[:, pl.ds(pl.multiple_of(quarter * ncols, ncols), ncols)], wbuf.at[2, :, pl.ds(ncols, ncols)], lsem.at[6])
    lo = pltpu.make_async_copy(wo_hbm, wo_v, lsem.at[7])
    lkc = [pltpu.make_async_copy(k_hbm.at[pl.ds(i * cb, cb)], kout.at[pl.ds(i * cb, cb)], kvsem.at[0, i]) for i in range(chunks)]
    lvc = [pltpu.make_async_copy(v_hbm.at[pl.ds(i * cb, cb)], vout.at[pl.ds(i * cb, cb)], kvsem.at[1, i]) for i in range(chunks)]
    lx.start()
    for i in range(2):
        for n in range(2):
            lw[i][n].start()

    barrier = pltpu.get_barrier_semaphore()
    for d in range(chips):
        for f in range(CORES):
            if d or f:
                pl.semaphore_signal(barrier, inc=1, device_id=dev(chip + d, lax.rem(core + f, CORES)), device_id_type=MESH)

    lane_b = (lax.broadcasted_iota(jnp.int32, pos2_ref.shape, 1) + lax.broadcasted_iota(jnp.int32, pos2_ref.shape, 0) * pos2_ref.shape[1]) // 2
    pv = jnp.zeros(pos2_ref.shape, jnp.int32)
    for b in range(batch):
        pv = jnp.where(lane_b == b, pos_ref[b], pv)
    pos2_ref[...] = pv

    lx.wait()
    for i in range(2):
        lw[i][0].wait()
        q = jnp.dot(x_v[:, :hd], wbuf[i, :hd], preferred_element_type=F32)
        lw[i][1].wait()
        if i == 0:
            lk.start()
            lv.start()
        q = q + jnp.dot(x_v[:, hd:], wbuf[i, hd:], preferred_element_type=F32)
        for h in range(4):
            qs[pl.ds(i * 4 + h, batch, stride=8), :] = q[:, h * 128:(h + 1) * 128]
    q_all[quarter] = qs[...].astype(BF16)
    pl.semaphore_wait(barrier, chips * CORES - 1)

    def spread(buf, rows, ss, rs):
        copies = [pltpu.make_async_remote_copy(buf.at[quarter], buf.at[quarter], ss.at[0], rs.at[0], device_id=partner, device_id_type=MESH)]
        for side, shift in ((0, 1), (1, chips - 1)):
            part = pl.ds(side * rows // 2, rows // 2)
            copies.append(pltpu.make_async_remote_copy(
                buf.at[quarter, part], buf.at[quarter, part], ss.at[1 + side], rs.at[1 + side], device_id=dev(chip + shift, core), device_id_type=MESH))
        return copies

    def hand_on(copies, buf, rows, ss, rs):
        other = ((chip + 1) % 2) * CORES + core
        for side in range(2):
            copies[1 + side].wait_recv()
            part = pl.ds(side * rows // 2, rows // 2)
            c = pltpu.make_async_remote_copy(buf.at[other, part], buf.at[other, part], ss.at[3 + side], rs.at[3 + side], device_id=partner, device_id_type=MESH)
            c.start()
            copies.append(c)

    def arrive(copies):
        copies[0].wait_recv()
        copies[3].wait_recv()
        copies[4].wait_recv()

    q_copies = spread(q_all, batch * 8, q_ss, q_rs)
    for c in q_copies:
        c.start()
    lkc[0].start()
    lvc[0].start()
    lk.wait()
    lv.wait()
    kv = jnp.dot(x_v[...], wbuf[2], preferred_element_type=F32)
    for w in range(2):
        for k in range(2):
            qs[pl.ds(w * 128 + k, batch, stride=2), :] = kv[:, w * 256 + k * 128:w * 256 + (k + 1) * 128]
    for hf in range(2):
        for w in range(2):
            kv_all[quarter, hf * 128 + w * 64:hf * 128 + w * 64 + 64, :] = qs[w * 128 + hf * 64:w * 128 + hf * 64 + 64, :].astype(BF16)
    n_copies = spread(kv_all, batch * 4, n_ss, n_rs)
    for c in n_copies:
        c.start()
    rowb = lax.broadcasted_iota(jnp.int32, (64, 128), 0) // 8 % 2
    bm0 = jnp.where(rowb == 0, 1.0, 0.0).astype(BF16)
    bm1 = jnp.where(rowb == 1, 1.0, 0.0).astype(BF16)

    hand_on(q_copies, q_all, batch * 8, q_ss, q_rs)
    for i in range(1, chunks):
        lkc[i].start()
        lvc[i].start()
    lo.start()
    hand_on(n_copies, kv_all, batch * 4, n_ss, n_rs)
    arrive(q_copies)

    qlane = lax.broadcasted_iota(jnp.int32, (8, 128), 1)
    own_head = lax.broadcasted_iota(jnp.int32, (8, 128), 0) == (qlane % 64) // 16 * 2 + (qlane % 8) // 4
    qseq = qlane // 64 * 2 + (qlane // 8) % 2
    mt_ref[...] = jnp.zeros_like(mt_ref)

    def scores(qi, buf):
        zero = jnp.zeros((64, 256), BF16)
        rows = []
        for ph in range(2):
            p0 = (2 * qi + ph) * 16
            q = jnp.concatenate([q_all[t, p0:p0 + 16, :] for t in range(4)], axis=0)
            blocks = [q * bm0, q * bm1]
            rows.append(jnp.concatenate(blocks + [zero] if ph == 0 else [zero] + blocks, axis=1))
        kc = jnp.concatenate([kout[4 * qi + j] for j in range(4)], axis=1)
        s = lax.dot_general(kc, jnp.concatenate(rows, axis=0), NT, preferred_element_type=F32).reshape(local_len, 8, 128)
        lim = jnp.full((8, 128), -1, jnp.int32)
        for j in range(4):
            lim = jnp.where(own_head & (qseq == j), pos_ref[4 * qi + j] - base, lim)
        s = jnp.where(lax.broadcasted_iota(jnp.int32, s.shape, 0) < lim[None], s, -jnp.inf)
        buf[...] = s.reshape(buf.shape)
        return jnp.maximum(jnp.max(jnp.max(s, axis=0), axis=0, keepdims=True), NEG)

    def weigh(qi, buf, m):
        p = jnp.exp2((buf[...] - m) * scale2)
        quad = qi % (cb // 4)
        mt_ref[0, quad:quad + 1, :] = m
        mt_ref[1, quad:quad + 1, :] = jnp.sum(p, axis=0, keepdims=True)
        pt = p.astype(BF16).T
        for ph in range(2):
            b0 = 4 * qi + 2 * ph
            vc = jnp.concatenate([vout[b0], vout[b0 + 1]], axis=1)
            o = jnp.dot(pt[ph * 64:(ph + 1) * 64, :], vc, preferred_element_type=F32)
            for t in range(4):
                for b in range(2):
                    r0 = (b0 % cb + b) * 8
                    oraw[t, r0:r0 + 8, :] = o[t * 16 + b * 8:t * 16 + b * 8 + 8, b * 128:(b + 1) * 128]

    rows_c = cb * 8
    carry = {}

    def attend(k):
        if k == 0:
            lkc[0].wait()
            carry['m'] = scores(0, sa)
        elif k % 2 == 1 and k < 2 * chunks - 1:
            lkc[(k + 1) // 2].wait()
        if k % 2 == 0:
            lvc[k // 2].wait()
        m_b = scores(2 * k + 1, sb)
        weigh(2 * k, sa, carry['m'])
        if k < 2 * chunks - 1:
            carry['m'] = scores(2 * k + 2, sa)
        weigh(2 * k + 1, sb, m_b)

    lane = lax.broadcasted_iota(jnp.int32, (8, 128), 1)
    od, oi, yd, yi, ag = {}, {}, {}, {}, {}

    def finalize(i):
        hf = i * cb // half
        first = i * rows_c - hf * half * 8
        rr = lax.broadcasted_iota(jnp.int32, (rows_c, 64), 0) + first
        cc = lax.broadcasted_iota(jnp.int32, (rows_c, 64), 1)
        rel = pos2_ref[hf:hf + 1, :] - base
        keep = (rr // 4 == cc) & (rel >= 0) & (rel < local_len)
        mt, lt = mt_ref[0].T, mt_ref[1].T

        def by_row(x, t):
            return jnp.concatenate([jnp.broadcast_to(x[(p % 2) * 64 + t * 16:(p % 2) * 64 + t * 16 + 16, p // 2:p // 2 + 1], (16, 128))
                                    for p in range(cb // 2)], axis=0)

        quarters = range(4)
        sn = [lax.dot_general(q_all[t, i * rows_c:(i + 1) * rows_c, :], kv_all[t, hf * 128:hf * 128 + 64, :], NT, preferred_element_type=F32) for t in quarters]
        mo = [by_row(mt, t) for t in quarters]
        lo_ = [by_row(lt, t) for t in quarters]
        sn = [jnp.where(keep, x, -jnp.inf) for x in sn]
        top = [jnp.max(x, axis=1, keepdims=True) for x in sn]
        mn = [jnp.maximum(x, y) for x, y in zip(mo, top)]
        pn = [jnp.exp2((x - y[:, :64]) * scale2) for x, y in zip(sn, mn)]
        on = [jnp.dot(pn[t].astype(BF16), kv_all[t, hf * 128 + 64:hf * 128 + 128, :], preferred_element_type=F32) for t in quarters]
        ln = [jnp.sum(x, axis=1, keepdims=True) for x in pn]
        for t in quarters:
            w = jnp.exp2((mo[t] - mn[t]) * scale2)
            mraw[t] = mn[t]
            lraw[t] = lo_[t] * w + ln[t]
            oraw[t] = oraw[t] * w + on[t]
        for e in range(CORES):
            for t in range(4):
                mp = jnp.zeros((8, 128), F32)
                lp = jnp.zeros((8, 128), F32)
                for h in range(4):
                    src = pl.ds(e * 4 + h, cb, stride=8)
                    om[i, e, t, h * cb:(h + 1) * cb, :] = oraw[t, src, :]
                    mh = mraw[t, src, :]
                    lh = lraw[t, src, :]
                    for g in range(cb // 8):
                        sel = lane == h * (cb // 8) + g
                        mp = jnp.where(sel, mh[g * 8:(g + 1) * 8], mp)
                        lp = jnp.where(sel, lh[g * 8:(g + 1) * 8], lp)
                om[i, e, t, cb * 4:cb * 4 + 8, :] = mp
                om[i, e, t, cb * 4 + 8:cb * 4 + 16, :] = lp
        od[i] = pltpu.make_async_remote_copy(om.at[i, 1 - core], op.at[i], od_s.at[i], od_r.at[i], device_id=partner, device_id_type=MESH)
        od[i].start()

    nrow = cb * 4

    def merge(parts):
        ms = [p[nrow:nrow + 8] for p in parts]
        m = functools.reduce(jnp.maximum, ms)
        ws = [jnp.exp2((x - m) * scale2) for x in ms]
        l = functools.reduce(jnp.add, [w * p[nrow + 8:nrow + 16] for w, p in zip(ws, parts)])
        return m, l, ws

    def chip_reduce(i):
        od[i].wait_recv()
        for t in range(4):
            fold(om.at[i, core, t], om[i, core, t], op[i, t])
        oi[i] = []
        for d in range(1, chips):
            c = pltpu.make_async_remote_copy(om.at[i, core, lax.rem(chip + d, chips)], orecv.at[i, d - 1], oi_s.at[i, d - 1], oi_r.at[i, d - 1],
                                             device_id=dev(chip + d, core), device_id_type=MESH)
            c.start()
            oi[i].append(c)

    def fold(dst, a, b):
        m, l, (wa, wb) = merge([a, b])
        for g in range(nrow // 8):
            r = slice(g * 8, g * 8 + 8)
            dst[g * 8:g * 8 + 8, :] = a[r] * wa[:, g:g + 1] + b[r] * wb[:, g:g + 1]
        dst[nrow:nrow + 8, :] = m
        dst[nrow + 8:nrow + 16, :] = l

    groups = (tuple(range(chunks - 2)), (chunks - 2,), (chunks - 1,))

    def rows_of(g):
        return pl.ds(groups[g][0] * cb, len(groups[g]) * cb)

    def project(g):
        heads = [[] for _ in range(4)]
        for i in groups[g]:
            for c in oi[i]:
                c.wait_recv()
            parts = [om[i, core, chip]] + [orecv[i, d] for d in range(chips - 1)]
            m, l, ws = merge(parts)
            rl = 1.0 / l
            for h in range(4):
                rows = []
                for r in range(h * (cb // 8), (h + 1) * (cb // 8)):
                    o = functools.reduce(jnp.add, [p[r * 8:r * 8 + 8] * w[:, r:r + 1] for p, w in zip(parts, ws)])
                    rows.append(o * rl[:, r:r + 1])
                heads[h].append(jnp.concatenate(rows, axis=0).astype(BF16))
        if g == 0:
            lo.wait()
        lhs = jnp.concatenate([jnp.concatenate(h, axis=0) for h in heads], axis=1)
        for e in range(CORES):
            for t in range(4):
                c0 = (e * 4 + t) * 512
                ys[e, t, rows_of(g), :] = jnp.dot(lhs, wo_v[:, c0:c0 + 512], preferred_element_type=F32)
        yd[g] = pltpu.make_async_remote_copy(ys.at[1 - core, :, rows_of(g)], yp.at[:, rows_of(g)], yd_s.at[g], yd_r.at[g], device_id=partner, device_id_type=MESH)
        yd[g].start()

    def y_chip(g):
        yd[g].wait_recv()
        r = rows_of(g)
        for t in range(chips):
            ys[core, t, r, :] = ys[core, t, r, :] + yp[t, r, :]
        yi[g] = []
        for d in range(1, chips):
            c = pltpu.make_async_remote_copy(ys.at[core, lax.rem(chip + d, chips), r], yr.at[d - 1, r], yi_s.at[g, d - 1], yi_r.at[g, d - 1],
                                             device_id=dev(chip + d, core), device_id_type=MESH)
            c.start()
            yi[g].append(c)

    def block(g, c):
        return (rows_of(g), pl.ds(pl.multiple_of((core * 4 + c) * 512, 512), 512))

    def lay_rows():
        for w in range(2):
            for t in range(4):
                for hf in range(2):
                    sa[:64, :] = kv_all[t, hf * 128 + w * 64:hf * 128 + w * 64 + 64, :].astype(F32)
                    for k in range(2):
                        qs[pl.ds(hf * half * 8 + t * 2 + k, half, stride=8), :] = sa[pl.ds(k, half, stride=2), :]
            rows_ref[w] = qs[...].astype(BF16)

    def y_final(g):
        if g == len(groups) - 1:
            lay_rows()
        for c in yi[g]:
            c.wait_recv()
        r = rows_of(g)
        y = ys[core, chip, r, :]
        for d in range(chips - 1):
            y = y + yr[d, r, :]
        yfull[block(g, chip)] = y.astype(BF16)
        ag[g] = []
        if g == len(groups) - 1:
            for d in range(chips):
                for f in range(CORES):
                    if d or f:
                        push(g, chip, dev(chip + d, lax.rem(core + f, CORES)))
        else:
            for d in range(1, chips):
                push(g, chip, dev(chip + d, core))
            push(g, chip, partner)

    def push(g, c, target):
        slot = len(ag[g])
        cp = pltpu.make_async_remote_copy(yfull.at[block(g, c)], yfull.at[block(g, c)], ag_s.at[g, slot], ag_r.at[g, slot], device_id=target, device_id_type=MESH)
        cp.start()
        ag[g].append(cp)

    def pass_on(g):
        for d in range(1, chips):
            ag[g][d - 1].wait_recv()
            push(g, lax.rem(chip + chips - d, chips), partner)

    plan = {1: [(finalize, 0)], 2: [(chip_reduce, 0)], 3: [(finalize, 1)], 4: [(chip_reduce, 1)],
            5: [(finalize, 2), (project, 0)], 6: [(chip_reduce, 2), (y_chip, 0)],
            7: [(finalize, 3), (chip_reduce, 3), (project, 1), (y_final, 0), (y_chip, 1), (project, 2), (pass_on, 0),
                (y_chip, 2), (y_final, 1), (y_final, 2), (pass_on, 1)]}
    for k in range(max(plan) + 1):
        if k < 2 * chunks:
            attend(k)
        if k == 1:
            arrive(n_copies)
        for stage, i in plan.get(k, ()):
            stage(i)
    for g in range(len(groups)):
        for c in ag[g] if g == len(groups) - 1 else ag[g][chips - 1:]:
            c.wait_recv()
    for c in q_copies + n_copies:
        c.wait_send()
    for g in range(len(groups)):
        for c in [yd[g]] + yi[g] + ag[g]:
            c.wait_send()
    for i in range(chunks):
        for c in [od[i]] + oi[i]:
            c.wait_send()


def write_kernel(which, k_in, new_ref, pos_ref, *refs):
    if which == 0:
        y_ref, k_out, k_ref, y_out, bsem, ysem = refs
        cy = pltpu.make_async_copy(y_ref, y_out, ysem)
    else:
        k_out, k_ref, bsem, ysem = refs
    batch, local_len = k_ref.shape[0], k_ref.shape[1] // 8
    base = lax.axis_index('seq') * local_len
    pieces = bsem.shape[0]
    pb = batch // pieces
    bulk = []
    for i in range(pieces):
        @pl.loop(i * pb, (i + 1) * pb)
        def _(b):
            rel = pos_ref[b] - base

            @pl.when((rel >= 0) & (rel < local_len))
            def _():
                k_ref[b, pl.ds(pl.multiple_of(rel * 8, 8), 8), :] = new_ref[which, pl.ds(pl.multiple_of(b * 8, 8), 8), :]
        part = pl.ds(i * pb, pb)
        c = pltpu.make_async_copy(k_ref.at[part], k_out.at[part], bsem.at[i])
        c.start()
        bulk.append(c)
    if which == 0:
        cy.start()
        bulk.append(cy)
    for c in bulk:
        c.wait()


def solution(mesh):
    cache_spec = P('rep', 'seq', None, None)
    in_specs = (P('rep', None), P(), P(), P(), P('seq', None), cache_spec, cache_spec, P('rep'))
    out_specs = (P('rep', None), cache_spec, cache_spec)
    chips = mesh.shape['seq'] // CORES
    assert chips == 4
    vm = pl.BlockSpec(memory_space=pltpu.VMEM)
    hbm = pl.BlockSpec(memory_space=pl.ANY)
    sm = pl.BlockSpec(memory_space=pltpu.SMEM)

    def local_step(x, wq, wk, wv, wo, k, v, pos):
        shape4 = k.shape
        batch, width = x.shape
        k3 = k.reshape(batch, -1, k.shape[-1])
        v3 = v.reshape(k3.shape)
        chunks = 4
        cb = batch // chunks
        dma = pltpu.SemaphoreType.DMA
        in_hbm = lambda a: pltpu.with_memory_space_constraint(a, pltpu.HBM)
        in_vmem = lambda a: pltpu.with_memory_space_constraint(a, pltpu.VMEM)
        y, ko, vo, new = pl.pallas_call(
            functools.partial(step_kernel, chips),
            out_shape=(pltpu.VMEM((batch, wo.shape[1]), BF16), pltpu.VMEM(k3.shape, BF16), pltpu.VMEM(k3.shape, BF16),
                       pltpu.VMEM((2, batch * 8, 128), BF16)),
            in_specs=[hbm] * 7 + [sm],
            out_specs=[vm] * 4,
            scratch_shapes=[
                pltpu.VMEM((batch, width), BF16), pltpu.VMEM((3, width, 512), BF16), pltpu.VMEM(wo.shape, BF16),
                pltpu.VMEM((batch * 8, 128), F32), pltpu.VMEM((4, batch * 8, 128), BF16), pltpu.VMEM((4, batch * 4, 128), BF16), pltpu.VMEM((k3.shape[1], 128), F32), pltpu.VMEM((k3.shape[1], 128), F32), pltpu.VMEM((2, 8, 128), F32), pltpu.VMEM((2, batch), jnp.int32),
                pltpu.VMEM((4, cb * 8, 128), F32), pltpu.VMEM((4, cb * 8, 128), F32), pltpu.VMEM((4, cb * 8, 128), F32),
                pltpu.VMEM((chunks, CORES, 4, cb * 4 + 16, 128), F32), pltpu.VMEM((chunks, 4, cb * 4 + 16, 128), F32),
                pltpu.VMEM((chunks, chips - 1, cb * 4 + 16, 128), F32),
                pltpu.VMEM((CORES, 4, batch, 512), F32), pltpu.VMEM((4, batch, 512), F32), pltpu.VMEM((chips - 1, batch, 512), F32),
                dma((8,)), dma((2, chunks)), dma((5,)), dma((5,)), dma((5,)), dma((5,)), dma((chunks,)), dma((chunks,)),
                dma((chunks, chips - 1)), dma((chunks, chips - 1)), dma((3,)), dma((3,)),
                dma((3, chips - 1)), dma((3, chips - 1)), dma((3, chips * CORES - 1)), dma((3, chips * CORES - 1))],
            compiler_params=pltpu.CompilerParams(collective_id=0, has_side_effects=True, vmem_limit_bytes=29 << 20),
            name='step',
        )(in_hbm(x), in_hbm(wq), in_hbm(wk), in_hbm(wv), in_hbm(wo), in_hbm(k3), in_hbm(v3), pos)

        def write(which, cache, pieces, *extra):
            return pl.pallas_call(
                functools.partial(write_kernel, which),
                out_shape=(jax.ShapeDtypeStruct(k3.shape, BF16), pltpu.VMEM(k3.shape, BF16), *(jax.ShapeDtypeStruct(e.shape, BF16) for e in extra)),
                in_specs=[vm, vm, sm] + [vm] * len(extra),
                out_specs=[hbm, vm] + [hbm] * len(extra),
                scratch_shapes=[dma((pieces,)), dma],
                input_output_aliases={0: 1},
                compiler_params=pltpu.CompilerParams(vmem_limit_bytes=4 << 20),
                name='write',
            )(in_vmem(cache), in_vmem(new), pos, *(in_vmem(e) for e in extra))
        ko, _, y = write(0, ko, 16, y)
        vo, _ = write(1, vo, 16)
        return y, ko.reshape(shape4), vo.reshape(shape4)

    return jax.shard_map(local_step, mesh=mesh, in_specs=in_specs, out_specs=out_specs, check_vma=False)
```

```python
import functools
import math

import jax
import jax.numpy as jnp
from jax import lax
from jax.experimental import pallas as pl
from jax.experimental.pallas import tpu as pltpu
from jax.sharding import PartitionSpec as P

MESH = pl.DeviceIdType.MESH
NEG = -3.4028234e38
F32, BF16 = jnp.float32, jnp.bfloat16
CORES = 2
NT = (((1,), (1,)), ((), ()))


def step_kernel(chips, x_hbm, wq_hbm, wk_hbm, wv_hbm, wo_hbm, k_hbm, v_hbm, pos_ref,
                yfull, kout, vout, rows_ref,
                x_v, wbuf, wo_v, qs, q_all, kv_all, sa, sb, mt_ref, pos2_ref, oraw, mraw, lraw, om, op, orecv,
                ys, yp, yr,
                lsem, kvsem, q_ss, q_rs, n_ss, n_rs, od_s, od_r, oi_s, oi_r, yd_s, yd_r, yi_s, yi_r, ag_s, ag_r):
    batch = k_hbm.shape[0]
    local_len = k_hbm.shape[1] // 8
    chunks = om.shape[0]
    cb = batch // chunks
    half = batch // 2
    scale2 = k_hbm.shape[2] ** -0.5 * math.log2(math.e)
    rep = lax.axis_index('rep')
    me = lax.axis_index('seq')
    chip, core = me // CORES, me % CORES
    base = me * local_len
    quarter = (chip % 2) * CORES + core

    def dev(c, e):
        return (rep, lax.rem(c, chips) * CORES + e)

    partner = dev(chip, 1 - core)
    ncols = 256
    lx = pltpu.make_async_copy(x_hbm, x_v, lsem.at[0])
    hd = wbuf.shape[1] // 2
    lw = [[pltpu.make_async_copy(wq_hbm.at[pl.ds(n * hd, hd), pl.ds(pl.multiple_of(quarter * 1024 + i * 512, 512), 512)],
                                 wbuf.at[i, pl.ds(n * hd, hd)], lsem.at[1 + i * 2 + n]) for n in range(2)] for i in range(2)]
    lk = pltpu.make_async_copy(wk_hbm.at[:, pl.ds(pl.multiple_of(quarter * ncols, ncols), ncols)], wbuf.at[2, :, pl.ds(0, ncols)], lsem.at[5])
    lv = pltpu.make_async_copy(wv_hbm.at[:, pl.ds(pl.multiple_of(quarter * ncols, ncols), ncols)], wbuf.at[2, :, pl.ds(ncols, ncols)], lsem.at[6])
    lo = pltpu.make_async_copy(wo_hbm, wo_v, lsem.at[7])
    lkc = [pltpu.make_async_copy(k_hbm.at[pl.ds(i * cb, cb)], kout.at[pl.ds(i * cb, cb)], kvsem.at[0, i]) for i in range(chunks)]
    lvc = [pltpu.make_async_copy(v_hbm.at[pl.ds(i * cb, cb)], vout.at[pl.ds(i * cb, cb)], kvsem.at[1, i]) for i in range(chunks)]
    lx.start()
    for i in range(2):
        for n in range(2):
            lw[i][n].start()

    barrier = pltpu.get_barrier_semaphore()
    for d in range(chips):
        for f in range(CORES):
            if d or f:
                pl.semaphore_signal(barrier, inc=1, device_id=dev(chip + d, lax.rem(core + f, CORES)), device_id_type=MESH)

    lane_b = (lax.broadcasted_iota(jnp.int32, pos2_ref.shape, 1) + lax.broadcasted_iota(jnp.int32, pos2_ref.shape, 0) * pos2_ref.shape[1]) // 2
    pv = jnp.zeros(pos2_ref.shape, jnp.int32)
    for b in range(batch):
        pv = jnp.where(lane_b == b, pos_ref[b], pv)
    pos2_ref[...] = pv

    lx.wait()
    for i in range(2):
        lw[i][0].wait()
        q = jnp.dot(x_v[:, :hd], wbuf[i, :hd], preferred_element_type=F32)
        lw[i][1].wait()
        if i == 0:
            lk.start()
            lv.start()
        q = q + jnp.dot(x_v[:, hd:], wbuf[i, hd:], preferred_element_type=F32)
        for h in range(4):
            qs[pl.ds(i * 4 + h, batch, stride=8), :] = q[:, h * 128:(h + 1) * 128]
    q_all[quarter] = qs[...].astype(BF16)
    pl.semaphore_wait(barrier, chips * CORES - 1)

    def spread(buf, rows, ss, rs):
        copies = [pltpu.make_async_remote_copy(buf.at[quarter], buf.at[quarter], ss.at[0], rs.at[0], device_id=partner, device_id_type=MESH)]
        for side, shift in ((0, 1), (1, chips - 1)):
            part = pl.ds(side * rows // 2, rows // 2)
            copies.append(pltpu.make_async_remote_copy(
                buf.at[quarter, part], buf.at[quarter, part], ss.at[1 + side], rs.at[1 + side], device_id=dev(chip + shift, core), device_id_type=MESH))
        return copies

    def hand_on(copies, buf, rows, ss, rs):
        other = ((chip + 1) % 2) * CORES + core
        for side in range(2):
            copies[1 + side].wait_recv()
            part = pl.ds(side * rows // 2, rows // 2)
            c = pltpu.make_async_remote_copy(buf.at[other, part], buf.at[other, part], ss.at[3 + side], rs.at[3 + side], device_id=partner, device_id_type=MESH)
            c.start()
            copies.append(c)

    def arrive(copies):
        copies[0].wait_recv()
        copies[3].wait_recv()
        copies[4].wait_recv()

    q_copies = spread(q_all, batch * 8, q_ss, q_rs)
    for c in q_copies:
        c.start()
    lkc[0].start()
    lvc[0].start()
    lk.wait()
    lv.wait()
    kv = jnp.dot(x_v[...], wbuf[2], preferred_element_type=F32)
    for w in range(2):
        for k in range(2):
            qs[pl.ds(w * 128 + k, batch, stride=2), :] = kv[:, w * 256 + k * 128:w * 256 + (k + 1) * 128]
    for hf in range(2):
        for w in range(2):
            kv_all[quarter, hf * 128 + w * 64:hf * 128 + w * 64 + 64, :] = qs[w * 128 + hf * 64:w * 128 + hf * 64 + 64, :].astype(BF16)
    n_copies = spread(kv_all, batch * 4, n_ss, n_rs)
    for c in n_copies:
        c.start()
    rowb = lax.broadcasted_iota(jnp.int32, (64, 128), 0) // 8 % 2
    bm0 = jnp.where(rowb == 0, 1.0, 0.0).astype(BF16)
    bm1 = jnp.where(rowb == 1, 1.0, 0.0).astype(BF16)

    hand_on(q_copies, q_all, batch * 8, q_ss, q_rs)
    for i in range(1, chunks):
        lkc[i].start()
        lvc[i].start()
    lo.start()
    hand_on(n_copies, kv_all, batch * 4, n_ss, n_rs)
    arrive(q_copies)

    qlane = lax.broadcasted_iota(jnp.int32, (8, 128), 1)
    own_head = lax.broadcasted_iota(jnp.int32, (8, 128), 0) == (qlane % 64) // 16 * 2 + (qlane % 8) // 4
    qseq = qlane // 64 * 2 + (qlane // 8) % 2
    mt_ref[...] = jnp.zeros_like(mt_ref)

    def scores(qi, buf):
        zero = jnp.zeros((64, 256), BF16)
        rows = []
        for ph in range(2):
            p0 = (2 * qi + ph) * 16
            q = jnp.concatenate([q_all[t, p0:p0 + 16, :] for t in range(4)], axis=0)
            blocks = [q * bm0, q * bm1]
            rows.append(jnp.concatenate(blocks + [zero] if ph == 0 else [zero] + blocks, axis=1))
        kc = jnp.concatenate([kout[4 * qi + j] for j in range(4)], axis=1)
        s = lax.dot_general(kc, jnp.concatenate(rows, axis=0), NT, preferred_element_type=F32).reshape(local_len, 8, 128)
        lim = jnp.full((8, 128), -1, jnp.int32)
        for j in range(4):
            lim = jnp.where(own_head & (qseq == j), pos_ref[4 * qi + j] - base, lim)
        s = jnp.where(lax.broadcasted_iota(jnp.int32, s.shape, 0) < lim[None], s, -jnp.inf)
        buf[...] = s.reshape(buf.shape)
        return jnp.maximum(jnp.max(jnp.max(s, axis=0), axis=0, keepdims=True), NEG)

    def weigh(qi, buf, m):
        p = jnp.exp2((buf[...] - m) * scale2)
        quad = qi % (cb // 4)
        mt_ref[0, quad:quad + 1, :] = m
        mt_ref[1, quad:quad + 1, :] = jnp.sum(p, axis=0, keepdims=True)
        pt = p.astype(BF16).T
        for ph in range(2):
            b0 = 4 * qi + 2 * ph
            vc = jnp.concatenate([vout[b0], vout[b0 + 1]], axis=1)
            o = jnp.dot(pt[ph * 64:(ph + 1) * 64, :], vc, preferred_element_type=F32)
            for t in range(4):
                for b in range(2):
                    r0 = (b0 % cb + b) * 8
                    oraw[t, r0:r0 + 8, :] = o[t * 16 + b * 8:t * 16 + b * 8 + 8, b * 128:(b + 1) * 128]

    rows_c = cb * 8
    carry = {}

    def attend(k):
        if k == 0:
            lkc[0].wait()
            carry['m'] = scores(0, sa)
        elif k % 2 == 1 and k < 2 * chunks - 1:
            lkc[(k + 1) // 2].wait()
        if k % 2 == 0:
            lvc[k // 2].wait()
        m_b = scores(2 * k + 1, sb)
        weigh(2 * k, sa, carry['m'])
        if k < 2 * chunks - 1:
            carry['m'] = scores(2 * k + 2, sa)
        weigh(2 * k + 1, sb, m_b)

    lane = lax.broadcasted_iota(jnp.int32, (8, 128), 1)
    od, oi, yd, yi, ag = {}, {}, {}, {}, {}

    def finalize(i):
        hf = i * cb // half
        first = i * rows_c - hf * half * 8
        rr = lax.broadcasted_iota(jnp.int32, (rows_c, 64), 0) + first
        cc = lax.broadcasted_iota(jnp.int32, (rows_c, 64), 1)
        rel = pos2_ref[hf:hf + 1, :] - base
        keep = (rr // 4 == cc) & (rel >= 0) & (rel < local_len)
        mt, lt = mt_ref[0].T, mt_ref[1].T

        def by_row(x, t):
            return jnp.concatenate([jnp.broadcast_to(x[(p % 2) * 64 + t * 16:(p % 2) * 64 + t * 16 + 16, p // 2:p // 2 + 1], (16, 128))
                                    for p in range(cb // 2)], axis=0)

        quarters = range(4)
        sn = [lax.dot_general(q_all[t, i * rows_c:(i + 1) * rows_c, :], kv_all[t, hf * 128:hf * 128 + 64, :], NT, preferred_element_type=F32) for t in quarters]
        mo = [by_row(mt, t) for t in quarters]
        lo_ = [by_row(lt, t) for t in quarters]
        sn = [jnp.where(keep, x, -jnp.inf) for x in sn]
        top = [jnp.max(x, axis=1, keepdims=True) for x in sn]
        mn = [jnp.maximum(x, y) for x, y in zip(mo, top)]
        pn = [jnp.exp2((x - y[:, :64]) * scale2) for x, y in zip(sn, mn)]
        on = [jnp.dot(pn[t].astype(BF16), kv_all[t, hf * 128 + 64:hf * 128 + 128, :], preferred_element_type=F32) for t in quarters]
        ln = [jnp.sum(x, axis=1, keepdims=True) for x in pn]
        for t in quarters:
            w = jnp.exp2((mo[t] - mn[t]) * scale2)
            mraw[t] = mn[t]
            lraw[t] = lo_[t] * w + ln[t]
            oraw[t] = oraw[t] * w + on[t]
        for e in range(CORES):
            for t in range(4):
                mp = jnp.zeros((8, 128), F32)
                lp = jnp.zeros((8, 128), F32)
                for h in range(4):
                    src = pl.ds(e * 4 + h, cb, stride=8)
                    om[i, e, t, h * cb:(h + 1) * cb, :] = oraw[t, src, :]
                    mh = mraw[t, src, :]
                    lh = lraw[t, src, :]
                    for g in range(cb // 8):
                        sel = lane == h * (cb // 8) + g
                        mp = jnp.where(sel, mh[g * 8:(g + 1) * 8], mp)
                        lp = jnp.where(sel, lh[g * 8:(g + 1) * 8], lp)
                om[i, e, t, cb * 4:cb * 4 + 8, :] = mp
                om[i, e, t, cb * 4 + 8:cb * 4 + 16, :] = lp
        od[i] = pltpu.make_async_remote_copy(om.at[i, 1 - core], op.at[i], od_s.at[i], od_r.at[i], device_id=partner, device_id_type=MESH)
        od[i].start()

    nrow = cb * 4

    def merge(parts):
        ms = [p[nrow:nrow + 8] for p in parts]
        m = functools.reduce(jnp.maximum, ms)
        ws = [jnp.exp2((x - m) * scale2) for x in ms]
        l = functools.reduce(jnp.add, [w * p[nrow + 8:nrow + 16] for w, p in zip(ws, parts)])
        return m, l, ws

    def chip_reduce(i):
        od[i].wait_recv()
        for t in range(4):
            fold(om.at[i, core, t], om[i, core, t], op[i, t])
        oi[i] = []
        for d in range(1, chips):
            c = pltpu.make_async_remote_copy(om.at[i, core, lax.rem(chip + d, chips)], orecv.at[i, d - 1], oi_s.at[i, d - 1], oi_r.at[i, d - 1],
                                             device_id=dev(chip + d, core), device_id_type=MESH)
            c.start()
            oi[i].append(c)

    def fold(dst, a, b):
        m, l, (wa, wb) = merge([a, b])
        for g in range(nrow // 8):
            r = slice(g * 8, g * 8 + 8)
            dst[g * 8:g * 8 + 8, :] = a[r] * wa[:, g:g + 1] + b[r] * wb[:, g:g + 1]
        dst[nrow:nrow + 8, :] = m
        dst[nrow + 8:nrow + 16, :] = l

    def project(i):
        for c in oi[i]:
            c.wait_recv()
        if i == 0:
            lo.wait()
        parts = [om[i, core, chip]] + [orecv[i, d] for d in range(chips - 1)]
        m, l, ws = merge(parts)
        rl = 1.0 / l
        heads = []
        for h in range(4):
            rows = []
            for g in range(h * (cb // 8), (h + 1) * (cb // 8)):
                o = functools.reduce(jnp.add, [p[g * 8:g * 8 + 8] * w[:, g:g + 1] for p, w in zip(parts, ws)])
                rows.append(o * rl[:, g:g + 1])
            heads.append(jnp.concatenate(rows, axis=0).astype(BF16))
        lhs = jnp.concatenate(heads, axis=1)
        for e in range(CORES):
            for t in range(4):
                c0 = (e * 4 + t) * 512
                ys[i, e, t] = jnp.dot(lhs, wo_v[:, c0:c0 + 512], preferred_element_type=F32)
        yd[i] = pltpu.make_async_remote_copy(ys.at[i, 1 - core], yp.at[i], yd_s.at[i], yd_r.at[i], device_id=partner, device_id_type=MESH)
        yd[i].start()

    def y_chip(i):
        yd[i].wait_recv()
        ys[i, core] = ys[i, core] + yp[i]
        yi[i] = []
        for d in range(1, chips):
            c = pltpu.make_async_remote_copy(ys.at[i, core, lax.rem(chip + d, chips)], yr.at[i, d - 1], yi_s.at[i, d - 1], yi_r.at[i, d - 1],
                                             device_id=dev(chip + d, core), device_id_type=MESH)
            c.start()
            yi[i].append(c)

    def block(i, c):
        return (pl.ds(i * cb, cb), pl.ds(pl.multiple_of((core * 4 + c) * 512, 512), 512))

    def lay_rows():
        for w in range(2):
            for t in range(4):
                for hf in range(2):
                    sa[:64, :] = kv_all[t, hf * 128 + w * 64:hf * 128 + w * 64 + 64, :].astype(F32)
                    for k in range(2):
                        qs[pl.ds(hf * half * 8 + t * 2 + k, half, stride=8), :] = sa[pl.ds(k, half, stride=2), :]
            rows_ref[w] = qs[...].astype(BF16)

    def y_final(i):
        if i == chunks - 1:
            lay_rows()
        for c in yi[i]:
            c.wait_recv()
        y = ys[i, core, chip]
        for d in range(chips - 1):
            y = y + yr[i, d]
        yfull[block(i, chip)] = y.astype(BF16)
        ag[i] = []
        if i == chunks - 1:
            for d in range(chips):
                for f in range(CORES):
                    if d or f:
                        push(i, chip, dev(chip + d, lax.rem(core + f, CORES)))
        else:
            for d in range(1, chips):
                push(i, chip, dev(chip + d, core))
            push(i, chip, partner)

    def push(i, c, target):
        slot = len(ag[i])
        cp = pltpu.make_async_remote_copy(yfull.at[block(i, c)], yfull.at[block(i, c)], ag_s.at[i, slot], ag_r.at[i, slot], device_id=target, device_id_type=MESH)
        cp.start()
        ag[i].append(cp)

    def pass_on(i):
        for d in range(1, chips):
            ag[i][d - 1].wait_recv()
            push(i, lax.rem(chip + chips - d, chips), partner)

    plan = {1: [(finalize, 0)], 2: [(chip_reduce, 0)], 3: [(finalize, 1)], 4: [(chip_reduce, 1)],
            5: [(finalize, 2), (project, 0)], 6: [(chip_reduce, 2), (y_chip, 0), (project, 1)],
            7: [(finalize, 3), (y_chip, 1), (chip_reduce, 3), (y_final, 0), (project, 2), (y_chip, 2), (y_final, 1), (project, 3), (pass_on, 0),
                (y_chip, 3), (y_final, 2), (pass_on, 1), (y_final, 3), (pass_on, 2)]}
    for k in range(max(plan) + 1):
        if k < 2 * chunks:
            attend(k)
        if k == 1:
            arrive(n_copies)
        for stage, i in plan.get(k, ()):
            stage(i)
    for i in range(chunks):
        for c in ag[i] if i == chunks - 1 else ag[i][chips - 1:]:
            c.wait_recv()
    for c in q_copies + n_copies:
        c.wait_send()
    for i in range(chunks):
        for c in [od[i], yd[i]] + oi[i] + yi[i] + ag[i]:
            c.wait_send()


def write_kernel(which, k_in, new_ref, pos_ref, *refs):
    if which == 0:
        y_ref, k_out, k_ref, y_out, bsem, ysem = refs
        cy = pltpu.make_async_copy(y_ref, y_out, ysem)
    else:
        k_out, k_ref, bsem, ysem = refs
    batch, local_len = k_ref.shape[0], k_ref.shape[1] // 8
    base = lax.axis_index('seq') * local_len
    pieces = bsem.shape[0]
    pb = batch // pieces
    bulk = []
    for i in range(pieces):
        @pl.loop(i * pb, (i + 1) * pb)
        def _(b):
            rel = pos_ref[b] - base

            @pl.when((rel >= 0) & (rel < local_len))
            def _():
                k_ref[b, pl.ds(pl.multiple_of(rel * 8, 8), 8), :] = new_ref[which, pl.ds(pl.multiple_of(b * 8, 8), 8), :]
        part = pl.ds(i * pb, pb)
        c = pltpu.make_async_copy(k_ref.at[part], k_out.at[part], bsem.at[i])
        c.start()
        bulk.append(c)
    if which == 0:
        cy.start()
        bulk.append(cy)
    for c in bulk:
        c.wait()


def solution(mesh):
    cache_spec = P('rep', 'seq', None, None)
    in_specs = (P('rep', None), P(), P(), P(), P('seq', None), cache_spec, cache_spec, P('rep'))
    out_specs = (P('rep', None), cache_spec, cache_spec)
    chips = mesh.shape['seq'] // CORES
    assert chips == 4
    vm = pl.BlockSpec(memory_space=pltpu.VMEM)
    hbm = pl.BlockSpec(memory_space=pl.ANY)
    sm = pl.BlockSpec(memory_space=pltpu.SMEM)

    def local_step(x, wq, wk, wv, wo, k, v, pos):
        shape4 = k.shape
        batch, width = x.shape
        k3 = k.reshape(batch, -1, k.shape[-1])
        v3 = v.reshape(k3.shape)
        chunks = 4
        cb = batch // chunks
        dma = pltpu.SemaphoreType.DMA
        in_hbm = lambda a: pltpu.with_memory_space_constraint(a, pltpu.HBM)
        in_vmem = lambda a: pltpu.with_memory_space_constraint(a, pltpu.VMEM)
        y, ko, vo, new = pl.pallas_call(
            functools.partial(step_kernel, chips),
            out_shape=(pltpu.VMEM((batch, wo.shape[1]), BF16), pltpu.VMEM(k3.shape, BF16), pltpu.VMEM(k3.shape, BF16),
                       pltpu.VMEM((2, batch * 8, 128), BF16)),
            in_specs=[hbm] * 7 + [sm],
            out_specs=[vm] * 4,
            scratch_shapes=[
                pltpu.VMEM((batch, width), BF16), pltpu.VMEM((3, width, 512), BF16), pltpu.VMEM(wo.shape, BF16),
                pltpu.VMEM((batch * 8, 128), F32), pltpu.VMEM((4, batch * 8, 128), BF16), pltpu.VMEM((4, batch * 4, 128), BF16), pltpu.VMEM((k3.shape[1], 128), F32), pltpu.VMEM((k3.shape[1], 128), F32), pltpu.VMEM((2, 8, 128), F32), pltpu.VMEM((2, batch), jnp.int32),
                pltpu.VMEM((4, cb * 8, 128), F32), pltpu.VMEM((4, cb * 8, 128), F32), pltpu.VMEM((4, cb * 8, 128), F32),
                pltpu.VMEM((chunks, CORES, 4, cb * 4 + 16, 128), F32), pltpu.VMEM((chunks, 4, cb * 4 + 16, 128), F32),
                pltpu.VMEM((chunks, chips - 1, cb * 4 + 16, 128), F32),
                pltpu.VMEM((chunks, CORES, 4, cb, 512), F32), pltpu.VMEM((chunks, 4, cb, 512), F32), pltpu.VMEM((chunks, chips - 1, cb, 512), F32),
                dma((8,)), dma((2, chunks)), dma((5,)), dma((5,)), dma((5,)), dma((5,)), dma((chunks,)), dma((chunks,)),
                dma((chunks, chips - 1)), dma((chunks, chips - 1)), dma((chunks,)), dma((chunks,)),
                dma((chunks, chips - 1)), dma((chunks, chips - 1)), dma((chunks, chips * CORES - 1)), dma((chunks, chips * CORES - 1))],
            compiler_params=pltpu.CompilerParams(collective_id=0, has_side_effects=True, vmem_limit_bytes=29 << 20),
            name='step',
        )(in_hbm(x), in_hbm(wq), in_hbm(wk), in_hbm(wv), in_hbm(wo), in_hbm(k3), in_hbm(v3), pos)

        def write(which, cache, pieces, *extra):
            return pl.pallas_call(
                functools.partial(write_kernel, which),
                out_shape=(jax.ShapeDtypeStruct(k3.shape, BF16), pltpu.VMEM(k3.shape, BF16), *(jax.ShapeDtypeStruct(e.shape, BF16) for e in extra)),
                in_specs=[vm, vm, sm] + [vm] * len(extra),
                out_specs=[hbm, vm] + [hbm] * len(extra),
                scratch_shapes=[dma((pieces,)), dma],
                input_output_aliases={0: 1},
                compiler_params=pltpu.CompilerParams(vmem_limit_bytes=4 << 20),
                name='write',
            )(in_vmem(cache), in_vmem(new), pos, *(in_vmem(e) for e in extra))
        ko, _, y = write(0, ko, 16, y)
        vo, _ = write(1, vo, 16)
        return y, ko.reshape(shape4), vo.reshape(shape4)

    return jax.shard_map(local_step, mesh=mesh, in_specs=in_specs, out_specs=out_specs, check_vma=False)
```

```python
import functools
import math

import jax
import jax.numpy as jnp
from jax import lax
from jax.experimental import pallas as pl
from jax.experimental.pallas import tpu as pltpu
from jax.sharding import PartitionSpec as P

MESH = pl.DeviceIdType.MESH
NEG = -3.4028234e38
F32, BF16 = jnp.float32, jnp.bfloat16
CORES = 2
NT = (((1,), (1,)), ((), ()))


def step_kernel(chips, x_hbm, wq_hbm, wk_hbm, wv_hbm, wo_hbm, k_hbm, v_hbm, pos_ref,
                yfull, kout, vout, rows_ref,
                x_v, wbuf, wo_v, qs, q_all, kv_all, sa, sb, mt_ref, pos2_ref, oraw, mraw, lraw, om, op, orecv,
                ys, yp, yr,
                lsem, kvsem, q_ss, q_rs, n_ss, n_rs, od_s, od_r, oi_s, oi_r, yd_s, yd_r, yi_s, yi_r, ag_s, ag_r):
    batch = k_hbm.shape[0]
    local_len = k_hbm.shape[1] // 8
    chunks = om.shape[0]
    cb = batch // chunks
    half = batch // 2
    scale2 = k_hbm.shape[2] ** -0.5 * math.log2(math.e)
    rep = lax.axis_index('rep')
    me = lax.axis_index('seq')
    chip, core = me // CORES, me % CORES
    base = me * local_len
    quarter = (chip % 2) * CORES + core

    def dev(c, e):
        return (rep, lax.rem(c, chips) * CORES + e)

    partner = dev(chip, 1 - core)
    ncols = 256
    lx = pltpu.make_async_copy(x_hbm, x_v, lsem.at[0])
    hd = wbuf.shape[1] // 2
    lw = [[pltpu.make_async_copy(wq_hbm.at[pl.ds(n * hd, hd), pl.ds(pl.multiple_of(quarter * 1024 + i * 512, 512), 512)],
                                 wbuf.at[i, pl.ds(n * hd, hd)], lsem.at[1 + i * 2 + n]) for n in range(2)] for i in range(2)]
    lk = pltpu.make_async_copy(wk_hbm.at[:, pl.ds(pl.multiple_of(quarter * ncols, ncols), ncols)], wbuf.at[2, :, pl.ds(0, ncols)], lsem.at[5])
    lv = pltpu.make_async_copy(wv_hbm.at[:, pl.ds(pl.multiple_of(quarter * ncols, ncols), ncols)], wbuf.at[2, :, pl.ds(ncols, ncols)], lsem.at[6])
    lo = pltpu.make_async_copy(wo_hbm, wo_v, lsem.at[7])
    lkc = [pltpu.make_async_copy(k_hbm.at[pl.ds(i * cb, cb)], kout.at[pl.ds(i * cb, cb)], kvsem.at[0, i]) for i in range(chunks)]
    lvc = [pltpu.make_async_copy(v_hbm.at[pl.ds(i * cb, cb)], vout.at[pl.ds(i * cb, cb)], kvsem.at[1, i]) for i in range(chunks)]
    lx.start()
    for i in range(2):
        for n in range(2):
            lw[i][n].start()

    barrier = pltpu.get_barrier_semaphore()
    for d in range(chips):
        for f in range(CORES):
            if d or f:
                pl.semaphore_signal(barrier, inc=1, device_id=dev(chip + d, lax.rem(core + f, CORES)), device_id_type=MESH)

    lane_b = (lax.broadcasted_iota(jnp.int32, pos2_ref.shape, 1) + lax.broadcasted_iota(jnp.int32, pos2_ref.shape, 0) * pos2_ref.shape[1]) // 2
    pv = jnp.zeros(pos2_ref.shape, jnp.int32)
    for b in range(batch):
        pv = jnp.where(lane_b == b, pos_ref[b], pv)
    pos2_ref[...] = pv

    lx.wait()
    for i in range(2):
        lw[i][0].wait()
        q = jnp.dot(x_v[:, :hd], wbuf[i, :hd], preferred_element_type=F32)
        lw[i][1].wait()
        if i == 0:
            lk.start()
            lv.start()
        q = q + jnp.dot(x_v[:, hd:], wbuf[i, hd:], preferred_element_type=F32)
        for h in range(4):
            qs[pl.ds(i * 4 + h, batch, stride=8), :] = q[:, h * 128:(h + 1) * 128]
    q_all[quarter] = qs[...].astype(BF16)
    pl.semaphore_wait(barrier, chips * CORES - 1)

    def spread(buf, rows, ss, rs):
        copies = [pltpu.make_async_remote_copy(buf.at[quarter], buf.at[quarter], ss.at[0], rs.at[0], device_id=partner, device_id_type=MESH)]
        for side, shift in ((0, 1), (1, chips - 1)):
            part = pl.ds(side * rows // 2, rows // 2)
            copies.append(pltpu.make_async_remote_copy(
                buf.at[quarter, part], buf.at[quarter, part], ss.at[1 + side], rs.at[1 + side], device_id=dev(chip + shift, core), device_id_type=MESH))
        return copies

    def hand_on(copies, buf, rows, ss, rs):
        other = ((chip + 1) % 2) * CORES + core
        for side in range(2):
            copies[1 + side].wait_recv()
            part = pl.ds(side * rows // 2, rows // 2)
            c = pltpu.make_async_remote_copy(buf.at[other, part], buf.at[other, part], ss.at[3 + side], rs.at[3 + side], device_id=partner, device_id_type=MESH)
            c.start()
            copies.append(c)

    def arrive(copies):
        copies[0].wait_recv()
        copies[3].wait_recv()
        copies[4].wait_recv()

    q_copies = spread(q_all, batch * 8, q_ss, q_rs)
    for c in q_copies:
        c.start()
    lkc[0].start()
    lvc[0].start()
    lk.wait()
    lv.wait()
    kv = jnp.dot(x_v[...], wbuf[2], preferred_element_type=F32)
    for w in range(2):
        for k in range(2):
            qs[pl.ds(w * 128 + k, batch, stride=2), :] = kv[:, w * 256 + k * 128:w * 256 + (k + 1) * 128]
    for hf in range(2):
        for w in range(2):
            kv_all[quarter, hf * 128 + w * 64:hf * 128 + w * 64 + 64, :] = qs[w * 128 + hf * 64:w * 128 + hf * 64 + 64, :].astype(BF16)
    n_copies = spread(kv_all, batch * 4, n_ss, n_rs)
    for c in n_copies:
        c.start()
    rowb = lax.broadcasted_iota(jnp.int32, (64, 128), 0) // 8 % 2
    bm0 = jnp.where(rowb == 0, 1.0, 0.0).astype(BF16)
    bm1 = jnp.where(rowb == 1, 1.0, 0.0).astype(BF16)

    hand_on(q_copies, q_all, batch * 8, q_ss, q_rs)
    for i in range(1, chunks):
        lkc[i].start()
        lvc[i].start()
    lo.start()
    hand_on(n_copies, kv_all, batch * 4, n_ss, n_rs)
    arrive(q_copies)

    qlane = lax.broadcasted_iota(jnp.int32, (8, 128), 1)
    own_head = lax.broadcasted_iota(jnp.int32, (8, 128), 0) == (qlane % 64) // 16 * 2 + (qlane % 8) // 4
    qseq = qlane // 64 * 2 + (qlane // 8) % 2
    mt_ref[...] = jnp.zeros_like(mt_ref)

    def scores(qi, buf):
        zero = jnp.zeros((64, 256), BF16)
        rows = []
        for ph in range(2):
            p0 = (2 * qi + ph) * 16
            q = jnp.concatenate([q_all[t, p0:p0 + 16, :] for t in range(4)], axis=0)
            blocks = [q * bm0, q * bm1]
            rows.append(jnp.concatenate(blocks + [zero] if ph == 0 else [zero] + blocks, axis=1))
        kc = jnp.concatenate([kout[4 * qi + j] for j in range(4)], axis=1)
        s = lax.dot_general(kc, jnp.concatenate(rows, axis=0), NT, preferred_element_type=F32).reshape(local_len, 8, 128)
        lim = jnp.full((8, 128), -1, jnp.int32)
        for j in range(4):
            lim = jnp.where(own_head & (qseq == j), pos_ref[4 * qi + j] - base, lim)
        s = jnp.where(lax.broadcasted_iota(jnp.int32, s.shape, 0) < lim[None], s, -jnp.inf)
        buf[...] = s.reshape(buf.shape)
        return jnp.maximum(jnp.max(jnp.max(s, axis=0), axis=0, keepdims=True), NEG)

    def weigh(qi, buf, m):
        p = jnp.exp2((buf[...] - m) * scale2)
        quad = qi % (cb // 4)
        mt_ref[0, quad:quad + 1, :] = m
        mt_ref[1, quad:quad + 1, :] = jnp.sum(p, axis=0, keepdims=True)
        pt = p.astype(BF16).T
        for ph in range(2):
            b0 = 4 * qi + 2 * ph
            vc = jnp.concatenate([vout[b0], vout[b0 + 1]], axis=1)
            o = jnp.dot(pt[ph * 64:(ph + 1) * 64, :], vc, preferred_element_type=F32)
            for t in range(4):
                for b in range(2):
                    r0 = (b0 % cb + b) * 8
                    oraw[t, r0:r0 + 8, :] = o[t * 16 + b * 8:t * 16 + b * 8 + 8, b * 128:(b + 1) * 128]

    rows_c = cb * 8
    carry = {}

    def attend(k):
        if k == 0:
            lkc[0].wait()
            carry['m'] = scores(0, sa)
        elif k % 2 == 1 and k < 2 * chunks - 1:
            lkc[(k + 1) // 2].wait()
        if k % 2 == 0:
            lvc[k // 2].wait()
        m_b = scores(2 * k + 1, sb)
        weigh(2 * k, sa, carry['m'])
        if k < 2 * chunks - 1:
            carry['m'] = scores(2 * k + 2, sa)
        weigh(2 * k + 1, sb, m_b)

    lane = lax.broadcasted_iota(jnp.int32, (8, 128), 1)
    od, oi, yd, yi, ag = {}, {}, {}, {}, {}

    def finalize(i):
        hf = i * cb // half
        first = i * rows_c - hf * half * 8
        rr = lax.broadcasted_iota(jnp.int32, (rows_c, 64), 0) + first
        cc = lax.broadcasted_iota(jnp.int32, (rows_c, 64), 1)
        rel = pos2_ref[hf:hf + 1, :] - base
        keep = (rr // 4 == cc) & (rel >= 0) & (rel < local_len)
        mt, lt = mt_ref[0].T, mt_ref[1].T

        def by_row(x, t):
            return jnp.concatenate([jnp.broadcast_to(x[(p % 2) * 64 + t * 16:(p % 2) * 64 + t * 16 + 16, p // 2:p // 2 + 1], (16, 128))
                                    for p in range(cb // 2)], axis=0)

        quarters = range(4)
        sn = [lax.dot_general(q_all[t, i * rows_c:(i + 1) * rows_c, :], kv_all[t, hf * 128:hf * 128 + 64, :], NT, preferred_element_type=F32) for t in quarters]
        mo = [by_row(mt, t) for t in quarters]
        lo_ = [by_row(lt, t) for t in quarters]
        sn = [jnp.where(keep, x, -jnp.inf) for x in sn]
        top = [jnp.max(x, axis=1, keepdims=True) for x in sn]
        mn = [jnp.maximum(x, y) for x, y in zip(mo, top)]
        pn = [jnp.exp2((x - y[:, :64]) * scale2) for x, y in zip(sn, mn)]
        on = [jnp.dot(pn[t].astype(BF16), kv_all[t, hf * 128 + 64:hf * 128 + 128, :], preferred_element_type=F32) for t in quarters]
        ln = [jnp.sum(x, axis=1, keepdims=True) for x in pn]
        for t in quarters:
            w = jnp.exp2((mo[t] - mn[t]) * scale2)
            mraw[t] = mn[t]
            lraw[t] = lo_[t] * w + ln[t]
            oraw[t] = oraw[t] * w + on[t]
        for e in range(CORES):
            for t in range(4):
                mp = jnp.zeros((8, 128), F32)
                lp = jnp.zeros((8, 128), F32)
                for h in range(4):
                    src = pl.ds(e * 4 + h, cb, stride=8)
                    om[i, e, t, h * cb:(h + 1) * cb, :] = oraw[t, src, :]
                    mh = mraw[t, src, :]
                    lh = lraw[t, src, :]
                    for g in range(cb // 8):
                        sel = lane == h * (cb // 8) + g
                        mp = jnp.where(sel, mh[g * 8:(g + 1) * 8], mp)
                        lp = jnp.where(sel, lh[g * 8:(g + 1) * 8], lp)
                om[i, e, t, cb * 4:cb * 4 + 8, :] = mp
                om[i, e, t, cb * 4 + 8:cb * 4 + 16, :] = lp
        od[i] = pltpu.make_async_remote_copy(om.at[i, 1 - core], op.at[i], od_s.at[i], od_r.at[i], device_id=partner, device_id_type=MESH)
        od[i].start()

    nrow = cb * 4

    def merge(parts):
        ms = [p[nrow:nrow + 8] for p in parts]
        m = functools.reduce(jnp.maximum, ms)
        ws = [jnp.exp2((x - m) * scale2) for x in ms]
        l = functools.reduce(jnp.add, [w * p[nrow + 8:nrow + 16] for w, p in zip(ws, parts)])
        return m, l, ws

    def chip_reduce(i):
        od[i].wait_recv()
        for t in range(4):
            fold(om.at[i, core, t], om[i, core, t], op[i, t])
        oi[i] = []
        for d in range(1, chips):
            c = pltpu.make_async_remote_copy(om.at[i, core, lax.rem(chip + d, chips)], orecv.at[i, d - 1], oi_s.at[i, d - 1], oi_r.at[i, d - 1],
                                             device_id=dev(chip + d, core), device_id_type=MESH)
            c.start()
            oi[i].append(c)

    def fold(dst, a, b):
        m, l, (wa, wb) = merge([a, b])
        for g in range(nrow // 8):
            r = slice(g * 8, g * 8 + 8)
            dst[g * 8:g * 8 + 8, :] = a[r] * wa[:, g:g + 1] + b[r] * wb[:, g:g + 1]
        dst[nrow:nrow + 8, :] = m
        dst[nrow + 8:nrow + 16, :] = l

    def project(i):
        for c in oi[i]:
            c.wait_recv()
        if i == 0:
            lo.wait()
        parts = [om[i, core, chip]] + [orecv[i, d] for d in range(chips - 1)]
        m, l, ws = merge(parts)
        rl = 1.0 / l
        heads = []
        for h in range(4):
            rows = []
            for g in range(h * (cb // 8), (h + 1) * (cb // 8)):
                o = functools.reduce(jnp.add, [p[g * 8:g * 8 + 8] * w[:, g:g + 1] for p, w in zip(parts, ws)])
                rows.append(o * rl[:, g:g + 1])
            heads.append(jnp.concatenate(rows, axis=0).astype(BF16))
        lhs = jnp.concatenate(heads, axis=1)
        for e in range(CORES):
            for t in range(4):
                c0 = (e * 4 + t) * 512
                ys[i, e, t] = jnp.dot(lhs, wo_v[:, c0:c0 + 512], preferred_element_type=F32)
        yd[i] = pltpu.make_async_remote_copy(ys.at[i, 1 - core], yp.at[i], yd_s.at[i], yd_r.at[i], device_id=partner, device_id_type=MESH)
        yd[i].start()

    def y_chip(i):
        yd[i].wait_recv()
        ys[i, core] = ys[i, core] + yp[i]
        yi[i] = []
        for d in range(1, chips):
            c = pltpu.make_async_remote_copy(ys.at[i, core, lax.rem(chip + d, chips)], yr.at[i, d - 1], yi_s.at[i, d - 1], yi_r.at[i, d - 1],
                                             device_id=dev(chip + d, core), device_id_type=MESH)
            c.start()
            yi[i].append(c)

    def block(i, c):
        return (pl.ds(i * cb, cb), pl.ds(pl.multiple_of((core * 4 + c) * 512, 512), 512))

    def lay_rows():
        for w in range(2):
            for t in range(4):
                for hf in range(2):
                    sa[:64, :] = kv_all[t, hf * 128 + w * 64:hf * 128 + w * 64 + 64, :].astype(F32)
                    for k in range(2):
                        qs[pl.ds(hf * half * 8 + t * 2 + k, half, stride=8), :] = sa[pl.ds(k, half, stride=2), :]
            rows_ref[w] = qs[...].astype(BF16)

    def y_final(i):
        if i == chunks - 1:
            lay_rows()
        for c in yi[i]:
            c.wait_recv()
        y = ys[i, core, chip]
        for d in range(chips - 1):
            y = y + yr[i, d]
        yfull[block(i, chip)] = y.astype(BF16)
        ag[i] = []
        if i == chunks - 1:
            for d in range(chips):
                for f in range(CORES):
                    if d or f:
                        push(i, chip, dev(chip + d, lax.rem(core + f, CORES)))
        else:
            for d in range(1, chips):
                push(i, chip, dev(chip + d, core))
            push(i, chip, partner)

    def push(i, c, target):
        slot = len(ag[i])
        cp = pltpu.make_async_remote_copy(yfull.at[block(i, c)], yfull.at[block(i, c)], ag_s.at[i, slot], ag_r.at[i, slot], device_id=target, device_id_type=MESH)
        cp.start()
        ag[i].append(cp)

    def pass_on(i):
        for d in range(1, chips):
            ag[i][d - 1].wait_recv()
            push(i, lax.rem(chip + chips - d, chips), partner)

    plan = {1: [(finalize, 0)], 2: [(chip_reduce, 0)], 3: [(finalize, 1)], 4: [(chip_reduce, 1)],
            5: [(finalize, 2), (project, 0)], 6: [(chip_reduce, 2), (y_chip, 0), (project, 1)],
            7: [(finalize, 3), (chip_reduce, 3), (y_chip, 1), (y_final, 0), (project, 2), (y_chip, 2), (y_final, 1), (project, 3), (pass_on, 0),
                (y_chip, 3), (y_final, 2), (pass_on, 1), (y_final, 3), (pass_on, 2)]}
    for k in range(max(plan) + 1):
        if k < 2 * chunks:
            attend(k)
        if k == 1:
            arrive(n_copies)
        for stage, i in plan.get(k, ()):
            stage(i)
    for i in range(chunks):
        for c in ag[i] if i == chunks - 1 else ag[i][chips - 1:]:
            c.wait_recv()
    for c in q_copies + n_copies:
        c.wait_send()
    for i in range(chunks):
        for c in [od[i], yd[i]] + oi[i] + yi[i] + ag[i]:
            c.wait_send()


def write_kernel(k_in, v_in, new_ref, pos_ref, y_ref, k_out, k_ref, v_ref, y_out, bsem, ysem):
    batch, local_len = k_ref.shape[0], k_ref.shape[1] // 8
    base = lax.axis_index('seq') * local_len
    pieces = bsem.shape[0]
    pb = batch // pieces
    cy = pltpu.make_async_copy(y_ref, y_out, ysem)

    def patch(cache, which, first, last):
        @pl.loop(first, last)
        def _(b):
            rel = pos_ref[b] - base

            @pl.when((rel >= 0) & (rel < local_len))
            def _():
                cache[b, pl.ds(pl.multiple_of(rel * 8, 8), 8), :] = new_ref[which, pl.ds(pl.multiple_of(b * 8, 8), 8), :]

    copies = []
    for i in range(pieces):
        patch(k_ref, 0, i * pb, (i + 1) * pb)
        part = pl.ds(i * pb, pb)
        c = pltpu.make_async_copy(k_ref.at[part], k_out.at[part], bsem.at[i])
        c.start()
        copies.append(c)
    cy.start()
    patch(v_ref, 1, 0, batch)
    for c in copies + [cy]:
        c.wait()


def solution(mesh):
    cache_spec = P('rep', 'seq', None, None)
    in_specs = (P('rep', None), P(), P(), P(), P('seq', None), cache_spec, cache_spec, P('rep'))
    out_specs = (P('rep', None), cache_spec, cache_spec)
    chips = mesh.shape['seq'] // CORES
    assert chips == 4
    vm = pl.BlockSpec(memory_space=pltpu.VMEM)
    hbm = pl.BlockSpec(memory_space=pl.ANY)
    sm = pl.BlockSpec(memory_space=pltpu.SMEM)

    def local_step(x, wq, wk, wv, wo, k, v, pos):
        shape4 = k.shape
        batch, width = x.shape
        k3 = k.reshape(batch, -1, k.shape[-1])
        v3 = v.reshape(k3.shape)
        chunks = 4
        cb = batch // chunks
        dma = pltpu.SemaphoreType.DMA
        in_hbm = lambda a: pltpu.with_memory_space_constraint(a, pltpu.HBM)
        in_vmem = lambda a: pltpu.with_memory_space_constraint(a, pltpu.VMEM)
        y, ko, vo, new = pl.pallas_call(
            functools.partial(step_kernel, chips),
            out_shape=(pltpu.VMEM((batch, wo.shape[1]), BF16), pltpu.VMEM(k3.shape, BF16), pltpu.VMEM(k3.shape, BF16),
                       pltpu.VMEM((2, batch * 8, 128), BF16)),
            in_specs=[hbm] * 7 + [sm],
            out_specs=[vm] * 4,
            scratch_shapes=[
                pltpu.VMEM((batch, width), BF16), pltpu.VMEM((3, width, 512), BF16), pltpu.VMEM(wo.shape, BF16),
                pltpu.VMEM((batch * 8, 128), F32), pltpu.VMEM((4, batch * 8, 128), BF16), pltpu.VMEM((4, batch * 4, 128), BF16), pltpu.VMEM((k3.shape[1], 128), F32), pltpu.VMEM((k3.shape[1], 128), F32), pltpu.VMEM((2, 8, 128), F32), pltpu.VMEM((2, batch), jnp.int32),
                pltpu.VMEM((4, cb * 8, 128), F32), pltpu.VMEM((4, cb * 8, 128), F32), pltpu.VMEM((4, cb * 8, 128), F32),
                pltpu.VMEM((chunks, CORES, 4, cb * 4 + 16, 128), F32), pltpu.VMEM((chunks, 4, cb * 4 + 16, 128), F32),
                pltpu.VMEM((chunks, chips - 1, cb * 4 + 16, 128), F32),
                pltpu.VMEM((chunks, CORES, 4, cb, 512), F32), pltpu.VMEM((chunks, 4, cb, 512), F32), pltpu.VMEM((chunks, chips - 1, cb, 512), F32),
                dma((8,)), dma((2, chunks)), dma((5,)), dma((5,)), dma((5,)), dma((5,)), dma((chunks,)), dma((chunks,)),
                dma((chunks, chips - 1)), dma((chunks, chips - 1)), dma((chunks,)), dma((chunks,)),
                dma((chunks, chips - 1)), dma((chunks, chips - 1)), dma((chunks, chips * CORES - 1)), dma((chunks, chips * CORES - 1))],
            compiler_params=pltpu.CompilerParams(collective_id=0, has_side_effects=True, vmem_limit_bytes=29 << 20),
            name='step',
        )(in_hbm(x), in_hbm(wq), in_hbm(wk), in_hbm(wv), in_hbm(wo), in_hbm(k3), in_hbm(v3), pos)

        pieces = 16
        ko, _, vo, y = pl.pallas_call(
            write_kernel,
            out_shape=(jax.ShapeDtypeStruct(k3.shape, BF16), pltpu.VMEM(k3.shape, BF16), pltpu.VMEM(k3.shape, BF16), jax.ShapeDtypeStruct(y.shape, BF16)),
            in_specs=[vm, vm, vm, sm, vm],
            out_specs=[hbm, vm, vm, hbm],
            scratch_shapes=[dma((pieces,)), dma],
            input_output_aliases={0: 1, 1: 2},
            compiler_params=pltpu.CompilerParams(vmem_limit_bytes=4 << 20),
            name='write',
        )(in_vmem(ko), in_vmem(vo), in_vmem(new), pos, in_vmem(y))
        return y, ko.reshape(shape4), vo.reshape(shape4)

    return jax.shard_map(local_step, mesh=mesh, in_specs=in_specs, out_specs=out_specs, check_vma=False)
```

```python
import functools
import math

import jax
import jax.numpy as jnp
from jax import lax
from jax.experimental import pallas as pl
from jax.experimental.pallas import tpu as pltpu
from jax.sharding import PartitionSpec as P

MESH = pl.DeviceIdType.MESH
NEG = -3.4028234e38
F32, BF16 = jnp.float32, jnp.bfloat16
CORES = 2
NT = (((1,), (1,)), ((), ()))


def step_kernel(chips, x_hbm, wq_hbm, wk_hbm, wv_hbm, wo_hbm, k_hbm, v_hbm, pos_ref,
                yfull, kout, vout, rows_ref,
                x_v, wbuf, wo_v, qs, q_all, kv_all, sa, sb, mt_ref, pos2_ref, oraw, mraw, lraw, om, op, orecv,
                ys, yp, yr,
                lsem, kvsem, q_ss, q_rs, n_ss, n_rs, od_s, od_r, oi_s, oi_r, yd_s, yd_r, yi_s, yi_r, ag_s, ag_r):
    batch = k_hbm.shape[0]
    local_len = k_hbm.shape[1] // 8
    chunks = om.shape[0]
    cb = batch // chunks
    half = batch // 2
    scale2 = k_hbm.shape[2] ** -0.5 * math.log2(math.e)
    rep = lax.axis_index('rep')
    me = lax.axis_index('seq')
    chip, core = me // CORES, me % CORES
    base = me * local_len
    quarter = (chip % 2) * CORES + core

    def dev(c, e):
        return (rep, lax.rem(c, chips) * CORES + e)

    partner = dev(chip, 1 - core)
    ncols = 256
    lx = pltpu.make_async_copy(x_hbm, x_v, lsem.at[0])
    hd = wbuf.shape[1] // 2
    lw = [[pltpu.make_async_copy(wq_hbm.at[pl.ds(n * hd, hd), pl.ds(pl.multiple_of(quarter * 1024 + i * 512, 512), 512)],
                                 wbuf.at[i, pl.ds(n * hd, hd)], lsem.at[1 + i * 2 + n]) for n in range(2)] for i in range(2)]
    lk = pltpu.make_async_copy(wk_hbm.at[:, pl.ds(pl.multiple_of(quarter * ncols, ncols), ncols)], wbuf.at[2, :, pl.ds(0, ncols)], lsem.at[5])
    lv = pltpu.make_async_copy(wv_hbm.at[:, pl.ds(pl.multiple_of(quarter * ncols, ncols), ncols)], wbuf.at[2, :, pl.ds(ncols, ncols)], lsem.at[6])
    lo = pltpu.make_async_copy(wo_hbm, wo_v, lsem.at[7])
    lkc = [pltpu.make_async_copy(k_hbm.at[pl.ds(i * cb, cb)], kout.at[pl.ds(i * cb, cb)], kvsem.at[0, i]) for i in range(chunks)]
    lvc = [pltpu.make_async_copy(v_hbm.at[pl.ds(i * cb, cb)], vout.at[pl.ds(i * cb, cb)], kvsem.at[1, i]) for i in range(chunks)]
    lx.start()
    for i in range(2):
        for n in range(2):
            lw[i][n].start()

    barrier = pltpu.get_barrier_semaphore()
    for d in range(chips):
        for f in range(CORES):
            if d or f:
                pl.semaphore_signal(barrier, inc=1, device_id=dev(chip + d, lax.rem(core + f, CORES)), device_id_type=MESH)

    lane_b = (lax.broadcasted_iota(jnp.int32, pos2_ref.shape, 1) + lax.broadcasted_iota(jnp.int32, pos2_ref.shape, 0) * pos2_ref.shape[1]) // 2
    pv = jnp.zeros(pos2_ref.shape, jnp.int32)
    for b in range(batch):
        pv = jnp.where(lane_b == b, pos_ref[b], pv)
    pos2_ref[...] = pv

    lx.wait()
    for i in range(2):
        lw[i][0].wait()
        q = jnp.dot(x_v[:, :hd], wbuf[i, :hd], preferred_element_type=F32)
        lw[i][1].wait()
        if i == 0:
            lk.start()
            lv.start()
        q = q + jnp.dot(x_v[:, hd:], wbuf[i, hd:], preferred_element_type=F32)
        for h in range(4):
            qs[pl.ds(i * 4 + h, batch, stride=8), :] = q[:, h * 128:(h + 1) * 128]
    q_all[quarter] = qs[...].astype(BF16)
    pl.semaphore_wait(barrier, chips * CORES - 1)

    def spread(buf, rows, ss, rs):
        copies = [pltpu.make_async_remote_copy(buf.at[quarter], buf.at[quarter], ss.at[0], rs.at[0], device_id=partner, device_id_type=MESH)]
        for side, shift in ((0, 1), (1, chips - 1)):
            part = pl.ds(side * rows // 2, rows // 2)
            copies.append(pltpu.make_async_remote_copy(
                buf.at[quarter, part], buf.at[quarter, part], ss.at[1 + side], rs.at[1 + side], device_id=dev(chip + shift, core), device_id_type=MESH))
        return copies

    def hand_on(copies, buf, rows, ss, rs):
        other = ((chip + 1) % 2) * CORES + core
        for side in range(2):
            copies[1 + side].wait_recv()
            part = pl.ds(side * rows // 2, rows // 2)
            c = pltpu.make_async_remote_copy(buf.at[other, part], buf.at[other, part], ss.at[3 + side], rs.at[3 + side], device_id=partner, device_id_type=MESH)
            c.start()
            copies.append(c)

    def arrive(copies):
        copies[0].wait_recv()
        copies[3].wait_recv()
        copies[4].wait_recv()

    q_copies = spread(q_all, batch * 8, q_ss, q_rs)
    for c in q_copies:
        c.start()
    lkc[0].start()
    lvc[0].start()
    lk.wait()
    lv.wait()
    kv = jnp.dot(x_v[...], wbuf[2], preferred_element_type=F32)
    for w in range(2):
        for k in range(2):
            qs[pl.ds(w * 128 + k, batch, stride=2), :] = kv[:, w * 256 + k * 128:w * 256 + (k + 1) * 128]
    for hf in range(2):
        for w in range(2):
            kv_all[quarter, hf * 128 + w * 64:hf * 128 + w * 64 + 64, :] = qs[w * 128 + hf * 64:w * 128 + hf * 64 + 64, :].astype(BF16)
    n_copies = spread(kv_all, batch * 4, n_ss, n_rs)
    for c in n_copies:
        c.start()
    rowb = lax.broadcasted_iota(jnp.int32, (64, 128), 0) // 8 % 2
    bm0 = jnp.where(rowb == 0, 1.0, 0.0).astype(BF16)
    bm1 = jnp.where(rowb == 1, 1.0, 0.0).astype(BF16)

    hand_on(q_copies, q_all, batch * 8, q_ss, q_rs)
    for i in range(1, chunks):
        lkc[i].start()
        lvc[i].start()
    lo.start()
    hand_on(n_copies, kv_all, batch * 4, n_ss, n_rs)
    arrive(q_copies)

    qlane = lax.broadcasted_iota(jnp.int32, (8, 128), 1)
    own_head = lax.broadcasted_iota(jnp.int32, (8, 128), 0) == (qlane % 64) // 16 * 2 + (qlane % 8) // 4
    qseq = qlane // 64 * 2 + (qlane // 8) % 2
    mt_ref[...] = jnp.zeros_like(mt_ref)

    def scores(qi, buf):
        zero = jnp.zeros((64, 256), BF16)
        rows = []
        for ph in range(2):
            p0 = (2 * qi + ph) * 16
            q = jnp.concatenate([q_all[t, p0:p0 + 16, :] for t in range(4)], axis=0)
            blocks = [q * bm0, q * bm1]
            rows.append(jnp.concatenate(blocks + [zero] if ph == 0 else [zero] + blocks, axis=1))
        kc = jnp.concatenate([kout[4 * qi + j] for j in range(4)], axis=1)
        s = lax.dot_general(kc, jnp.concatenate(rows, axis=0), NT, preferred_element_type=F32).reshape(local_len, 8, 128)
        lim = jnp.full((8, 128), -1, jnp.int32)
        for j in range(4):
            lim = jnp.where(own_head & (qseq == j), pos_ref[4 * qi + j] - base, lim)
        s = jnp.where(lax.broadcasted_iota(jnp.int32, s.shape, 0) < lim[None], s, -jnp.inf)
        buf[...] = s.reshape(buf.shape)
        return jnp.maximum(jnp.max(jnp.max(s, axis=0), axis=0, keepdims=True), NEG)

    def weigh(qi, buf, m):
        p = jnp.exp2((buf[...] - m) * scale2)
        quad = qi % (cb // 4)
        mt_ref[0, quad:quad + 1, :] = m
        mt_ref[1, quad:quad + 1, :] = jnp.sum(p, axis=0, keepdims=True)
        pt = p.astype(BF16).T
        for ph in range(2):
            b0 = 4 * qi + 2 * ph
            vc = jnp.concatenate([vout[b0], vout[b0 + 1]], axis=1)
            o = jnp.dot(pt[ph * 64:(ph + 1) * 64, :], vc, preferred_element_type=F32)
            for t in range(4):
                for b in range(2):
                    r0 = (b0 % cb + b) * 8
                    oraw[t, r0:r0 + 8, :] = o[t * 16 + b * 8:t * 16 + b * 8 + 8, b * 128:(b + 1) * 128]

    rows_c = cb * 8
    carry = {}

    def attend(k):
        if k == 0:
            lkc[0].wait()
            carry['m'] = scores(0, sa)
        elif k % 2 == 1 and k < 2 * chunks - 1:
            lkc[(k + 1) // 2].wait()
        if k % 2 == 0:
            lvc[k // 2].wait()
        m_b = scores(2 * k + 1, sb)
        weigh(2 * k, sa, carry['m'])
        if k < 2 * chunks - 1:
            carry['m'] = scores(2 * k + 2, sa)
        weigh(2 * k + 1, sb, m_b)

    lane = lax.broadcasted_iota(jnp.int32, (8, 128), 1)
    od, oi, yd, yi, ag = {}, {}, {}, {}, {}

    def finalize(i):
        hf = i * cb // half
        first = i * rows_c - hf * half * 8
        rr = lax.broadcasted_iota(jnp.int32, (rows_c, 64), 0) + first
        cc = lax.broadcasted_iota(jnp.int32, (rows_c, 64), 1)
        rel = pos2_ref[hf:hf + 1, :] - base
        keep = (rr // 4 == cc) & (rel >= 0) & (rel < local_len)
        mt, lt = mt_ref[0].T, mt_ref[1].T

        def by_row(x, t):
            return jnp.concatenate([jnp.broadcast_to(x[(p % 2) * 64 + t * 16:(p % 2) * 64 + t * 16 + 16, p // 2:p // 2 + 1], (16, 128))
                                    for p in range(cb // 2)], axis=0)

        quarters = range(4)
        sn = [lax.dot_general(q_all[t, i * rows_c:(i + 1) * rows_c, :], kv_all[t, hf * 128:hf * 128 + 64, :], NT, preferred_element_type=F32) for t in quarters]
        mo = [by_row(mt, t) for t in quarters]
        lo_ = [by_row(lt, t) for t in quarters]
        sn = [jnp.where(keep, x, -jnp.inf) for x in sn]
        top = [jnp.max(x, axis=1, keepdims=True) for x in sn]
        mn = [jnp.maximum(x, y) for x, y in zip(mo, top)]
        pn = [jnp.exp2((x - y[:, :64]) * scale2) for x, y in zip(sn, mn)]
        on = [jnp.dot(pn[t].astype(BF16), kv_all[t, hf * 128 + 64:hf * 128 + 128, :], preferred_element_type=F32) for t in quarters]
        ln = [jnp.sum(x, axis=1, keepdims=True) for x in pn]
        for t in quarters:
            w = jnp.exp2((mo[t] - mn[t]) * scale2)
            mraw[t] = mn[t]
            lraw[t] = lo_[t] * w + ln[t]
            oraw[t] = oraw[t] * w + on[t]
        for e in range(CORES):
            for t in range(4):
                mp = jnp.zeros((8, 128), F32)
                lp = jnp.zeros((8, 128), F32)
                for h in range(4):
                    src = pl.ds(e * 4 + h, cb, stride=8)
                    om[i, e, t, h * cb:(h + 1) * cb, :] = oraw[t, src, :]
                    mh = mraw[t, src, :]
                    lh = lraw[t, src, :]
                    for g in range(cb // 8):
                        sel = lane == h * (cb // 8) + g
                        mp = jnp.where(sel, mh[g * 8:(g + 1) * 8], mp)
                        lp = jnp.where(sel, lh[g * 8:(g + 1) * 8], lp)
                om[i, e, t, cb * 4:cb * 4 + 8, :] = mp
                om[i, e, t, cb * 4 + 8:cb * 4 + 16, :] = lp
        od[i] = pltpu.make_async_remote_copy(om.at[i, 1 - core], op.at[i], od_s.at[i], od_r.at[i], device_id=partner, device_id_type=MESH)
        od[i].start()

    nrow = cb * 4

    def merge(parts):
        ms = [p[nrow:nrow + 8] for p in parts]
        m = functools.reduce(jnp.maximum, ms)
        ws = [jnp.exp2((x - m) * scale2) for x in ms]
        l = functools.reduce(jnp.add, [w * p[nrow + 8:nrow + 16] for w, p in zip(ws, parts)])
        return m, l, ws

    def chip_reduce(i):
        od[i].wait_recv()
        for t in range(4):
            fold(om.at[i, core, t], om[i, core, t], op[i, t])
        oi[i] = []
        for d in range(1, chips):
            c = pltpu.make_async_remote_copy(om.at[i, core, lax.rem(chip + d, chips)], orecv.at[i, d - 1], oi_s.at[i, d - 1], oi_r.at[i, d - 1],
                                             device_id=dev(chip + d, core), device_id_type=MESH)
            c.start()
            oi[i].append(c)

    def fold(dst, a, b):
        m, l, (wa, wb) = merge([a, b])
        for g in range(nrow // 8):
            r = slice(g * 8, g * 8 + 8)
            dst[g * 8:g * 8 + 8, :] = a[r] * wa[:, g:g + 1] + b[r] * wb[:, g:g + 1]
        dst[nrow:nrow + 8, :] = m
        dst[nrow + 8:nrow + 16, :] = l

    def project(i):
        for c in oi[i]:
            c.wait_recv()
        if i == 0:
            lo.wait()
        parts = [om[i, core, chip]] + [orecv[i, d] for d in range(chips - 1)]
        m, l, ws = merge(parts)
        rl = 1.0 / l
        heads = []
        for h in range(4):
            rows = []
            for g in range(h * (cb // 8), (h + 1) * (cb // 8)):
                o = functools.reduce(jnp.add, [p[g * 8:g * 8 + 8] * w[:, g:g + 1] for p, w in zip(parts, ws)])
                rows.append(o * rl[:, g:g + 1])
            heads.append(jnp.concatenate(rows, axis=0).astype(BF16))
        lhs = jnp.concatenate(heads, axis=1)
        for e in range(CORES):
            for t in range(4):
                c0 = (e * 4 + t) * 512
                ys[i, e, t] = jnp.dot(lhs, wo_v[:, c0:c0 + 512], preferred_element_type=F32)
        yd[i] = pltpu.make_async_remote_copy(ys.at[i, 1 - core], yp.at[i], yd_s.at[i], yd_r.at[i], device_id=partner, device_id_type=MESH)
        yd[i].start()

    def y_chip(i):
        yd[i].wait_recv()
        ys[i, core] = ys[i, core] + yp[i]
        yi[i] = []
        for d in range(1, chips):
            c = pltpu.make_async_remote_copy(ys.at[i, core, lax.rem(chip + d, chips)], yr.at[i, d - 1], yi_s.at[i, d - 1], yi_r.at[i, d - 1],
                                             device_id=dev(chip + d, core), device_id_type=MESH)
            c.start()
            yi[i].append(c)

    def block(i, c):
        return (pl.ds(i * cb, cb), pl.ds(pl.multiple_of((core * 4 + c) * 512, 512), 512))

    def lay_rows():
        for w in range(2):
            for t in range(4):
                for hf in range(2):
                    sa[:64, :] = kv_all[t, hf * 128 + w * 64:hf * 128 + w * 64 + 64, :].astype(F32)
                    for k in range(2):
                        qs[pl.ds(hf * half * 8 + t * 2 + k, half, stride=8), :] = sa[pl.ds(k, half, stride=2), :]
            rows_ref[w] = qs[...].astype(BF16)

    def y_final(i):
        if i == chunks - 1:
            lay_rows()
        for c in yi[i]:
            c.wait_recv()
        y = ys[i, core, chip]
        for d in range(chips - 1):
            y = y + yr[i, d]
        yfull[block(i, chip)] = y.astype(BF16)
        ag[i] = []
        if i == chunks - 1:
            for d in range(chips):
                for f in range(CORES):
                    if d or f:
                        push(i, chip, dev(chip + d, lax.rem(core + f, CORES)))
        else:
            for d in range(1, chips):
                push(i, chip, dev(chip + d, core))
            push(i, chip, partner)

    def push(i, c, target):
        slot = len(ag[i])
        cp = pltpu.make_async_remote_copy(yfull.at[block(i, c)], yfull.at[block(i, c)], ag_s.at[i, slot], ag_r.at[i, slot], device_id=target, device_id_type=MESH)
        cp.start()
        ag[i].append(cp)

    def pass_on(i):
        for d in range(1, chips):
            ag[i][d - 1].wait_recv()
            push(i, lax.rem(chip + chips - d, chips), partner)

    plan = {1: [(finalize, 0)], 2: [(chip_reduce, 0)], 3: [(finalize, 1)], 4: [(chip_reduce, 1)],
            5: [(finalize, 2), (project, 0)], 6: [(chip_reduce, 2), (y_chip, 0), (project, 1)],
            7: [(finalize, 3), (y_chip, 1), (chip_reduce, 3), (y_final, 0), (project, 2), (y_chip, 2), (y_final, 1), (project, 3), (pass_on, 0),
                (y_chip, 3), (y_final, 2), (pass_on, 1), (y_final, 3), (pass_on, 2)]}
    for k in range(max(plan) + 1):
        if k < 2 * chunks:
            attend(k)
        if k == 1:
            arrive(n_copies)
        for stage, i in plan.get(k, ()):
            stage(i)
    for i in range(chunks):
        for c in ag[i] if i == chunks - 1 else ag[i][chips - 1:]:
            c.wait_recv()
    for c in q_copies + n_copies:
        c.wait_send()
    for i in range(chunks):
        for c in [od[i], yd[i]] + oi[i] + yi[i] + ag[i]:
            c.wait_send()


def write_kernel(k_in, v_in, new_ref, pos_ref, y_ref, k_out, k_ref, v_ref, y_out, bsem, ysem):
    batch, local_len = k_ref.shape[0], k_ref.shape[1] // 8
    base = lax.axis_index('seq') * local_len
    pieces = bsem.shape[0]
    pb = batch // pieces
    cy = pltpu.make_async_copy(y_ref, y_out, ysem)

    def patch(cache, which, first, last):
        @pl.loop(first, last)
        def _(b):
            rel = pos_ref[b] - base

            @pl.when((rel >= 0) & (rel < local_len))
            def _():
                cache[b, pl.ds(pl.multiple_of(rel * 8, 8), 8), :] = new_ref[which, pl.ds(pl.multiple_of(b * 8, 8), 8), :]

    copies = []
    for i in range(pieces):
        patch(k_ref, 0, i * pb, (i + 1) * pb)
        part = pl.ds(i * pb, pb)
        c = pltpu.make_async_copy(k_ref.at[part], k_out.at[part], bsem.at[i])
        c.start()
        copies.append(c)
    cy.start()
    patch(v_ref, 1, 0, batch)
    for c in copies + [cy]:
        c.wait()


def solution(mesh):
    cache_spec = P('rep', 'seq', None, None)
    in_specs = (P('rep', None), P(), P(), P(), P('seq', None), cache_spec, cache_spec, P('rep'))
    out_specs = (P('rep', None), cache_spec, cache_spec)
    chips = mesh.shape['seq'] // CORES
    assert chips == 4
    vm = pl.BlockSpec(memory_space=pltpu.VMEM)
    hbm = pl.BlockSpec(memory_space=pl.ANY)
    sm = pl.BlockSpec(memory_space=pltpu.SMEM)

    def local_step(x, wq, wk, wv, wo, k, v, pos):
        shape4 = k.shape
        batch, width = x.shape
        k3 = k.reshape(batch, -1, k.shape[-1])
        v3 = v.reshape(k3.shape)
        chunks = 4
        cb = batch // chunks
        dma = pltpu.SemaphoreType.DMA
        in_hbm = lambda a: pltpu.with_memory_space_constraint(a, pltpu.HBM)
        in_vmem = lambda a: pltpu.with_memory_space_constraint(a, pltpu.VMEM)
        y, ko, vo, new = pl.pallas_call(
            functools.partial(step_kernel, chips),
            out_shape=(pltpu.VMEM((batch, wo.shape[1]), BF16), pltpu.VMEM(k3.shape, BF16), pltpu.VMEM(k3.shape, BF16),
                       pltpu.VMEM((2, batch * 8, 128), BF16)),
            in_specs=[hbm] * 7 + [sm],
            out_specs=[vm] * 4,
            scratch_shapes=[
                pltpu.VMEM((batch, width), BF16), pltpu.VMEM((3, width, 512), BF16), pltpu.VMEM(wo.shape, BF16),
                pltpu.VMEM((batch * 8, 128), F32), pltpu.VMEM((4, batch * 8, 128), BF16), pltpu.VMEM((4, batch * 4, 128), BF16), pltpu.VMEM((k3.shape[1], 128), F32), pltpu.VMEM((k3.shape[1], 128), F32), pltpu.VMEM((2, 8, 128), F32), pltpu.VMEM((2, batch), jnp.int32),
                pltpu.VMEM((4, cb * 8, 128), F32), pltpu.VMEM((4, cb * 8, 128), F32), pltpu.VMEM((4, cb * 8, 128), F32),
                pltpu.VMEM((chunks, CORES, 4, cb * 4 + 16, 128), F32), pltpu.VMEM((chunks, 4, cb * 4 + 16, 128), F32),
                pltpu.VMEM((chunks, chips - 1, cb * 4 + 16, 128), F32),
                pltpu.VMEM((chunks, CORES, 4, cb, 512), F32), pltpu.VMEM((chunks, 4, cb, 512), F32), pltpu.VMEM((chunks, chips - 1, cb, 512), F32),
                dma((8,)), dma((2, chunks)), dma((5,)), dma((5,)), dma((5,)), dma((5,)), dma((chunks,)), dma((chunks,)),
                dma((chunks, chips - 1)), dma((chunks, chips - 1)), dma((chunks,)), dma((chunks,)),
                dma((chunks, chips - 1)), dma((chunks, chips - 1)), dma((chunks, chips * CORES - 1)), dma((chunks, chips * CORES - 1))],
            compiler_params=pltpu.CompilerParams(collective_id=0, has_side_effects=True, vmem_limit_bytes=29 << 20),
            name='step',
        )(in_hbm(x), in_hbm(wq), in_hbm(wk), in_hbm(wv), in_hbm(wo), in_hbm(k3), in_hbm(v3), pos)

        pieces = 16
        ko, _, vo, y = pl.pallas_call(
            write_kernel,
            out_shape=(jax.ShapeDtypeStruct(k3.shape, BF16), pltpu.VMEM(k3.shape, BF16), pltpu.VMEM(k3.shape, BF16), jax.ShapeDtypeStruct(y.shape, BF16)),
            in_specs=[vm, vm, vm, sm, vm],
            out_specs=[hbm, vm, vm, hbm],
            scratch_shapes=[dma((pieces,)), dma],
            input_output_aliases={0: 1, 1: 2},
            compiler_params=pltpu.CompilerParams(vmem_limit_bytes=4 << 20),
            name='write',
        )(in_vmem(ko), in_vmem(vo), in_vmem(new), pos, in_vmem(y))
        return y, ko.reshape(shape4), vo.reshape(shape4)

    return jax.shard_map(local_step, mesh=mesh, in_specs=in_specs, out_specs=out_specs, check_vma=False)
```
